16 devices in a mesh: dp: 2 (over y, z), sp: 8 (over x, core).
Axes of the slice: x: 4, y: 2, z: 1, core: 2. Of those that a mesh axis runs over, the one named last changes fastest.
The devices are a block of a 4x4x8 slice.
Arguments:
- dec_hidden: bfloat16 [2048, 512], P(('dp', 'sp')), parts along dimension 0
- enc_memory: bfloat16 [16384, 512], P(('dp', 'sp')), parts along dimension 0
- mem_len: int32 [2], P('dp'), parts along dimension 0
- norm_self: bfloat16 [2, 512], replicated
- norm_cross: bfloat16 [2, 512], replicated
- norm_mlp: bfloat16 [2, 512], replicated
- self_q: bfloat16 [2, 512, 512], replicated
- self_k: bfloat16 [2, 512, 512], replicated
- self_v: bfloat16 [2, 512, 512], replicated
- self_o: bfloat16 [2, 8, 64, 512], replicated
- cross_q: bfloat16 [2, 512, 512], replicated
- cross_k: bfloat16 [2, 512, 512], replicated
- cross_v: bfloat16 [2, 512, 512], replicated
- cross_o: bfloat16 [2, 8, 64, 512], replicated
- mlp_gate: bfloat16 [2, 512, 2048], replicated
- mlp_up: bfloat16 [2, 512, 2048], replicated
- mlp_down: bfloat16 [2, 2048, 512], replicated
Outputs:
- output: bfloat16 [2048, 512], P(('dp', 'sp')), parts along dimension 0
There are 2 independent parts. The reference program is written for one: setup_inputs(seed, part) draws one part's arguments, and reference() takes and returns one part's arrays. A program takes and returns all parts, laid end to end along the dimension named above; an argument that names none is the same for every part.
All inputs are finite; a program needn't handle non-finite values.
Results may differ from the reference program's by a relative error of at most 0.0152673.
Values are sent between devices in bfloat16 or wider.
A program may use at most 768 MiB of HBM per device.

```python
import jax
import jax.numpy as jnp
from jax import lax

D = 512
HEADS = 8
KV_HEADS = 8
HEAD = 64
FF = 2048
LAYERS = 2
TQ = 1024
TM = 8192
WAVES = 4
EPS = 1e-6
NEG_BIG = -1e30
SOFT_SCALE = HEAD ** -0.5
DKV = KV_HEADS * HEAD


def smooth_field(wave_key, n_rows, n_cols):
    directions = jax.random.normal(wave_key, (WAVES, n_cols), jnp.float32)
    positions = jnp.arange(n_rows, dtype=jnp.float32) / n_rows
    freq_list = jnp.arange(1, WAVES + 1, dtype=jnp.float32)
    wave_rows = jnp.cos(jnp.pi * positions[:, None] * freq_list[None, :])
    return jnp.dot(wave_rows, directions)


def setup_inputs(seed: int = 0, part: int = 0) -> dict:
    part_key = jax.random.fold_in(jax.random.key(seed), part)
    part_keys = jax.random.split(part_key, 5)
    shared = jax.random.split(jax.random.key(seed + 1), 16)

    def weight(key_index, shape_tail, fan_in):
        raw_draw = jax.random.normal(shared[key_index], (LAYERS,) + shape_tail, jnp.float32)
        return (raw_draw * fan_in ** -0.5).astype(jnp.bfloat16)

    def gain(key_index):
        return jax.random.uniform(shared[key_index], (LAYERS, D), jnp.float32, 0.5, 1.5).astype(jnp.bfloat16)

    dec_hidden = jax.random.normal(part_keys[0], (TQ, D), jnp.float32) + smooth_field(part_keys[1], TQ, D)
    enc_memory = jax.random.normal(part_keys[2], (TM, D), jnp.float32) + smooth_field(part_keys[3], TM, D)
    mem_len = jax.random.randint(part_keys[4], (1,), TM // 4, 3 * TM // 4 + 1, dtype=jnp.int32)
    return {
        'dec_hidden': dec_hidden.astype(jnp.bfloat16),
        'enc_memory': enc_memory.astype(jnp.bfloat16),
        'mem_len': mem_len,
        'norm_self': gain(0),
        'norm_cross': gain(1),
        'norm_mlp': gain(2),
        'self_q': weight(3, (D, D), D),
        'self_k': weight(4, (D, D), D),
        'self_v': weight(5, (D, D), D),
        'self_o': weight(6, (HEADS, HEAD, D), D),
        'cross_q': weight(7, (D, D), D),
        'cross_k': weight(8, (D, DKV), D),
        'cross_v': weight(9, (D, DKV), D),
        'cross_o': weight(10, (HEADS, HEAD, D), D),
        'mlp_gate': weight(11, (D, FF), D),
        'mlp_up': weight(12, (D, FF), D),
        'mlp_down': weight(13, (FF, D), FF),
    }


def rms_norm(hidden, gain_vec):
    hidden32 = hidden.astype(jnp.float32)
    inv_rms = lax.rsqrt(jnp.mean(hidden32 * hidden32, axis=-1, keepdims=True) + EPS)
    return (hidden32 * inv_rms * gain_vec.astype(jnp.float32)).astype(jnp.bfloat16)


def project(acts, weight_mat):
    return jnp.dot(acts, weight_mat, preferred_element_type=jnp.float32).astype(jnp.bfloat16)


def add_residual(hidden, update):
    return (hidden.astype(jnp.float32) + update).astype(jnp.bfloat16)


def head_attend(query_h, key_h, value_h, allowed):
    scores = jnp.dot(query_h, key_h.T, preferred_element_type=jnp.float32) * SOFT_SCALE
    scores = jnp.where(allowed, scores, NEG_BIG)
    weights = jnp.exp(scores - jnp.max(scores, axis=-1, keepdims=True))
    numerator = jnp.dot(weights.astype(jnp.bfloat16), value_h, preferred_element_type=jnp.float32)
    return numerator / jnp.sum(weights, axis=-1, keepdims=True)


def multi_head(queries, keys_all, values_all, allowed):
    q_rows = queries.shape[0]
    k_rows = keys_all.shape[0]
    kv_count = keys_all.shape[1] // HEAD
    q_heads = queries.reshape(q_rows, HEADS, HEAD).transpose(1, 0, 2)
    k_heads = jnp.repeat(keys_all.reshape(k_rows, kv_count, HEAD).transpose(1, 0, 2), HEADS // kv_count, axis=0)
    v_heads = jnp.repeat(values_all.reshape(k_rows, kv_count, HEAD).transpose(1, 0, 2), HEADS // kv_count, axis=0)
    per_head = lax.map(lambda head_trio: head_attend(head_trio[0], head_trio[1], head_trio[2], allowed), (q_heads, k_heads, v_heads))
    return per_head.transpose(1, 0, 2).astype(jnp.bfloat16)


def reference(dec_hidden, enc_memory, mem_len, norm_self, norm_cross, norm_mlp, self_q, self_k, self_v, self_o, cross_q, cross_k, cross_v, cross_o, mlp_gate, mlp_up, mlp_down):
    causal = jnp.arange(TQ)[:, None] >= jnp.arange(TQ)[None, :]
    mem_valid = (jnp.arange(TM) < mem_len[0])[None, :]
    stacked = {
        'norm_self': norm_self, 'norm_cross': norm_cross, 'norm_mlp': norm_mlp,
        'self_q': self_q, 'self_k': self_k, 'self_v': self_v, 'self_o': self_o,
        'cross_q': cross_q, 'cross_k': cross_k, 'cross_v': cross_v, 'cross_o': cross_o,
        'mlp_gate': mlp_gate, 'mlp_up': mlp_up, 'mlp_down': mlp_down,
    }

    def layer_step(hidden, params):
        normed = rms_norm(hidden, params['norm_self'])
        attended = multi_head(project(normed, params['self_q']), project(normed, params['self_k']), project(normed, params['self_v']), causal)
        update = jnp.einsum('thd,hdo->to', attended.astype(jnp.float32), params['self_o'].astype(jnp.float32))
        hidden = add_residual(hidden, update)
        normed = rms_norm(hidden, params['norm_cross'])
        attended = multi_head(project(normed, params['cross_q']), project(enc_memory, params['cross_k']), project(enc_memory, params['cross_v']), mem_valid)
        update = jnp.einsum('thd,hdo->to', attended.astype(jnp.float32), params['cross_o'].astype(jnp.float32))
        hidden = add_residual(hidden, update)
        normed = rms_norm(hidden, params['norm_mlp'])
        gate_pre = jnp.dot(normed, params['mlp_gate'], preferred_element_type=jnp.float32)
        up_proj = jnp.dot(normed, params['mlp_up'], preferred_element_type=jnp.float32)
        hidden_act = (jax.nn.silu(gate_pre) * up_proj).astype(jnp.bfloat16)
        update = jnp.dot(hidden_act, params['mlp_down'], preferred_element_type=jnp.float32)
        return add_residual(hidden, update), None

    final_hidden, _ = lax.scan(layer_step, dec_hidden, stacked)
    return final_hidden
```

```python
import functools

import jax
import jax.numpy as jnp
from jax import lax
from jax.experimental import pallas as pl
from jax.experimental.pallas import tpu as pltpu
from jax.sharding import PartitionSpec as P

EPS = 1e-6
NEG_BIG = -1e30
CORES = 2
KEY_BLOCK = 512
FF_BLOCK = 512
MEM_BLOCK = 256
F32 = jnp.float32
BF16 = jnp.bfloat16
MESH = pl.DeviceIdType.MESH
WEIGHTS = ('self_q', 'self_k', 'self_v', 'self_o', 'cross_k', 'cross_v', 'cross_q', 'cross_o', 'mlp_gate', 'mlp_up', 'mlp_down')
HALVED = ('cross_k', 'cross_v')


def rms_norm(hidden, gain_row):
    hidden32 = hidden.astype(F32)
    inv_rms = lax.rsqrt(jnp.mean(hidden32 * hidden32, axis=-1, keepdims=True) + EPS)
    return (hidden32 * inv_rms * gain_row.astype(F32)).astype(BF16)


def mm(a, b):
    return jnp.dot(a, b, preferred_element_type=F32)


def mm_t(a, b):
    return lax.dot_general(a, b, (((1,), (1,)), ((), ())), preferred_element_type=F32)


def lane_groups(rows, lanes, head_dim):
    return lax.broadcasted_iota(jnp.int32, (rows, lanes), 1) // head_dim


def stack_heads(q, head_dim, scale):
    rows, lanes = q.shape
    scaled = q.astype(F32) * scale
    group = lane_groups(rows, lanes, head_dim)
    return jnp.concatenate([jnp.where(group == h, scaled, 0.0).astype(BF16) for h in range(lanes // head_dim)], axis=0)


def attend(q_stack, key_block, value_block, n_keys, allowed, scores_ref):
    rows = q_stack.shape[0]
    run_max = None
    for start in range(0, n_keys, KEY_BLOCK):
        scores = mm_t(q_stack, key_block(start))
        scores = jnp.where(allowed(start), scores, NEG_BIG)
        scores_ref[:, start:start + KEY_BLOCK] = scores
        for lane in range(0, KEY_BLOCK, 128):
            tile = scores[:, lane:lane + 128]
            run_max = tile if run_max is None else jnp.maximum(run_max, tile)
    top = jnp.max(run_max, axis=-1, keepdims=True)
    run_sum = None
    numerator = None
    for start in range(0, n_keys, KEY_BLOCK):
        weights = jnp.exp(scores_ref[:, start:start + KEY_BLOCK] - top)
        for lane in range(0, KEY_BLOCK, 128):
            tile = weights[:, lane:lane + 128]
            run_sum = tile if run_sum is None else run_sum + tile
        part = mm(weights.astype(BF16), value_block(start))
        numerator = part if numerator is None else numerator + part
    return numerator, top, jnp.sum(run_sum, axis=-1, keepdims=True)


def unstack_heads(stacked, rows, head_dim):
    lanes = stacked.shape[1]
    group = lane_groups(rows, lanes, head_dim)
    out = stacked[:rows]
    for h in range(1, lanes // head_dim):
        out = jnp.where(group == h, stacked[h * rows:(h + 1) * rows], out)
    return out


def kernel(group, n_layers, head_dim, *refs):
    n_w = len(WEIGHTS)
    hidden_ref, memory_ref, mem_len_ref, norm_self, norm_cross, norm_mlp = refs[:6]
    w_hbm = dict(zip(WEIGHTS, refs[6:6 + n_w]))
    out_ref = refs[6 + n_w]
    scratch = refs[7 + n_w:]
    w = dict(zip(WEIGHTS, scratch[:n_w]))
    (mem_v, x_all, k_all, v_all, mem_k, mem_vals, q_send, q_all, part_send, part_recv, stat_send, stat_recv, hid, scores_ref,
     w_sem, mem_sem, mem_send, mem_recv, x_send, x_relay, x_recv, q_ssem, q_rsem, p_ssem, p_rsem, s_ssem, s_rsem) = scratch[n_w:]

    rows, width = hidden_ref.shape
    mem_rows = memory_ref.shape[0]
    chips = group // CORES
    half = q_send.shape[-1]
    hpg = half // head_dim
    scale = head_dim ** -0.5
    me = lax.axis_index('sp')
    chip, core = me // CORES, me % CORES
    partner = chip * CORES + (1 - core)

    def remote(src, dst, ssem, rsem, dev):
        return pltpu.make_async_remote_copy(src_ref=src, dst_ref=dst, send_sem=ssem, recv_sem=rsem, device_id={'sp': dev}, device_id_type=MESH)

    def weight_copy(name, layer):
        src = w_hbm[name].at[layer]
        if name in HALVED:
            src = w_hbm[name].at[layer, :, pl.ds(pl.multiple_of(core * half, half), half)]
        return pltpu.make_async_copy(src, w[name].at[layer], w_sem.at[WEIGHTS.index(name), layer])

    mem_copy = pltpu.make_async_copy(memory_ref, mem_v.at[core], mem_sem.at[0])

    for name in ('self_q', 'self_k', 'self_v'):
        weight_copy(name, 0).start()
    mem_copy.start()
    for layer in range(n_layers):
        for name in HALVED:
            weight_copy(name, layer).start()
    for layer in range(n_layers):
        for name in WEIGHTS:
            if name in HALVED or (layer == 0 and name in ('self_q', 'self_k', 'self_v')):
                continue
            weight_copy(name, layer).start()

    barrier = pltpu.get_barrier_semaphore()
    for step in range(1, group):
        pl.semaphore_signal(barrier, inc=1, device_id={'sp': lax.rem(me + step, group)}, device_id_type=MESH)
    pl.semaphore_wait(barrier, group - 1)

    def x_to_chip(layer, d):
        return remote(x_all.at[layer, me], x_all.at[layer, me], x_send.at[layer, d], x_recv.at[layer, me], me + d * CORES)

    def x_to_partner(layer):
        return remote(x_all.at[layer, me], x_all.at[layer, me], x_send.at[layer, 0], x_recv.at[layer, me], partner)

    def x_relayed(layer, d):
        src = me - d * CORES
        return remote(x_all.at[layer, src], x_all.at[layer, src], x_relay.at[layer, d], x_recv.at[layer, src], partner)

    def x_arrival(layer, src):
        return remote(x_all.at[layer, src], x_all.at[layer, src], x_send.at[layer, 0], x_recv.at[layer, src], partner)

    def q_copy(layer, d, k):
        dst = lax.rem(chip + d, chips) * CORES + k
        return remote(q_send.at[layer, k], q_all.at[layer, me], q_ssem.at[layer, d * CORES + k], q_rsem.at[layer, me], dst)

    def q_to_partner(layer):
        return remote(q_send.at[layer, 1 - core], q_all.at[layer, me], q_ssem.at[layer, 0], q_rsem.at[layer, me], partner)

    def q_arrival(layer, src):
        return remote(q_send.at[layer, 0], q_all.at[layer, src], q_ssem.at[layer, 0], q_rsem.at[layer, src], partner)

    def part_copy(layer, src):
        return remote(part_send.at[layer, src], part_recv.at[layer, me], p_ssem.at[layer, src], p_rsem.at[layer, me], src)

    def stat_copy(layer, src):
        return remote(stat_send.at[layer, src], stat_recv.at[layer, me], s_ssem.at[layer, src], s_rsem.at[layer, me], src)

    def part_arrival(layer, src):
        return remote(part_send.at[layer, src], part_recv.at[layer, src], p_ssem.at[layer, src], p_rsem.at[layer, src], partner)

    def stat_arrival(layer, src):
        return remote(stat_send.at[layer, src], stat_recv.at[layer, src], s_ssem.at[layer, src], s_rsem.at[layer, src], partner)

    mem_out = remote(mem_v.at[core], mem_v.at[core], mem_send.at[0], mem_recv.at[0], partner)
    mem_in = remote(mem_v.at[1 - core], mem_v.at[1 - core], mem_send.at[0], mem_recv.at[0], partner)

    def project_memory(slot):
        def body(i, carry):
            at = pl.ds(pl.multiple_of(i * MEM_BLOCK, MEM_BLOCK), MEM_BLOCK)
            to = pl.ds(pl.multiple_of(slot * mem_rows + i * MEM_BLOCK, MEM_BLOCK), MEM_BLOCK)
            block = mem_v[slot, at, :]
            for layer in range(n_layers):
                mem_k[layer, to, :] = mm(block, w['cross_k'][layer]).astype(BF16)
                mem_vals[layer, to, :] = mm(block, w['cross_v'][layer]).astype(BF16)
            return carry
        lax.fori_loop(0, mem_rows // MEM_BLOCK, body, 0)

    hid[...] = hidden_ref[...]
    for src in range(group):
        @pl.when(src > me)
        def _():
            k_all[src] = jnp.zeros((rows, width), BF16)
            v_all[src] = jnp.zeros((rows, width), BF16)

    for layer in range(n_layers):
        x_all[layer, me] = rms_norm(hid[...], norm_self[layer:layer + 1, :])
        for d in (2, 1, 3):
            if d < chips:
                @pl.when(chip + d < chips)
                def _():
                    x_to_chip(layer, d).start()

        @pl.when(core == 0)
        def _():
            x_to_partner(layer).start()

        if layer == 0:
            for name in ('self_q', 'self_k', 'self_v'):
                weight_copy(name, layer).wait()
        else:
            for name in ('self_q', 'self_k', 'self_v'):
                weight_copy(name, layer).wait()

        def project_rows(src):
            block = x_all[layer, src]
            k_all[src] = mm(block, w['self_k'][layer]).astype(BF16)
            v_all[src] = mm(block, w['self_v'][layer]).astype(BF16)

        project_rows(me)
        queries = mm(x_all[layer, me], w['self_q'][layer]).astype(BF16)

        if layer == 0:
            mem_copy.wait()
            mem_out.start()
            for other in range(n_layers):
                for name in HALVED:
                    weight_copy(name, other).wait()
            project_memory(core)

        for d in range(1, chips):
            @pl.when(chip - d >= 0)
            def _():
                x_arrival(layer, me - d * CORES).wait_recv()
                x_relayed(layer, d).start()
                project_rows(me - d * CORES)

        @pl.when(core == 1)
        def _():
            x_arrival(layer, partner).wait_recv()
            project_rows(partner)

        for d in range(1, chips):
            @pl.when(chip - d >= 0)
            def _():
                x_arrival(layer, partner - d * CORES).wait_recv()
                project_rows(partner - d * CORES)

        if layer == 0:
            mem_in.wait_recv()
            project_memory(1 - core)

        all_rows = group * rows
        query_at = me * rows + lax.rem(lax.broadcasted_iota(jnp.int32, (hpg * rows, KEY_BLOCK), 0), rows)
        key_at = lax.broadcasted_iota(jnp.int32, (hpg * rows, KEY_BLOCK), 1)
        per_block = KEY_BLOCK // rows
        attended = []
        for g in range(CORES):
            lanes = slice(g * half, (g + 1) * half)
            num, _, den = attend(
                stack_heads(queries[:, lanes], head_dim, scale),
                lambda start: k_all[start // rows:start // rows + per_block, :, lanes].reshape(KEY_BLOCK, half),
                lambda start: v_all[start // rows:start // rows + per_block, :, lanes].reshape(KEY_BLOCK, half),
                all_rows, lambda start: key_at + start <= query_at, scores_ref)
            attended.append(unstack_heads(num / den, rows, head_dim).astype(BF16))
        attended = jnp.concatenate(attended, axis=-1)
        weight_copy('self_o', layer).wait()
        hidden = (hid[...].astype(F32) + mm(attended, w['self_o'][layer])).astype(BF16)
        hid[...] = hidden

        weight_copy('cross_q', layer).wait()
        queries = mm(rms_norm(hidden, norm_cross[layer:layer + 1, :]), w['cross_q'][layer]).astype(BF16)
        for g in range(CORES):
            q_send[layer, g] = queries[:, g * half:(g + 1) * half]
        q_to_partner(layer).start()
        for d in (1, 3, 2):
            if d < chips:
                for k in range(CORES):
                    q_copy(layer, d, k).start()
        q_all[layer, me] = q_send[layer, core]

        mem_at = chip * (CORES * mem_rows) + lax.broadcasted_iota(jnp.int32, (1, KEY_BLOCK), 1)
        last = group - 1

        def chunk(j, carry):
            is_last = j // last
            is_first = 1 - (j + last - 1) // last
            mid = 1 - is_first - is_last
            pair = (j + 1) // CORES - 1
            d = mid * (1 + CORES * pair - 3 * (pair // 2))
            k = is_first * core + is_last * (1 - core) + mid * lax.rem(j + 1, CORES)
            src = lax.rem(chip + d, chips) * CORES + k

            @pl.when(j > 0)
            def _():
                q_arrival(layer, src).wait_recv()

            num, top, den = attend(
                stack_heads(q_all[layer, src], head_dim, scale),
                lambda start: mem_k[layer, start:start + KEY_BLOCK, :],
                lambda start: mem_vals[layer, start:start + KEY_BLOCK, :],
                CORES * mem_rows, lambda start: mem_at + start < mem_len_ref[0], scores_ref)
            part = unstack_heads(num, rows, head_dim).astype(BF16)
            lane = lax.broadcasted_iota(jnp.int32, (rows, 128), 1)
            stats = jnp.zeros((rows, 128), F32)
            for h in range(hpg):
                stats = jnp.where(lane == h, top[h * rows:(h + 1) * rows], stats)
                stats = jnp.where(lane == hpg + h, den[h * rows:(h + 1) * rows], stats)
            stats = jnp.transpose(stats)[:2 * hpg]

            @pl.when(j == 0)
            def _():
                part_recv[layer, me] = part
                stat_recv[layer, me] = stats

            @pl.when(j > 0)
            def _():
                part_send[layer, src] = part
                stat_send[layer, src] = stats
                part_copy(layer, src).start()
                stat_copy(layer, src).start()
            return carry

        lax.fori_loop(0, group, chunk, 0)

        def arrived(step, carry):
            src = lax.rem(me + step, group)
            stat_arrival(layer, src).wait_recv()
            part_arrival(layer, src).wait_recv()
            return carry

        lax.fori_loop(1, group, arrived, 0)

        factors = [None] * group
        for g in range(CORES):
            members = [c * CORES + g for c in range(chips)]
            tops = [stat_recv[layer, i, 0:hpg] for i in members]
            dens = [stat_recv[layer, i, hpg:2 * hpg] for i in members]
            best = functools.reduce(jnp.maximum, tops)
            shares = [jnp.exp(t - best) for t in tops]
            total = functools.reduce(jnp.add, [s * d for s, d in zip(shares, dens)])
            for i, s in zip(members, shares):
                factors[i] = s / total
        packed = jnp.concatenate(factors + [jnp.zeros((128 - group * hpg, rows), F32)], axis=0)
        packed = jnp.transpose(packed)
        lane_group = lane_groups(rows, half, head_dim)
        attended = []
        for g in range(CORES):
            total = jnp.zeros((rows, half), F32)
            for c in range(chips):
                i = c * CORES + g
                factor = jnp.zeros((rows, half), F32)
                for h in range(hpg):
                    factor = jnp.where(lane_group == h, packed[:, i * hpg + h:i * hpg + h + 1], factor)
                total = total + part_recv[layer, i].astype(F32) * factor
            attended.append(total.astype(BF16))
        attended = jnp.concatenate(attended, axis=-1)
        weight_copy('cross_o', layer).wait()
        hidden = (hid[...].astype(F32) + mm(attended, w['cross_o'][layer])).astype(BF16)

        normed = rms_norm(hidden, norm_mlp[layer:layer + 1, :])
        for name in ('mlp_gate', 'mlp_up', 'mlp_down'):
            weight_copy(name, layer).wait()
        update = None
        for start in range(0, w['mlp_gate'].shape[-1], FF_BLOCK):
            cols = slice(start, start + FF_BLOCK)
            gate = mm(normed, w['mlp_gate'][layer, :, cols])
            up = mm(normed, w['mlp_up'][layer, :, cols])
            act = (gate * jax.nn.sigmoid(gate) * up).astype(BF16)
            part = mm(act, w['mlp_down'][layer, cols, :])
            update = part if update is None else update + part
        hidden = (hidden.astype(F32) + update).astype(BF16)
        hid[...] = hidden

    out_ref[...] = hid[...]

    mem_out.wait_send()
    for layer in range(n_layers):
        for d in range(1, chips):
            @pl.when(chip + d < chips)
            def _():
                x_to_chip(layer, d).wait_send()

            @pl.when(chip - d >= 0)
            def _():
                x_relayed(layer, d).wait_send()

            for k in range(CORES):
                q_copy(layer, d, k).wait_send()

        @pl.when(core == 0)
        def _():
            x_to_partner(layer).wait_send()
        q_to_partner(layer).wait_send()

        def sent(step, carry):
            src = lax.rem(me + step, group)
            part_copy(layer, src).wait_send()
            stat_copy(layer, src).wait_send()
            return carry

        lax.fori_loop(1, group, sent, 0)


def solution(mesh):
    group = mesh.shape['sp']
    row_spec = P(('dp', 'sp'), None)

    def local_step(hidden, memory, mem_len, norm_self, norm_cross, norm_mlp, self_q, self_k, self_v, self_o, cross_q, cross_k, cross_v, cross_o, mlp_gate, mlp_up, mlp_down):
        rows, width = hidden.shape
        mem_rows = memory.shape[0]
        n_layers, n_heads, head_dim = self_o.shape[:3]
        inner = n_heads * head_dim
        half = inner // CORES
        hpg = half // head_dim
        all_keys = max(group * rows, CORES * mem_rows)
        weights = dict(
            self_q=self_q, self_k=self_k, self_v=self_v, self_o=self_o.reshape(n_layers, inner, width), cross_k=cross_k, cross_v=cross_v,
            cross_q=cross_q, cross_o=cross_o.reshape(n_layers, inner, width), mlp_gate=mlp_gate, mlp_up=mlp_up, mlp_down=mlp_down)
        w_scratch = [
            pltpu.VMEM((n_layers, width, half) if name in HALVED else weights[name].shape, BF16) for name in WEIGHTS]
        dma = pltpu.SemaphoreType.DMA
        vmem = pl.BlockSpec(memory_space=pltpu.VMEM)
        hbm = pl.BlockSpec(memory_space=pl.ANY)
        return pl.pallas_call(
            functools.partial(kernel, group, n_layers, head_dim),
            out_shape=jax.ShapeDtypeStruct((rows, width), BF16),
            in_specs=[vmem, hbm, pl.BlockSpec(memory_space=pltpu.SMEM), vmem, vmem, vmem] + [hbm] * len(WEIGHTS),
            out_specs=vmem,
            scratch_shapes=w_scratch + [
                pltpu.VMEM((CORES, mem_rows, width), BF16),
                pltpu.VMEM((n_layers, group, rows, width), BF16),
                pltpu.VMEM((group, rows, width), BF16),
                pltpu.VMEM((group, rows, width), BF16),
                pltpu.VMEM((n_layers, CORES * mem_rows, half), BF16),
                pltpu.VMEM((n_layers, CORES * mem_rows, half), BF16),
                pltpu.VMEM((n_layers, CORES, rows, half), BF16),
                pltpu.VMEM((n_layers, group, rows, half), BF16),
                pltpu.VMEM((n_layers, group, rows, half), BF16),
                pltpu.VMEM((n_layers, group, rows, half), BF16),
                pltpu.VMEM((n_layers, group, 2 * hpg, rows), F32),
                pltpu.VMEM((n_layers, group, 2 * hpg, rows), F32),
                pltpu.VMEM((rows, width), BF16),
                pltpu.VMEM((hpg * rows, all_keys), F32),
                dma((len(WEIGHTS), n_layers)),
                dma((1,)), dma((1,)), dma((1,)),
                dma((n_layers, group // CORES)), dma((n_layers, group // CORES)), dma((n_layers, group)),
                dma((n_layers, group)), dma((n_layers, group)),
                dma((n_layers, group)), dma((n_layers, group)),
                dma((n_layers, group)), dma((n_layers, group)),
            ],
            compiler_params=pltpu.CompilerParams(collective_id=0, has_side_effects=True, vmem_limit_bytes=60 * 1024 * 1024),
        )(hidden, memory, mem_len, norm_self, norm_cross, norm_mlp, *[weights[name] for name in WEIGHTS])

    return jax.shard_map(local_step, mesh=mesh, in_specs=(row_spec, row_spec, P('dp')) + (P(),) * 14, out_specs=row_spec, check_vma=False)
```

```python
import functools

import jax
import jax.numpy as jnp
from jax import lax
from jax.experimental import pallas as pl
from jax.experimental.pallas import tpu as pltpu
from jax.sharding import PartitionSpec as P

EPS = 1e-6
NEG_BIG = -1e30
CORES = 2
KEY_BLOCK = 512
FF_BLOCK = 512
MEM_BLOCK = 256
MEM_LEN_MAX = 6144
F32 = jnp.float32
BF16 = jnp.bfloat16
MESH = pl.DeviceIdType.MESH
WEIGHTS = ('self_q', 'self_k', 'self_v', 'self_o', 'cross_k', 'cross_v', 'cross_q', 'cross_o', 'mlp_gate', 'mlp_up', 'mlp_down')
HALVED = ('cross_k', 'cross_v')


def rms_norm(hidden, gain_row):
    hidden32 = hidden.astype(F32)
    inv_rms = lax.rsqrt(jnp.mean(hidden32 * hidden32, axis=-1, keepdims=True) + EPS)
    return (hidden32 * inv_rms * gain_row.astype(F32)).astype(BF16)


def mm(a, b):
    return jnp.dot(a, b, preferred_element_type=F32)


def mm_t(a, b):
    return lax.dot_general(a, b, (((1,), (1,)), ((), ())), preferred_element_type=F32)


def lane_groups(rows, lanes, head_dim):
    return lax.broadcasted_iota(jnp.int32, (rows, lanes), 1) // head_dim


def stack_heads(q, head_dim, scale):
    rows, lanes = q.shape
    scaled = q.astype(F32) * scale
    group = lane_groups(rows, lanes, head_dim)
    return jnp.concatenate([jnp.where(group == h, scaled, 0.0).astype(BF16) for h in range(lanes // head_dim)], axis=0)


def score(q_stack, key_block, n_keys, allowed, scores_ref, max_ref):
    run_max = None
    for start in range(0, n_keys, KEY_BLOCK):
        scores = mm_t(q_stack, key_block(start))
        scores = jnp.where(allowed(start), scores, NEG_BIG)
        scores_ref[:, start:start + KEY_BLOCK] = scores
        for lane in range(0, KEY_BLOCK, 128):
            tile = scores[:, lane:lane + 128]
            run_max = tile if run_max is None else jnp.maximum(run_max, tile)
    max_ref[...] = run_max


def gather_values(value_block, n_keys, scores_ref, max_ref):
    top = jnp.max(max_ref[...], axis=-1, keepdims=True)
    run_sum = None
    numerator = None
    for start in range(0, n_keys, KEY_BLOCK):
        weights = jnp.exp(scores_ref[:, start:start + KEY_BLOCK] - top)
        for lane in range(0, KEY_BLOCK, 128):
            tile = weights[:, lane:lane + 128]
            run_sum = tile if run_sum is None else run_sum + tile
        part = mm(weights.astype(BF16), value_block(start))
        numerator = part if numerator is None else numerator + part
    return numerator, top, jnp.sum(run_sum, axis=-1, keepdims=True)


def unstack_heads(stacked, rows, head_dim):
    lanes = stacked.shape[1]
    group = lane_groups(rows, lanes, head_dim)
    out = stacked[:rows]
    for h in range(1, lanes // head_dim):
        out = jnp.where(group == h, stacked[h * rows:(h + 1) * rows], out)
    return out


class Phase:
    def __init__(self):
        self.cur = None

    def __call__(self, name):
        if self.cur is not None:
            self.cur.__exit__(None, None, None)
        self.cur = jax.named_scope(name) if name else None
        if self.cur is not None:
            self.cur.__enter__()


def kernel(group, n_layers, head_dim, *refs):
    n_w = len(WEIGHTS)
    hidden_ref, memory_ref, mem_len_ref, norm_self, norm_cross, norm_mlp = refs[:6]
    w_hbm = dict(zip(WEIGHTS, refs[6:6 + n_w]))
    out_ref = refs[6 + n_w]
    scratch = refs[7 + n_w:]
    w = dict(zip(WEIGHTS, scratch[:n_w]))
    (mem_v, x_all, k_all, v_all, mem_k, mem_vals, q_send, q_all, part_send, part_recv, stat_send, stat_recv, hid, scores_a, scores_b, max_a, max_b,
     w_sem, mem_sem, mem_send, mem_recv, x_send, x_relay, x_recv, q_ssem, q_rsem, p_ssem, p_rsem, s_ssem, s_rsem) = scratch[n_w:]

    rows, width = hidden_ref.shape
    mem_rows = memory_ref.shape[0]
    chips = group // CORES
    mem_chips = -(-MEM_LEN_MAX // (CORES * mem_rows))
    half = q_send.shape[-1]
    hpg = half // head_dim
    scale = head_dim ** -0.5
    me = lax.axis_index('sp')
    chip, core = me // CORES, me % CORES
    partner = chip * CORES + (1 - core)

    def remote(src, dst, ssem, rsem, dev):
        return pltpu.make_async_remote_copy(src_ref=src, dst_ref=dst, send_sem=ssem, recv_sem=rsem, device_id={'sp': dev}, device_id_type=MESH)

    def weight_copy(name, layer):
        src = w_hbm[name].at[layer]
        if name in HALVED:
            src = w_hbm[name].at[layer, :, pl.ds(pl.multiple_of(core * half, half), half)]
        return pltpu.make_async_copy(src, w[name].at[layer], w_sem.at[WEIGHTS.index(name), layer])

    phase = Phase()
    phase('start')
    mem_copy = pltpu.make_async_copy(memory_ref, mem_v.at[core], mem_sem.at[0])

    for name in ('self_q', 'self_k', 'self_v'):
        weight_copy(name, 0).start()
    mem_copy.start()
    for layer in range(n_layers):
        for name in HALVED:
            weight_copy(name, layer).start()
    for layer in range(n_layers):
        for name in WEIGHTS:
            if name in HALVED or (layer == 0 and name in ('self_q', 'self_k', 'self_v')):
                continue
            weight_copy(name, layer).start()

    phase('barrier')
    barrier = pltpu.get_barrier_semaphore()
    for step in range(1, group):
        pl.semaphore_signal(barrier, inc=1, device_id={'sp': lax.rem(me + step, group)}, device_id_type=MESH)
    pl.semaphore_wait(barrier, group - 1)

    def x_to_chip(layer, d):
        return remote(x_all.at[layer, me], x_all.at[layer, me], x_send.at[layer, d], x_recv.at[layer, me], me + d * CORES)

    def x_to_partner(layer):
        return remote(x_all.at[layer, me], x_all.at[layer, me], x_send.at[layer, 0], x_recv.at[layer, me], partner)

    def x_relayed(layer, d):
        src = me - d * CORES
        return remote(x_all.at[layer, src], x_all.at[layer, src], x_relay.at[layer, d], x_recv.at[layer, src], partner)

    def x_arrival(layer, src):
        return remote(x_all.at[layer, src], x_all.at[layer, src], x_send.at[layer, 0], x_recv.at[layer, src], partner)

    def q_copy(layer, d, k):
        dst = lax.rem(chip + d, chips) * CORES + k
        return remote(q_send.at[layer, k], q_all.at[layer, me], q_ssem.at[layer, d * CORES + k], q_rsem.at[layer, me], dst)

    def q_to_partner(layer):
        return remote(q_send.at[layer, 1 - core], q_all.at[layer, me], q_ssem.at[layer, 0], q_rsem.at[layer, me], partner)

    def q_arrival(layer, src):
        return remote(q_send.at[layer, 0], q_all.at[layer, src], q_ssem.at[layer, 0], q_rsem.at[layer, src], partner)

    def part_copy(layer, src):
        return remote(part_send.at[layer, src], part_recv.at[layer, me], p_ssem.at[layer, src], p_rsem.at[layer, me], src)

    def stat_copy(layer, src):
        return remote(stat_send.at[layer, src], stat_recv.at[layer, me], s_ssem.at[layer, src], s_rsem.at[layer, me], src)

    def part_arrival(layer, src):
        return remote(part_send.at[layer, src], part_recv.at[layer, src], p_ssem.at[layer, src], p_rsem.at[layer, src], partner)

    def stat_arrival(layer, src):
        return remote(stat_send.at[layer, src], stat_recv.at[layer, src], s_ssem.at[layer, src], s_rsem.at[layer, src], partner)

    mem_out = remote(mem_v.at[core], mem_v.at[core], mem_send.at[0], mem_recv.at[0], partner)
    mem_in = remote(mem_v.at[1 - core], mem_v.at[1 - core], mem_send.at[0], mem_recv.at[0], partner)

    def project_memory(slot):
        def body(i, carry):
            at = pl.ds(pl.multiple_of(i * MEM_BLOCK, MEM_BLOCK), MEM_BLOCK)
            to = pl.ds(pl.multiple_of(slot * mem_rows + i * MEM_BLOCK, MEM_BLOCK), MEM_BLOCK)
            block = mem_v[slot, at, :]
            for layer in range(n_layers):
                mem_k[layer, to, :] = mm(block, w['cross_k'][layer]).astype(BF16)
                mem_vals[layer, to, :] = mm(block, w['cross_v'][layer]).astype(BF16)
            return carry
        lax.fori_loop(0, mem_rows // MEM_BLOCK, body, 0)

    phase('zero')
    hid[...] = hidden_ref[...]
    for src in range(group):
        @pl.when(src > me)
        def _():
            k_all[src] = jnp.zeros((rows, width), BF16)
            v_all[src] = jnp.zeros((rows, width), BF16)

    for layer in range(n_layers):
        phase(f'xnorm{layer}')
        x_all[layer, me] = rms_norm(hid[...], norm_self[layer:layer + 1, :])
        for d in (2, 1, 3):
            if d < chips:
                @pl.when(chip + d < chips)
                def _():
                    x_to_chip(layer, d).start()

        @pl.when(core == 0)
        def _():
            x_to_partner(layer).start()

        if layer == 0:
            for name in ('self_q', 'self_k', 'self_v'):
                weight_copy(name, layer).wait()
        else:
            for name in ('self_q', 'self_k', 'self_v'):
                weight_copy(name, layer).wait()

        def project_rows(src):
            block = x_all[layer, src]
            k_all[src] = mm(block, w['self_k'][layer]).astype(BF16)
            v_all[src] = mm(block, w['self_v'][layer]).astype(BF16)

        phase(f'ownproj{layer}')
        project_rows(me)
        queries = mm(x_all[layer, me], w['self_q'][layer]).astype(BF16)

        phase(f'memproj{layer}')
        if layer == 0:
            mem_copy.wait()
            for other in range(n_layers):
                for name in HALVED:
                    weight_copy(name, other).wait()

            @pl.when(chip < mem_chips)
            def _():
                mem_out.start()
                project_memory(core)
        phase(f'xwait{layer}')

        for d in range(1, chips):
            @pl.when(chip - d >= 0)
            def _():
                x_arrival(layer, me - d * CORES).wait_recv()
                x_relayed(layer, d).start()
                project_rows(me - d * CORES)

        @pl.when(core == 1)
        def _():
            x_arrival(layer, partner).wait_recv()
            project_rows(partner)

        for d in range(1, chips):
            @pl.when(chip - d >= 0)
            def _():
                x_arrival(layer, partner - d * CORES).wait_recv()
                project_rows(partner - d * CORES)

        phase(f'memproj2{layer}')
        if layer == 0:
            @pl.when(chip < mem_chips)
            def _():
                mem_in.wait_recv()
                project_memory(1 - core)

        phase(f'selfatt{layer}')
        all_rows = group * rows
        query_at = me * rows + lax.rem(lax.broadcasted_iota(jnp.int32, (hpg * rows, KEY_BLOCK), 0), rows)
        key_at = lax.broadcasted_iota(jnp.int32, (hpg * rows, KEY_BLOCK), 1)
        per_block = KEY_BLOCK // rows
        stores = ((scores_a, max_a), (scores_b, max_b))
        for g in range(CORES):
            lanes = slice(g * half, (g + 1) * half)
            score(stack_heads(queries[:, lanes], head_dim, scale),
                  lambda start: k_all[start // rows:start // rows + per_block, :, lanes].reshape(KEY_BLOCK, half),
                  all_rows, lambda start: key_at + start <= query_at, *stores[g])
        attended = []
        for g in range(CORES):
            lanes = slice(g * half, (g + 1) * half)
            num, _, den = gather_values(
                lambda start: v_all[start // rows:start // rows + per_block, :, lanes].reshape(KEY_BLOCK, half), all_rows, *stores[g])
            attended.append(unstack_heads(num / den, rows, head_dim).astype(BF16))
        attended = jnp.concatenate(attended, axis=-1)
        phase(f'oproj{layer}')
        weight_copy('self_o', layer).wait()
        hidden = (hid[...].astype(F32) + mm(attended, w['self_o'][layer])).astype(BF16)
        hid[...] = hidden

        phase(f'qproj{layer}')
        weight_copy('cross_q', layer).wait()
        queries = mm(rms_norm(hidden, norm_cross[layer:layer + 1, :]), w['cross_q'][layer]).astype(BF16)
        for g in range(CORES):
            q_send[layer, g] = queries[:, g * half:(g + 1) * half]
        q_order = [(d, k) for t in range(1, chips) for k, d in ((0, chips - t), (1, t))]

        @pl.when(chip < mem_chips)
        def _():
            q_to_partner(layer).start()
        for d, k in q_order:
            @pl.when(lax.rem(chip + d, chips) < mem_chips)
            def _():
                q_copy(layer, d, k).start()
        q_all[layer, me] = q_send[layer, core]

        mem_at = chip * (CORES * mem_rows) + lax.broadcasted_iota(jnp.int32, (1, KEY_BLOCK), 1)
        n_keys = CORES * mem_rows

        def source(turn, second):
            low = 1 - (turn + chips - 1) // chips
            d = turn * (1 - core) + (chips - turn) * core
            k = low * (core + second - 2 * core * second) + (1 - low) * second
            return lax.rem(chip + d, chips) * CORES + k

        def score_of(src, scores_ref, max_ref):
            score(stack_heads(q_all[layer, src], head_dim, scale), lambda start: mem_k[layer, start:start + KEY_BLOCK, :], n_keys,
                  lambda start: mem_at + start < mem_len_ref[0], scores_ref, max_ref)

        def values_of(scores_ref, max_ref):
            num, top, den = gather_values(lambda start: mem_vals[layer, start:start + KEY_BLOCK, :], n_keys, scores_ref, max_ref)
            part = unstack_heads(num, rows, head_dim).astype(BF16)
            lane = lax.broadcasted_iota(jnp.int32, (rows, 128), 1)
            stats = jnp.zeros((rows, 128), F32)
            for h in range(hpg):
                stats = jnp.where(lane == h, top[h * rows:(h + 1) * rows], stats)
                stats = jnp.where(lane == hpg + h, den[h * rows:(h + 1) * rows], stats)
            return part, jnp.transpose(stats)[:2 * hpg]

        def put(src, part, stats):
            part_send[layer, src] = part
            stat_send[layer, src] = stats

        def send(src):
            part_copy(layer, src).start()
            stat_copy(layer, src).start()

        phase(f'cross{layer}')

        def turn_body(turn, carry):
            first, second = source(turn, 0), source(turn, 1)
            q_arrival(layer, second).wait_recv()
            score_of(second, scores_b, max_b)
            put(first, *values_of(scores_a, max_a))

            @pl.when(turn > 0)
            def _():
                send(first)
            after = source(lax.rem(turn + 1, chips), 0)

            @pl.when(turn < chips - 1)
            def _():
                q_arrival(layer, after).wait_recv()
            score_of(after, scores_a, max_a)
            put(second, *values_of(scores_b, max_b))
            send(second)
            return carry

        @pl.when(chip < mem_chips)
        def _():
            score_of(me, scores_a, max_a)
            lax.fori_loop(0, chips, turn_body, 0)
            part_recv[layer, me] = part_send[layer, me]
            stat_recv[layer, me] = stat_send[layer, me]
        phase(f'arrived{layer}')

        for src in range(mem_chips * CORES):
            @pl.when(src != me)
            def _():
                stat_arrival(layer, src).wait_recv()
                part_arrival(layer, src).wait_recv()

        phase(f'combine{layer}')
        factors = [None] * (mem_chips * CORES)
        for g in range(CORES):
            members = [c * CORES + g for c in range(mem_chips)]
            tops = [stat_recv[layer, i, 0:hpg] for i in members]
            dens = [stat_recv[layer, i, hpg:2 * hpg] for i in members]
            best = functools.reduce(jnp.maximum, tops)
            shares = [jnp.exp(t - best) for t in tops]
            total = functools.reduce(jnp.add, [s * d for s, d in zip(shares, dens)])
            for i, s in zip(members, shares):
                factors[i] = s / total
        packed = jnp.concatenate(factors + [jnp.zeros((128 - mem_chips * CORES * hpg, rows), F32)], axis=0)
        packed = jnp.transpose(packed)
        lane_group = lane_groups(rows, half, head_dim)
        attended = []
        for g in range(CORES):
            total = jnp.zeros((rows, half), F32)
            for c in range(mem_chips):
                i = c * CORES + g
                factor = jnp.zeros((rows, half), F32)
                for h in range(hpg):
                    factor = jnp.where(lane_group == h, packed[:, i * hpg + h:i * hpg + h + 1], factor)
                total = total + part_recv[layer, i].astype(F32) * factor
            attended.append(total.astype(BF16))
        attended = jnp.concatenate(attended, axis=-1)
        phase(f'co{layer}')
        weight_copy('cross_o', layer).wait()
        hidden = (hid[...].astype(F32) + mm(attended, w['cross_o'][layer])).astype(BF16)

        phase(f'mlp{layer}')
        normed = rms_norm(hidden, norm_mlp[layer:layer + 1, :])
        for name in ('mlp_gate', 'mlp_up', 'mlp_down'):
            weight_copy(name, layer).wait()
        update = None
        for start in range(0, w['mlp_gate'].shape[-1], FF_BLOCK):
            cols = slice(start, start + FF_BLOCK)
            gate = mm(normed, w['mlp_gate'][layer, :, cols])
            up = mm(normed, w['mlp_up'][layer, :, cols])
            act = (gate * jax.nn.sigmoid(gate) * up).astype(BF16)
            part = mm(act, w['mlp_down'][layer, cols, :])
            update = part if update is None else update + part
        hidden = (hidden.astype(F32) + update).astype(BF16)
        hid[...] = hidden

    phase('end')
    out_ref[...] = hid[...]

    @pl.when(chip < mem_chips)
    def _():
        mem_out.wait_send()
    for layer in range(n_layers):
        for d in range(1, chips):
            @pl.when(chip + d < chips)
            def _():
                x_to_chip(layer, d).wait_send()

            @pl.when(chip - d >= 0)
            def _():
                x_relayed(layer, d).wait_send()

            @pl.when(lax.rem(chip + d, chips) < mem_chips)
            def _():
                for k in range(CORES):
                    q_copy(layer, d, k).wait_send()

        @pl.when(core == 0)
        def _():
            x_to_partner(layer).wait_send()

        @pl.when(chip < mem_chips)
        def _():
            q_to_partner(layer).wait_send()
            for step in range(1, group):
                part_copy(layer, lax.rem(me + step, group)).wait_send()
                stat_copy(layer, lax.rem(me + step, group)).wait_send()
    phase(None)


def solution(mesh):
    group = mesh.shape['sp']
    row_spec = P(('dp', 'sp'), None)

    def local_step(hidden, memory, mem_len, norm_self, norm_cross, norm_mlp, self_q, self_k, self_v, self_o, cross_q, cross_k, cross_v, cross_o, mlp_gate, mlp_up, mlp_down):
        rows, width = hidden.shape
        mem_rows = memory.shape[0]
        n_layers, n_heads, head_dim = self_o.shape[:3]
        inner = n_heads * head_dim
        half = inner // CORES
        hpg = half // head_dim
        all_keys = max(group * rows, CORES * mem_rows)
        weights = dict(
            self_q=self_q, self_k=self_k, self_v=self_v, self_o=self_o.reshape(n_layers, inner, width), cross_k=cross_k, cross_v=cross_v,
            cross_q=cross_q, cross_o=cross_o.reshape(n_layers, inner, width), mlp_gate=mlp_gate, mlp_up=mlp_up, mlp_down=mlp_down)
        w_scratch = [
            pltpu.VMEM((n_layers, width, half) if name in HALVED else weights[name].shape, BF16) for name in WEIGHTS]
        dma = pltpu.SemaphoreType.DMA
        vmem = pl.BlockSpec(memory_space=pltpu.VMEM)
        hbm = pl.BlockSpec(memory_space=pl.ANY)
        return pl.pallas_call(
            functools.partial(kernel, group, n_layers, head_dim),
            out_shape=jax.ShapeDtypeStruct((rows, width), BF16),
            in_specs=[vmem, hbm, pl.BlockSpec(memory_space=pltpu.SMEM), vmem, vmem, vmem] + [hbm] * len(WEIGHTS),
            out_specs=vmem,
            scratch_shapes=w_scratch + [
                pltpu.VMEM((CORES, mem_rows, width), BF16),
                pltpu.VMEM((n_layers, group, rows, width), BF16),
                pltpu.VMEM((group, rows, width), BF16),
                pltpu.VMEM((group, rows, width), BF16),
                pltpu.VMEM((n_layers, CORES * mem_rows, half), BF16),
                pltpu.VMEM((n_layers, CORES * mem_rows, half), BF16),
                pltpu.VMEM((n_layers, CORES, rows, half), BF16),
                pltpu.VMEM((n_layers, group, rows, half), BF16),
                pltpu.VMEM((n_layers, group, rows, half), BF16),
                pltpu.VMEM((n_layers, group, rows, half), BF16),
                pltpu.VMEM((n_layers, group, 2 * hpg, rows), F32),
                pltpu.VMEM((n_layers, group, 2 * hpg, rows), F32),
                pltpu.VMEM((rows, width), BF16),
                pltpu.VMEM((hpg * rows, all_keys), F32),
                pltpu.VMEM((hpg * rows, all_keys), F32),
                pltpu.VMEM((hpg * rows, 128), F32),
                pltpu.VMEM((hpg * rows, 128), F32),
                dma((len(WEIGHTS), n_layers)),
                dma((1,)), dma((1,)), dma((1,)),
                dma((n_layers, group // CORES)), dma((n_layers, group // CORES)), dma((n_layers, group)),
                dma((n_layers, group)), dma((n_layers, group)),
                dma((n_layers, group)), dma((n_layers, group)),
                dma((n_layers, group)), dma((n_layers, group)),
            ],
            compiler_params=pltpu.CompilerParams(collective_id=0, has_side_effects=True, vmem_limit_bytes=60 * 1024 * 1024),
        )(hidden, memory, mem_len, norm_self, norm_cross, norm_mlp, *[weights[name] for name in WEIGHTS])

    return jax.shard_map(local_step, mesh=mesh, in_specs=(row_spec, row_spec, P('dp')) + (P(),) * 14, out_specs=row_spec, check_vma=False)
```

```python
import functools

import jax
import jax.numpy as jnp
from jax import lax
from jax.experimental import pallas as pl
from jax.experimental.pallas import tpu as pltpu
from jax.sharding import PartitionSpec as P

EPS = 1e-6
NEG_BIG = -1e30
CORES = 2
KEY_BLOCK = 512
FF_BLOCK = 512
MEM_BLOCK = 256
ROW_BLOCK = 64
MEM_LEN_MAX = 6144
F32 = jnp.float32
BF16 = jnp.bfloat16
MESH = pl.DeviceIdType.MESH
WEIGHTS = ('self_q', 'self_k', 'self_v', 'self_o', 'cross_k', 'cross_v', 'cross_q', 'cross_o', 'mlp_gate', 'mlp_up', 'mlp_down')
HALVED = ('cross_k', 'cross_v')


def rms_norm(hidden, gain_row):
    hidden32 = hidden.astype(F32)
    inv_rms = lax.rsqrt(jnp.mean(hidden32 * hidden32, axis=-1, keepdims=True) + EPS)
    return (hidden32 * inv_rms * gain_row.astype(F32)).astype(BF16)


def mm(a, b):
    return jnp.dot(a, b, preferred_element_type=F32)


def mm_t(a, b):
    return lax.dot_general(a, b, (((1,), (1,)), ((), ())), preferred_element_type=F32)


def lane_groups(rows, lanes, head_dim):
    return lax.broadcasted_iota(jnp.int32, (rows, lanes), 1) // head_dim


def stack_heads(q, head_dim, scale):
    rows, lanes = q.shape
    scaled = q.astype(F32) * scale
    group = lane_groups(rows, lanes, head_dim)
    return jnp.concatenate([jnp.where(group == h, scaled, 0.0).astype(BF16) for h in range(lanes // head_dim)], axis=0)


def score_steps(q_stack, key_block, n_keys, allowed, scores_ref):
    def step(start):
        scores = mm_t(q_stack, key_block(start))
        scores_ref[:, start:start + KEY_BLOCK] = jnp.where(allowed(start), scores, NEG_BIG)
    return [functools.partial(step, start) for start in range(0, n_keys, KEY_BLOCK)]


def exponent_steps(n_keys, scores_ref, weights_ref, tops, dens):
    def step(row):
        at = slice(row, row + ROW_BLOCK)
        top = jnp.max(functools.reduce(jnp.maximum, [scores_ref[at, lane:lane + 128] for lane in range(0, n_keys, 128)]), axis=-1, keepdims=True)
        run_sum = None
        for lane in range(0, n_keys, 256):
            weights = jnp.exp(scores_ref[at, lane:lane + 256] - top)
            weights_ref[at, lane:lane + 256] = weights.astype(BF16)
            pair = weights[:, :128] + weights[:, 128:]
            run_sum = pair if run_sum is None else run_sum + pair
        tops.append(top)
        dens.append(jnp.sum(run_sum, axis=-1, keepdims=True))
    return [functools.partial(step, row) for row in range(0, scores_ref.shape[0], ROW_BLOCK)]


def value_steps(value_block, n_keys, weights_ref, parts):
    def step(start):
        part = mm(weights_ref[:, start:start + KEY_BLOCK], value_block(start))
        parts[:] = [part if not parts else parts[0] + part]
    return [functools.partial(step, start) for start in range(0, n_keys, KEY_BLOCK)]


def interleave(*lists):
    order = sorted(((i + 0.5) / len(steps), n, i) for n, steps in enumerate(lists) for i in range(len(steps)))
    for _, n, i in order:
        lists[n][i]()


def unstack_heads(stacked, rows, head_dim):
    lanes = stacked.shape[1]
    group = lane_groups(rows, lanes, head_dim)
    out = stacked[:rows]
    for h in range(1, lanes // head_dim):
        out = jnp.where(group == h, stacked[h * rows:(h + 1) * rows], out)
    return out


class Phase:
    def __init__(self):
        self.cur = None

    def __call__(self, name):
        if self.cur is not None:
            self.cur.__exit__(None, None, None)
        self.cur = jax.named_scope(name) if name else None
        if self.cur is not None:
            self.cur.__enter__()


def kernel(group, n_layers, head_dim, *refs):
    n_w = len(WEIGHTS)
    hidden_ref, memory_ref, mem_len_ref, norm_self, norm_cross, norm_mlp = refs[:6]
    w_hbm = dict(zip(WEIGHTS, refs[6:6 + n_w]))
    out_ref = refs[6 + n_w]
    scratch = refs[7 + n_w:]
    w = dict(zip(WEIGHTS, scratch[:n_w]))
    (mem_v, x_all, k_all, v_all, mem_k, mem_vals, q_send, q_all, part_send, part_recv, stat_send, stat_recv, hid, scores_a, scores_b, weights_a, weights_b,
     w_sem, mem_sem, mem_send, mem_recv, x_send, x_relay, x_recv, q_ssem, q_rsem, p_ssem, p_rsem, s_ssem, s_rsem) = scratch[n_w:]

    rows, width = hidden_ref.shape
    mem_rows = memory_ref.shape[0]
    chips = group // CORES
    mem_chips = -(-MEM_LEN_MAX // (CORES * mem_rows))
    half = q_send.shape[-1]
    hpg = half // head_dim
    scale = head_dim ** -0.5
    me = lax.axis_index('sp')
    chip, core = me // CORES, me % CORES
    partner = chip * CORES + (1 - core)

    def remote(src, dst, ssem, rsem, dev):
        return pltpu.make_async_remote_copy(src_ref=src, dst_ref=dst, send_sem=ssem, recv_sem=rsem, device_id={'sp': dev}, device_id_type=MESH)

    def weight_copy(name, layer):
        src = w_hbm[name].at[layer]
        if name in HALVED:
            src = w_hbm[name].at[layer, :, pl.ds(pl.multiple_of(core * half, half), half)]
        return pltpu.make_async_copy(src, w[name].at[layer], w_sem.at[WEIGHTS.index(name), layer])

    phase = Phase()
    phase('start')
    mem_copy = pltpu.make_async_copy(memory_ref, mem_v.at[core], mem_sem.at[0])

    for name in ('self_q', 'self_k', 'self_v'):
        weight_copy(name, 0).start()
    mem_copy.start()
    for layer in range(n_layers):
        for name in HALVED:
            weight_copy(name, layer).start()
    for layer in range(n_layers):
        for name in WEIGHTS:
            if name in HALVED or (layer == 0 and name in ('self_q', 'self_k', 'self_v')):
                continue
            weight_copy(name, layer).start()

    phase('barrier')
    barrier = pltpu.get_barrier_semaphore()
    for step in range(1, group):
        pl.semaphore_signal(barrier, inc=1, device_id={'sp': lax.rem(me + step, group)}, device_id_type=MESH)
    pl.semaphore_wait(barrier, group - 1)

    def x_to_chip(layer, d):
        return remote(x_all.at[layer, me], x_all.at[layer, me], x_send.at[layer, d], x_recv.at[layer, me], me + d * CORES)

    def x_to_partner(layer):
        return remote(x_all.at[layer, me], x_all.at[layer, me], x_send.at[layer, 0], x_recv.at[layer, me], partner)

    def x_relayed(layer, d):
        src = me - d * CORES
        return remote(x_all.at[layer, src], x_all.at[layer, src], x_relay.at[layer, d], x_recv.at[layer, src], partner)

    def x_arrival(layer, src):
        return remote(x_all.at[layer, src], x_all.at[layer, src], x_send.at[layer, 0], x_recv.at[layer, src], partner)

    def q_copy(layer, d, k):
        dst = lax.rem(chip + d, chips) * CORES + k
        return remote(q_send.at[layer, k], q_all.at[layer, me], q_ssem.at[layer, d * CORES + k], q_rsem.at[layer, me], dst)

    def q_to_partner(layer):
        return remote(q_send.at[layer, 1 - core], q_all.at[layer, me], q_ssem.at[layer, 0], q_rsem.at[layer, me], partner)

    def q_arrival(layer, src):
        return remote(q_send.at[layer, 0], q_all.at[layer, src], q_ssem.at[layer, 0], q_rsem.at[layer, src], partner)

    def part_copy(layer, src):
        return remote(part_send.at[layer, src], part_recv.at[layer, me], p_ssem.at[layer, src], p_rsem.at[layer, me], src)

    def stat_copy(layer, src):
        return remote(stat_send.at[layer, src], stat_recv.at[layer, me], s_ssem.at[layer, src], s_rsem.at[layer, me], src)

    def part_arrival(layer, src):
        return remote(part_send.at[layer, src], part_recv.at[layer, src], p_ssem.at[layer, src], p_rsem.at[layer, src], partner)

    def stat_arrival(layer, src):
        return remote(stat_send.at[layer, src], stat_recv.at[layer, src], s_ssem.at[layer, src], s_rsem.at[layer, src], partner)

    mem_out = remote(mem_v.at[core], mem_v.at[core], mem_send.at[0], mem_recv.at[0], partner)
    mem_in = remote(mem_v.at[1 - core], mem_v.at[1 - core], mem_send.at[0], mem_recv.at[0], partner)

    def project_memory(slot):
        def body(i, carry):
            at = pl.ds(pl.multiple_of(i * MEM_BLOCK, MEM_BLOCK), MEM_BLOCK)
            to = pl.ds(pl.multiple_of(slot * mem_rows + i * MEM_BLOCK, MEM_BLOCK), MEM_BLOCK)
            block = mem_v[slot, at, :]
            for layer in range(n_layers):
                mem_k[layer, to, :] = mm(block, w['cross_k'][layer]).astype(BF16)
                mem_vals[layer, to, :] = mm(block, w['cross_v'][layer]).astype(BF16)
            return carry
        lax.fori_loop(0, mem_rows // MEM_BLOCK, body, 0)

    phase('zero')
    hid[...] = hidden_ref[...]
    for src in range(group):
        @pl.when(src > me)
        def _():
            k_all[src] = jnp.zeros((rows, width), BF16)
            v_all[src] = jnp.zeros((rows, width), BF16)

    for layer in range(n_layers):
        phase(f'xnorm{layer}')
        x_all[layer, me] = rms_norm(hid[...], norm_self[layer:layer + 1, :])
        for d in (2, 1, 3):
            if d < chips:
                @pl.when(chip + d < chips)
                def _():
                    x_to_chip(layer, d).start()

        @pl.when(core == 0)
        def _():
            x_to_partner(layer).start()

        if layer == 0:
            for name in ('self_q', 'self_k', 'self_v'):
                weight_copy(name, layer).wait()
        else:
            for name in ('self_q', 'self_k', 'self_v'):
                weight_copy(name, layer).wait()

        def project_rows(src):
            block = x_all[layer, src]
            k_all[src] = mm(block, w['self_k'][layer]).astype(BF16)
            v_all[src] = mm(block, w['self_v'][layer]).astype(BF16)

        phase(f'ownproj{layer}')
        project_rows(me)
        queries = mm(x_all[layer, me], w['self_q'][layer]).astype(BF16)

        phase(f'memproj{layer}')
        if layer == 0:
            mem_copy.wait()
            for other in range(n_layers):
                for name in HALVED:
                    weight_copy(name, other).wait()

            @pl.when(chip < mem_chips)
            def _():
                mem_out.start()
                project_memory(core)
        phase(f'xwait{layer}')

        for d in range(1, chips):
            @pl.when(chip - d >= 0)
            def _():
                x_arrival(layer, me - d * CORES).wait_recv()
                x_relayed(layer, d).start()
                project_rows(me - d * CORES)

        @pl.when(core == 1)
        def _():
            x_arrival(layer, partner).wait_recv()
            project_rows(partner)

        for d in range(1, chips):
            @pl.when(chip - d >= 0)
            def _():
                x_arrival(layer, partner - d * CORES).wait_recv()
                project_rows(partner - d * CORES)

        phase(f'memproj2{layer}')
        if layer == 0:
            @pl.when(chip < mem_chips)
            def _():
                mem_in.wait_recv()
                project_memory(1 - core)

        phase(f'selfatt{layer}')
        all_rows = group * rows
        query_at = me * rows + lax.rem(lax.broadcasted_iota(jnp.int32, (hpg * rows, KEY_BLOCK), 0), rows)
        key_at = lax.broadcasted_iota(jnp.int32, (hpg * rows, KEY_BLOCK), 1)
        per_block = KEY_BLOCK // rows
        stores = ((scores_a, weights_a), (scores_b, weights_b))
        tops, dens, parts = [[], []], [[], []], [[], []]

        def self_steps(g):
            lanes = slice(g * half, (g + 1) * half)
            s_ref, w_ref = stores[g]
            return (
                score_steps(stack_heads(queries[:, lanes], head_dim, scale),
                            lambda start: k_all[start // rows:start // rows + per_block, :, lanes].reshape(KEY_BLOCK, half),
                            all_rows, lambda start: key_at + start <= query_at, s_ref),
                exponent_steps(all_rows, s_ref, w_ref, tops[g], dens[g]),
                value_steps(lambda start: v_all[start // rows:start // rows + per_block, :, lanes].reshape(KEY_BLOCK, half),
                            all_rows, w_ref, parts[g]))

        steps = [self_steps(g) for g in range(CORES)]
        interleave(steps[0][0])
        interleave(steps[0][1], steps[1][0])
        interleave(steps[0][2], steps[1][1])
        interleave(steps[1][2])
        attended = [unstack_heads(parts[g][0] / jnp.concatenate(dens[g], axis=0), rows, head_dim).astype(BF16) for g in range(CORES)]
        attended = jnp.concatenate(attended, axis=-1)
        phase(f'oproj{layer}')
        weight_copy('self_o', layer).wait()
        hidden = (hid[...].astype(F32) + mm(attended, w['self_o'][layer])).astype(BF16)
        hid[...] = hidden

        phase(f'qproj{layer}')
        weight_copy('cross_q', layer).wait()
        queries = mm(rms_norm(hidden, norm_cross[layer:layer + 1, :]), w['cross_q'][layer]).astype(BF16)
        for g in range(CORES):
            q_send[layer, g] = queries[:, g * half:(g + 1) * half]
        q_order = [(d, k) for d in (1, 3, 2) if d < chips for k in range(CORES)]

        @pl.when(chip < mem_chips)
        def _():
            q_to_partner(layer).start()
        for d, k in q_order:
            @pl.when(lax.rem(chip + d, chips) < mem_chips)
            def _():
                q_copy(layer, d, k).start()
        q_all[layer, me] = q_send[layer, core]

        mem_at = chip * (CORES * mem_rows) + lax.broadcasted_iota(jnp.int32, (1, KEY_BLOCK), 1)
        n_keys = CORES * mem_rows

        def wait_queries(src):
            @pl.when(src != me)
            def _():
                q_arrival(layer, src).wait_recv()

        def score_of(src, scores_ref):
            return score_steps(stack_heads(q_all[layer, src], head_dim, scale), lambda start: mem_k[layer, start:start + KEY_BLOCK, :], n_keys,
                               lambda start: mem_at + start < mem_len_ref[0], scores_ref)

        def put_stats(src, tops, dens):
            top, den = jnp.concatenate(tops, axis=0), jnp.concatenate(dens, axis=0)
            lane = lax.broadcasted_iota(jnp.int32, (rows, 128), 1)
            stats = jnp.zeros((rows, 128), F32)
            for h in range(hpg):
                stats = jnp.where(lane == h, top[h * rows:(h + 1) * rows], stats)
                stats = jnp.where(lane == hpg + h, den[h * rows:(h + 1) * rows], stats)
            stat_send[layer, src] = jnp.transpose(stats)[:2 * hpg]

        def values_of(weights_ref, parts):
            return value_steps(lambda start: mem_vals[layer, start:start + KEY_BLOCK, :], n_keys, weights_ref, parts)

        def put_part(src, parts):
            part_send[layer, src] = unstack_heads(parts[0], rows, head_dim).astype(BF16)

        def stages(after, s_after, now, s_now, w_now, before, w_before):
            tops, dens, parts = [], [], []
            interleave(score_of(after, s_after), exponent_steps(n_keys, s_now, w_now, tops, dens), values_of(w_before, parts))
            put_stats(now, tops, dens)
            put_part(before, parts)

        def send(src, copy):
            @pl.when(src != me)
            def _():
                copy(layer, src).start()

        phase(f'cross{layer}')

        def turn_body(turn, carry):
            first = turn * 2
            second, before, after = first + 1, lax.rem(first + group - 1, group), jnp.minimum(first + 2, group - 1)
            wait_queries(second)
            stages(second, scores_b, first, scores_a, weights_a, before, weights_b)
            send(first, stat_copy)

            @pl.when(turn > 0)
            def _():
                send(before, part_copy)

            @pl.when(turn < group // 2 - 1)
            def _():
                wait_queries(first + 2)
            stages(after, scores_a, second, scores_b, weights_b, first, weights_a)
            send(second, stat_copy)
            send(first, part_copy)
            return carry

        @pl.when(chip < mem_chips)
        def _():
            wait_queries(0)
            interleave(score_of(0, scores_a))
            lax.fori_loop(0, group // 2, turn_body, 0)
            parts = []
            interleave(values_of(weights_b, parts))
            put_part(group - 1, parts)
            send(group - 1, part_copy)
            part_recv[layer, me] = part_send[layer, me]
            stat_recv[layer, me] = stat_send[layer, me]
        phase(f'arrived{layer}')

        for src in range(mem_chips * CORES):
            @pl.when(src != me)
            def _():
                stat_arrival(layer, src).wait_recv()
                part_arrival(layer, src).wait_recv()

        phase(f'combine{layer}')
        factors = [None] * (mem_chips * CORES)
        for g in range(CORES):
            members = [c * CORES + g for c in range(mem_chips)]
            tops = [stat_recv[layer, i, 0:hpg] for i in members]
            dens = [stat_recv[layer, i, hpg:2 * hpg] for i in members]
            best = functools.reduce(jnp.maximum, tops)
            shares = [jnp.exp(t - best) for t in tops]
            total = functools.reduce(jnp.add, [s * d for s, d in zip(shares, dens)])
            for i, s in zip(members, shares):
                factors[i] = s / total
        packed = jnp.concatenate(factors + [jnp.zeros((128 - mem_chips * CORES * hpg, rows), F32)], axis=0)
        packed = jnp.transpose(packed)
        lane_group = lane_groups(rows, half, head_dim)
        attended = []
        for g in range(CORES):
            total = jnp.zeros((rows, half), F32)
            for c in range(mem_chips):
                i = c * CORES + g
                factor = jnp.zeros((rows, half), F32)
                for h in range(hpg):
                    factor = jnp.where(lane_group == h, packed[:, i * hpg + h:i * hpg + h + 1], factor)
                total = total + part_recv[layer, i].astype(F32) * factor
            attended.append(total.astype(BF16))
        attended = jnp.concatenate(attended, axis=-1)
        phase(f'co{layer}')
        weight_copy('cross_o', layer).wait()
        hidden = (hid[...].astype(F32) + mm(attended, w['cross_o'][layer])).astype(BF16)

        phase(f'mlp{layer}')
        normed = rms_norm(hidden, norm_mlp[layer:layer + 1, :])
        for name in ('mlp_gate', 'mlp_up', 'mlp_down'):
            weight_copy(name, layer).wait()
        update = None
        for start in range(0, w['mlp_gate'].shape[-1], FF_BLOCK):
            cols = slice(start, start + FF_BLOCK)
            gate = mm(normed, w['mlp_gate'][layer, :, cols])
            up = mm(normed, w['mlp_up'][layer, :, cols])
            act = (gate * jax.nn.sigmoid(gate) * up).astype(BF16)
            part = mm(act, w['mlp_down'][layer, cols, :])
            update = part if update is None else update + part
        hidden = (hidden.astype(F32) + update).astype(BF16)
        hid[...] = hidden

    phase('end')
    out_ref[...] = hid[...]

    @pl.when(chip < mem_chips)
    def _():
        mem_out.wait_send()
    for layer in range(n_layers):
        for d in range(1, chips):
            @pl.when(chip + d < chips)
            def _():
                x_to_chip(layer, d).wait_send()

            @pl.when(chip - d >= 0)
            def _():
                x_relayed(layer, d).wait_send()

            @pl.when(lax.rem(chip + d, chips) < mem_chips)
            def _():
                for k in range(CORES):
                    q_copy(layer, d, k).wait_send()

        @pl.when(core == 0)
        def _():
            x_to_partner(layer).wait_send()

        @pl.when(chip < mem_chips)
        def _():
            q_to_partner(layer).wait_send()
            for step in range(1, group):
                part_copy(layer, lax.rem(me + step, group)).wait_send()
                stat_copy(layer, lax.rem(me + step, group)).wait_send()
    phase(None)


def solution(mesh):
    group = mesh.shape['sp']
    row_spec = P(('dp', 'sp'), None)

    def local_step(hidden, memory, mem_len, norm_self, norm_cross, norm_mlp, self_q, self_k, self_v, self_o, cross_q, cross_k, cross_v, cross_o, mlp_gate, mlp_up, mlp_down):
        rows, width = hidden.shape
        mem_rows = memory.shape[0]
        n_layers, n_heads, head_dim = self_o.shape[:3]
        inner = n_heads * head_dim
        half = inner // CORES
        hpg = half // head_dim
        all_keys = max(group * rows, CORES * mem_rows)
        weights = dict(
            self_q=self_q, self_k=self_k, self_v=self_v, self_o=self_o.reshape(n_layers, inner, width), cross_k=cross_k, cross_v=cross_v,
            cross_q=cross_q, cross_o=cross_o.reshape(n_layers, inner, width), mlp_gate=mlp_gate, mlp_up=mlp_up, mlp_down=mlp_down)
        w_scratch = [
            pltpu.VMEM((n_layers, width, half) if name in HALVED else weights[name].shape, BF16) for name in WEIGHTS]
        dma = pltpu.SemaphoreType.DMA
        vmem = pl.BlockSpec(memory_space=pltpu.VMEM)
        hbm = pl.BlockSpec(memory_space=pl.ANY)
        return pl.pallas_call(
            functools.partial(kernel, group, n_layers, head_dim),
            out_shape=jax.ShapeDtypeStruct((rows, width), BF16),
            in_specs=[vmem, hbm, pl.BlockSpec(memory_space=pltpu.SMEM), vmem, vmem, vmem] + [hbm] * len(WEIGHTS),
            out_specs=vmem,
            scratch_shapes=w_scratch + [
                pltpu.VMEM((CORES, mem_rows, width), BF16),
                pltpu.VMEM((n_layers, group, rows, width), BF16),
                pltpu.VMEM((group, rows, width), BF16),
                pltpu.VMEM((group, rows, width), BF16),
                pltpu.VMEM((n_layers, CORES * mem_rows, half), BF16),
                pltpu.VMEM((n_layers, CORES * mem_rows, half), BF16),
                pltpu.VMEM((n_layers, CORES, rows, half), BF16),
                pltpu.VMEM((n_layers, group, rows, half), BF16),
                pltpu.VMEM((n_layers, group, rows, half), BF16),
                pltpu.VMEM((n_layers, group, rows, half), BF16),
                pltpu.VMEM((n_layers, group, 2 * hpg, rows), F32),
                pltpu.VMEM((n_layers, group, 2 * hpg, rows), F32),
                pltpu.VMEM((rows, width), BF16),
                pltpu.VMEM((hpg * rows, all_keys), F32),
                pltpu.VMEM((hpg * rows, all_keys), F32),
                pltpu.VMEM((hpg * rows, all_keys), BF16),
                pltpu.VMEM((hpg * rows, all_keys), BF16),
                dma((len(WEIGHTS), n_layers)),
                dma((1,)), dma((1,)), dma((1,)),
                dma((n_layers, group // CORES)), dma((n_layers, group // CORES)), dma((n_layers, group)),
                dma((n_layers, group)), dma((n_layers, group)),
                dma((n_layers, group)), dma((n_layers, group)),
                dma((n_layers, group)), dma((n_layers, group)),
            ],
            compiler_params=pltpu.CompilerParams(collective_id=0, has_side_effects=True, vmem_limit_bytes=60 * 1024 * 1024),
        )(hidden, memory, mem_len, norm_self, norm_cross, norm_mlp, *[weights[name] for name in WEIGHTS])

    return jax.shard_map(local_step, mesh=mesh, in_specs=(row_spec, row_spec, P('dp')) + (P(),) * 14, out_specs=row_spec, check_vma=False)
```

```python
import functools

import jax
import jax.numpy as jnp
from jax import lax
from jax.experimental import pallas as pl
from jax.experimental.pallas import tpu as pltpu
from jax.sharding import PartitionSpec as P

EPS = 1e-6
NEG_BIG = -1e30
CORES = 2
KEY_BLOCK = 512
FF_BLOCK = 512
MEM_BLOCK = 256
ROW_BLOCK = 64
LAG = 1
LOWEST = -3.4e38
MEM_LEN_MAX = 6144
F32 = jnp.float32
BF16 = jnp.bfloat16
MESH = pl.DeviceIdType.MESH
WEIGHTS = ('self_q', 'self_k', 'self_v', 'self_o', 'cross_k', 'cross_v', 'cross_q', 'cross_o', 'mlp_gate', 'mlp_up', 'mlp_down')
HALVED = ('cross_k', 'cross_v')


def rms_norm(hidden, gain_row):
    hidden32 = hidden.astype(F32)
    inv_rms = lax.rsqrt(jnp.mean(hidden32 * hidden32, axis=-1, keepdims=True) + EPS)
    return (hidden32 * inv_rms * gain_row.astype(F32)).astype(BF16)


def mm(a, b):
    return jnp.dot(a, b, preferred_element_type=F32)


def mm_t(a, b):
    return lax.dot_general(a, b, (((1,), (1,)), ((), ())), preferred_element_type=F32)


def lane_groups(rows, lanes, head_dim):
    return lax.broadcasted_iota(jnp.int32, (rows, lanes), 1) // head_dim


def stack_heads(q, head_dim, scale):
    rows, lanes = q.shape
    scaled = q.astype(F32) * scale
    group = lane_groups(rows, lanes, head_dim)
    return jnp.concatenate([jnp.where(group == h, scaled, 0.0).astype(BF16) for h in range(lanes // head_dim)], axis=0)


def score_steps(q_stack, key_block, n_keys, allowed, scores_ref):
    def step(start):
        scores = mm_t(q_stack, key_block(start))
        scores_ref[:, start:start + KEY_BLOCK] = jnp.where(allowed(start), scores, NEG_BIG)
    return [functools.partial(step, start) for start in range(0, n_keys, KEY_BLOCK)]


def exponent_steps(n_keys, scores_ref, weights_ref, tops, dens, lag=0):
    sums = []

    def step(row):
        at = slice(row, row + ROW_BLOCK)
        tiles = [scores_ref[at, lane:lane + 128] for lane in range(0, n_keys, 128)]
        if lag and len(sums) >= lag:
            tiles.insert(0, jnp.minimum(sums[-lag], LOWEST))
        top = jnp.max(functools.reduce(jnp.maximum, tiles), axis=-1, keepdims=True)
        run_sum = None
        for lane in range(0, n_keys, 256):
            weights = jnp.exp(scores_ref[at, lane:lane + 256] - top)
            weights_ref[at, lane:lane + 256] = weights.astype(BF16)
            pair = weights[:, :128] + weights[:, 128:]
            run_sum = pair if run_sum is None else run_sum + pair
        sums.append(run_sum)
        tops.append(top)
        dens.append(jnp.sum(run_sum, axis=-1, keepdims=True))
    return [functools.partial(step, row) for row in range(0, scores_ref.shape[0], ROW_BLOCK)]


def value_steps(value_block, n_keys, weights_ref, parts):
    def step(start):
        part = mm(weights_ref[:, start:start + KEY_BLOCK], value_block(start))
        parts[:] = [part if not parts else parts[0] + part]
    return [functools.partial(step, start) for start in range(0, n_keys, KEY_BLOCK)]


def interleave(*lists):
    order = sorted(((i + 0.5) / len(steps), n, i) for n, steps in enumerate(lists) for i in range(len(steps)))
    for _, n, i in order:
        lists[n][i]()


def unstack_heads(stacked, rows, head_dim):
    lanes = stacked.shape[1]
    group = lane_groups(rows, lanes, head_dim)
    out = stacked[:rows]
    for h in range(1, lanes // head_dim):
        out = jnp.where(group == h, stacked[h * rows:(h + 1) * rows], out)
    return out


class Phase:
    def __init__(self):
        self.cur = None

    def __call__(self, name):
        if self.cur is not None:
            self.cur.__exit__(None, None, None)
        self.cur = jax.named_scope(name) if name else None
        if self.cur is not None:
            self.cur.__enter__()


def kernel(group, n_layers, head_dim, *refs):
    n_w = len(WEIGHTS)
    hidden_ref, memory_ref, mem_len_ref, norm_self, norm_cross, norm_mlp = refs[:6]
    w_hbm = dict(zip(WEIGHTS, refs[6:6 + n_w]))
    out_ref = refs[6 + n_w]
    scratch = refs[7 + n_w:]
    w = dict(zip(WEIGHTS, scratch[:n_w]))
    (mem_v, x_all, k_all, v_all, mem_k, mem_vals, q_send, q_all, part_send, part_recv, stat_send, stat_recv, hid, scores_a, scores_b, weights_a, weights_b,
     w_sem, mem_sem, mem_send, mem_recv, x_send, x_relay, x_recv, q_ssem, q_rsem, p_ssem, p_rsem, s_ssem, s_rsem) = scratch[n_w:]

    rows, width = hidden_ref.shape
    mem_rows = memory_ref.shape[0]
    chips = group // CORES
    mem_chips = -(-MEM_LEN_MAX // (CORES * mem_rows))
    half = q_send.shape[-1]
    hpg = half // head_dim
    scale = head_dim ** -0.5
    me = lax.axis_index('sp')
    chip, core = me // CORES, me % CORES
    partner = chip * CORES + (1 - core)

    def remote(src, dst, ssem, rsem, dev):
        return pltpu.make_async_remote_copy(src_ref=src, dst_ref=dst, send_sem=ssem, recv_sem=rsem, device_id={'sp': dev}, device_id_type=MESH)

    def weight_copy(name, layer):
        src = w_hbm[name].at[layer]
        if name in HALVED:
            src = w_hbm[name].at[layer, :, pl.ds(pl.multiple_of(core * half, half), half)]
        return pltpu.make_async_copy(src, w[name].at[layer], w_sem.at[WEIGHTS.index(name), layer])

    phase = Phase()
    phase('start')
    mem_copy = pltpu.make_async_copy(memory_ref, mem_v.at[core], mem_sem.at[0])

    for name in ('self_q', 'self_k', 'self_v'):
        weight_copy(name, 0).start()
    mem_copy.start()
    for layer in range(n_layers):
        for name in HALVED:
            weight_copy(name, layer).start()
    for layer in range(n_layers):
        for name in WEIGHTS:
            if name in HALVED or (layer == 0 and name in ('self_q', 'self_k', 'self_v')):
                continue
            weight_copy(name, layer).start()

    phase('barrier')
    barrier = pltpu.get_barrier_semaphore()
    for step in range(1, group):
        pl.semaphore_signal(barrier, inc=1, device_id={'sp': lax.rem(me + step, group)}, device_id_type=MESH)
    pl.semaphore_wait(barrier, group - 1)

    top_chip = chip // (chips - 1)
    half_rows = rows // 2

    def x_copy(layer, src, part, ssem, dst):
        at = x_all.at[layer, src, pl.ds(pl.multiple_of(part * half_rows, half_rows), half_rows)]
        return remote(at, at, ssem, x_recv.at[layer, src, part], dst)

    def x_sends(layer):
        up = me + CORES
        across = (chips - 1) * CORES + core
        send = x_send.at
        return [
            (chip == 1, x_copy(layer, me, 1, send[layer, 2], core)),
            (chip < chips - 1, x_copy(layer, me, 0, send[layer, 0], up)),
            (chip == 0, x_copy(layer, me, 1, send[layer, 2], across)),
            (chip < chips - 1, x_copy(layer, me, 1, send[layer, 1], up)),
            (chip == 0, x_copy(layer, me, 0, send[layer, 3], across)),
            (core == 0, x_copy(layer, me, 0, send[layer, 4], partner)),
            (core == 0, x_copy(layer, me, 1, send[layer, 5], partner)),
        ]

    def x_source(turn):
        return top_chip * (turn * 2 - 3 * (turn // 2)) + (1 - top_chip) * (chip - 1 - turn)

    def x_forward(layer):
        src = x_source(0) * CORES + core
        return x_copy(layer, src, top_chip, x_send.at[layer, 6], me + CORES - 2 * CORES * top_chip)

    def x_forward_first(layer):
        return x_copy(layer, CORES + core, 1, x_send.at[layer, 6], (chips - 1) * CORES + core)

    def x_relay_copy(layer, turn, part):
        return x_copy(layer, x_source(turn) * CORES + core, part, x_relay.at[layer, turn, part], partner)

    def x_arrival(layer, src, part):
        return x_copy(layer, src, part, x_send.at[layer, 0], partner)

    def q_copy(layer, d, k):
        dst = lax.rem(chip + d, chips) * CORES + k
        return remote(q_send.at[layer, k], q_all.at[layer, me], q_ssem.at[layer, d * CORES + k], q_rsem.at[layer, me], dst)

    def q_to_partner(layer):
        return remote(q_send.at[layer, 1 - core], q_all.at[layer, me], q_ssem.at[layer, 0], q_rsem.at[layer, me], partner)

    def q_arrival(layer, src):
        return remote(q_send.at[layer, 0], q_all.at[layer, src], q_ssem.at[layer, 0], q_rsem.at[layer, src], partner)

    def part_copy(layer, src):
        return remote(part_send.at[layer, src], part_recv.at[layer, me], p_ssem.at[layer, src], p_rsem.at[layer, me], src)

    def stat_copy(layer, src):
        return remote(stat_send.at[layer, src], stat_recv.at[layer, me], s_ssem.at[layer, src], s_rsem.at[layer, me], src)

    def part_arrival(layer, src):
        return remote(part_send.at[layer, src], part_recv.at[layer, src], p_ssem.at[layer, src], p_rsem.at[layer, src], partner)

    def stat_arrival(layer, src):
        return remote(stat_send.at[layer, src], stat_recv.at[layer, src], s_ssem.at[layer, src], s_rsem.at[layer, src], partner)

    mem_out = remote(mem_v.at[core], mem_v.at[core], mem_send.at[0], mem_recv.at[0], partner)
    mem_in = remote(mem_v.at[1 - core], mem_v.at[1 - core], mem_send.at[0], mem_recv.at[0], partner)

    def project_memory(slot, layer):
        def body(i, carry):
            at = pl.ds(pl.multiple_of(i * MEM_BLOCK, MEM_BLOCK), MEM_BLOCK)
            to = pl.ds(pl.multiple_of(slot * mem_rows + i * MEM_BLOCK, MEM_BLOCK), MEM_BLOCK)
            block = mem_v[slot, at, :]
            mem_k[layer, to, :] = mm(block, w['cross_k'][layer]).astype(BF16)
            mem_vals[layer, to, :] = mm(block, w['cross_v'][layer]).astype(BF16)
            return carry
        lax.fori_loop(0, mem_rows // MEM_BLOCK, body, 0)

    phase('zero')
    hid[...] = hidden_ref[...]
    for src in range(group):
        @pl.when(src > me)
        def _():
            k_all[src] = jnp.zeros((rows, width), BF16)
            v_all[src] = jnp.zeros((rows, width), BF16)

    for layer in range(n_layers):
        phase(f'xnorm{layer}')
        x_all[layer, me] = rms_norm(hid[...], norm_self[layer:layer + 1, :])
        for condition, copy in x_sends(layer):
            pl.when(condition)(copy.start)

        for name in ('self_q', 'self_k', 'self_v'):
            weight_copy(name, layer).wait()

        def project_rows(src):
            block = x_all[layer, src]
            k_all[src] = mm(block, w['self_k'][layer]).astype(BF16)
            v_all[src] = mm(block, w['self_v'][layer]).astype(BF16)

        phase(f'ownproj{layer}')
        project_rows(me)
        queries = mm(x_all[layer, me], w['self_q'][layer]).astype(BF16)

        phase(f'memproj{layer}')
        if layer == 0:
            mem_copy.wait()
            for other in range(n_layers):
                for name in HALVED:
                    weight_copy(name, other).wait()

            @pl.when(chip < mem_chips)
            def _():
                mem_out.start()
                for other in range(n_layers):
                    project_memory(core, other)
        phase(f'xwait{layer}')

        @pl.when(chip == 0)
        def _():
            x_arrival(layer, CORES + core, 1).wait_recv()
            x_forward_first(layer).start()

        for turn in range(chips - 1):
            @pl.when(turn < chip)
            def _():
                src = x_source(turn) * CORES + core
                first = top_chip if turn == 0 else 0
                for i, part in enumerate((first, 1 - first)):
                    x_arrival(layer, src, part).wait_recv()
                    if turn == 0 and i == 0:
                        pl.when(chip > 0)(x_forward(layer).start)
                    x_relay_copy(layer, turn, part).start()
                project_rows(src)

        phase(f'memproj2{layer}')

        @pl.when(chip < mem_chips)
        def _():
            if layer == 0:
                mem_in.wait_recv()
            project_memory(1 - core, layer)

        phase(f'xwait2{layer}')
        @pl.when(core == 1)
        def _():
            for part in (0, 1):
                x_arrival(layer, partner, part).wait_recv()
            project_rows(partner)

        for turn in range(chips - 1):
            @pl.when(turn < chip)
            def _():
                src = x_source(turn) * CORES + (1 - core)
                for part in (0, 1):
                    x_arrival(layer, src, part).wait_recv()
                project_rows(src)

        phase(f'selfatt{layer}')
        all_rows = group * rows
        query_at = me * rows + lax.rem(lax.broadcasted_iota(jnp.int32, (hpg * rows, KEY_BLOCK), 0), rows)
        key_at = lax.broadcasted_iota(jnp.int32, (hpg * rows, KEY_BLOCK), 1)
        per_block = KEY_BLOCK // rows
        stores = ((scores_a, weights_a), (scores_b, weights_b))
        tops, dens, parts = [[], []], [[], []], [[], []]

        def self_steps(g):
            lanes = slice(g * half, (g + 1) * half)
            s_ref, w_ref = stores[g]
            return (
                score_steps(stack_heads(queries[:, lanes], head_dim, scale),
                            lambda start: k_all[start // rows:start // rows + per_block, :, lanes].reshape(KEY_BLOCK, half),
                            all_rows, lambda start: key_at + start <= query_at, s_ref),
                exponent_steps(all_rows, s_ref, w_ref, tops[g], dens[g]),
                value_steps(lambda start: v_all[start // rows:start // rows + per_block, :, lanes].reshape(KEY_BLOCK, half),
                            all_rows, w_ref, parts[g]))

        steps = [self_steps(g) for g in range(CORES)]
        interleave(steps[0][0])
        interleave(steps[0][1], steps[1][0])
        interleave(steps[0][2], steps[1][1])
        interleave(steps[1][2])
        attended = [unstack_heads(parts[g][0] / jnp.concatenate(dens[g], axis=0), rows, head_dim).astype(BF16) for g in range(CORES)]
        attended = jnp.concatenate(attended, axis=-1)
        phase(f'oproj{layer}')
        weight_copy('self_o', layer).wait()
        hidden = (hid[...].astype(F32) + mm(attended, w['self_o'][layer])).astype(BF16)
        hid[...] = hidden

        phase(f'qproj{layer}')
        weight_copy('cross_q', layer).wait()
        queries = mm(rms_norm(hidden, norm_cross[layer:layer + 1, :]), w['cross_q'][layer]).astype(BF16)
        for g in range(CORES):
            q_send[layer, g] = queries[:, g * half:(g + 1) * half]
        q_order = [(d, k) for d in (1, 3, 2) if d < chips for k in range(CORES)]

        @pl.when(chip < mem_chips)
        def _():
            q_to_partner(layer).start()
        for d, k in q_order:
            @pl.when(lax.rem(chip + d, chips) < mem_chips)
            def _():
                q_copy(layer, d, k).start()
        q_all[layer, me] = q_send[layer, core]

        mem_at = chip * (CORES * mem_rows) + lax.broadcasted_iota(jnp.int32, (1, KEY_BLOCK), 1)
        n_keys = CORES * mem_rows

        def wait_queries(src):
            @pl.when(src != me)
            def _():
                q_arrival(layer, src).wait_recv()

        def score_of(src, scores_ref):
            return score_steps(stack_heads(q_all[layer, src], head_dim, scale), lambda start: mem_k[layer, start:start + KEY_BLOCK, :], n_keys,
                               lambda start: mem_at + start < mem_len_ref[0], scores_ref)

        def put_stats(src, tops, dens):
            top, den = jnp.concatenate(tops, axis=0), jnp.concatenate(dens, axis=0)
            lane = lax.broadcasted_iota(jnp.int32, (rows, 128), 1)
            stats = jnp.zeros((rows, 128), F32)
            for h in range(hpg):
                stats = jnp.where(lane == h, top[h * rows:(h + 1) * rows], stats)
                stats = jnp.where(lane == hpg + h, den[h * rows:(h + 1) * rows], stats)
            stat_send[layer, src] = jnp.transpose(stats)[:2 * hpg]

        def values_of(weights_ref, parts):
            return value_steps(lambda start: mem_vals[layer, start:start + KEY_BLOCK, :], n_keys, weights_ref, parts)

        def put_part(src, parts):
            part_send[layer, src] = unstack_heads(parts[0], rows, head_dim).astype(BF16)

        def stages(after, s_after, now, s_now, w_now, before, w_before):
            tops, dens, parts = [], [], []
            interleave(score_of(after, s_after), exponent_steps(n_keys, s_now, w_now, tops, dens, LAG), values_of(w_before, parts))
            put_stats(now, tops, dens)
            put_part(before, parts)

        def send(src, copy):
            @pl.when(src != me)
            def _():
                copy(layer, src).start()

        phase(f'cross{layer}')

        def turn_body(turn, carry):
            first = turn * 2
            second, before, after = first + 1, lax.rem(first + group - 1, group), jnp.minimum(first + 2, group - 1)
            wait_queries(second)
            stages(second, scores_b, first, scores_a, weights_a, before, weights_b)
            send(first, stat_copy)

            @pl.when(turn > 0)
            def _():
                send(before, part_copy)

            @pl.when(turn < group // 2 - 1)
            def _():
                wait_queries(first + 2)
            stages(after, scores_a, second, scores_b, weights_b, first, weights_a)
            send(second, stat_copy)
            send(first, part_copy)
            return carry

        @pl.when(chip < mem_chips)
        def _():
            wait_queries(0)
            interleave(score_of(0, scores_a))
            lax.fori_loop(0, group // 2, turn_body, 0)
            parts = []
            interleave(values_of(weights_b, parts))
            put_part(group - 1, parts)
            send(group - 1, part_copy)
            part_recv[layer, me] = part_send[layer, me]
            stat_recv[layer, me] = stat_send[layer, me]
        phase(f'arrived{layer}')

        for src in range(mem_chips * CORES):
            @pl.when(src != me)
            def _():
                stat_arrival(layer, src).wait_recv()
                part_arrival(layer, src).wait_recv()

        phase(f'combine{layer}')
        factors = [None] * (mem_chips * CORES)
        for g in range(CORES):
            members = [c * CORES + g for c in range(mem_chips)]
            tops = [stat_recv[layer, i, 0:hpg] for i in members]
            dens = [stat_recv[layer, i, hpg:2 * hpg] for i in members]
            best = functools.reduce(jnp.maximum, tops)
            shares = [jnp.exp(t - best) for t in tops]
            total = functools.reduce(jnp.add, [s * d for s, d in zip(shares, dens)])
            for i, s in zip(members, shares):
                factors[i] = s / total
        packed = jnp.concatenate(factors + [jnp.zeros((128 - mem_chips * CORES * hpg, rows), F32)], axis=0)
        packed = jnp.transpose(packed)
        lane_group = lane_groups(rows, half, head_dim)
        attended = []
        for g in range(CORES):
            total = jnp.zeros((rows, half), F32)
            for c in range(mem_chips):
                i = c * CORES + g
                factor = jnp.zeros((rows, half), F32)
                for h in range(hpg):
                    factor = jnp.where(lane_group == h, packed[:, i * hpg + h:i * hpg + h + 1], factor)
                total = total + part_recv[layer, i].astype(F32) * factor
            attended.append(total.astype(BF16))
        attended = jnp.concatenate(attended, axis=-1)
        phase(f'co{layer}')
        weight_copy('cross_o', layer).wait()
        hidden = (hid[...].astype(F32) + mm(attended, w['cross_o'][layer])).astype(BF16)

        phase(f'mlp{layer}')
        normed = rms_norm(hidden, norm_mlp[layer:layer + 1, :])
        for name in ('mlp_gate', 'mlp_up', 'mlp_down'):
            weight_copy(name, layer).wait()
        update = None
        for start in range(0, w['mlp_gate'].shape[-1], FF_BLOCK):
            cols = slice(start, start + FF_BLOCK)
            gate = mm(normed, w['mlp_gate'][layer, :, cols])
            up = mm(normed, w['mlp_up'][layer, :, cols])
            act = (gate * jax.nn.sigmoid(gate) * up).astype(BF16)
            part = mm(act, w['mlp_down'][layer, cols, :])
            update = part if update is None else update + part
        hidden = (hidden.astype(F32) + update).astype(BF16)
        hid[...] = hidden

    phase('end')
    out_ref[...] = hid[...]

    @pl.when(chip < mem_chips)
    def _():
        mem_out.wait_send()
    for layer in range(n_layers):
        for condition, copy in x_sends(layer):
            pl.when(condition)(copy.wait_send)
        pl.when(chip == 0)(x_forward_first(layer).wait_send)
        pl.when(chip > 0)(x_forward(layer).wait_send)
        for turn in range(chips - 1):
            @pl.when(turn < chip)
            def _():
                for part in (0, 1):
                    x_relay_copy(layer, turn, part).wait_send()
        for d in range(1, chips):
            @pl.when(lax.rem(chip + d, chips) < mem_chips)
            def _():
                for k in range(CORES):
                    q_copy(layer, d, k).wait_send()

        @pl.when(chip < mem_chips)
        def _():
            q_to_partner(layer).wait_send()
            for step in range(1, group):
                part_copy(layer, lax.rem(me + step, group)).wait_send()
                stat_copy(layer, lax.rem(me + step, group)).wait_send()
    phase(None)


def solution(mesh):
    group = mesh.shape['sp']
    row_spec = P(('dp', 'sp'), None)

    def local_step(hidden, memory, mem_len, norm_self, norm_cross, norm_mlp, self_q, self_k, self_v, self_o, cross_q, cross_k, cross_v, cross_o, mlp_gate, mlp_up, mlp_down):
        rows, width = hidden.shape
        mem_rows = memory.shape[0]
        n_layers, n_heads, head_dim = self_o.shape[:3]
        inner = n_heads * head_dim
        half = inner // CORES
        hpg = half // head_dim
        all_keys = max(group * rows, CORES * mem_rows)
        weights = dict(
            self_q=self_q, self_k=self_k, self_v=self_v, self_o=self_o.reshape(n_layers, inner, width), cross_k=cross_k, cross_v=cross_v,
            cross_q=cross_q, cross_o=cross_o.reshape(n_layers, inner, width), mlp_gate=mlp_gate, mlp_up=mlp_up, mlp_down=mlp_down)
        w_scratch = [
            pltpu.VMEM((n_layers, width, half) if name in HALVED else weights[name].shape, BF16) for name in WEIGHTS]
        dma = pltpu.SemaphoreType.DMA
        vmem = pl.BlockSpec(memory_space=pltpu.VMEM)
        hbm = pl.BlockSpec(memory_space=pl.ANY)
        return pl.pallas_call(
            functools.partial(kernel, group, n_layers, head_dim),
            out_shape=jax.ShapeDtypeStruct((rows, width), BF16),
            in_specs=[vmem, hbm, pl.BlockSpec(memory_space=pltpu.SMEM), vmem, vmem, vmem] + [hbm] * len(WEIGHTS),
            out_specs=vmem,
            scratch_shapes=w_scratch + [
                pltpu.VMEM((CORES, mem_rows, width), BF16),
                pltpu.VMEM((n_layers, group, rows, width), BF16),
                pltpu.VMEM((group, rows, width), BF16),
                pltpu.VMEM((group, rows, width), BF16),
                pltpu.VMEM((n_layers, CORES * mem_rows, half), BF16),
                pltpu.VMEM((n_layers, CORES * mem_rows, half), BF16),
                pltpu.VMEM((n_layers, CORES, rows, half), BF16),
                pltpu.VMEM((n_layers, group, rows, half), BF16),
                pltpu.VMEM((n_layers, group, rows, half), BF16),
                pltpu.VMEM((n_layers, group, rows, half), BF16),
                pltpu.VMEM((n_layers, group, 2 * hpg, rows), F32),
                pltpu.VMEM((n_layers, group, 2 * hpg, rows), F32),
                pltpu.VMEM((rows, width), BF16),
                pltpu.VMEM((hpg * rows, all_keys), F32),
                pltpu.VMEM((hpg * rows, all_keys), F32),
                pltpu.VMEM((hpg * rows, all_keys), BF16),
                pltpu.VMEM((hpg * rows, all_keys), BF16),
                dma((len(WEIGHTS), n_layers)),
                dma((1,)), dma((1,)), dma((1,)),
                dma((n_layers, 7)), dma((n_layers, group // CORES - 1, 2)), dma((n_layers, group, 2)),
                dma((n_layers, group)), dma((n_layers, group)),
                dma((n_layers, group)), dma((n_layers, group)),
                dma((n_layers, group)), dma((n_layers, group)),
            ],
            compiler_params=pltpu.CompilerParams(collective_id=0, has_side_effects=True, vmem_limit_bytes=60 * 1024 * 1024),
        )(hidden, memory, mem_len, norm_self, norm_cross, norm_mlp, *[weights[name] for name in WEIGHTS])

    return jax.shard_map(local_step, mesh=mesh, in_specs=(row_spec, row_spec, P('dp')) + (P(),) * 14, out_specs=row_spec, check_vma=False)
```

```python
import functools

import jax
import jax.numpy as jnp
from jax import lax
from jax.experimental import pallas as pl
from jax.experimental.pallas import tpu as pltpu
from jax.sharding import PartitionSpec as P

EPS = 1e-6
NEG_BIG = -1e30
CORES = 2
KEY_BLOCK = 512
FF_BLOCK = 512
MEM_BLOCK = 256
ROW_BLOCK = 64
LAG = 1
LOWEST = -3.4e38
MEM_LEN_MAX = 6144
F32 = jnp.float32
BF16 = jnp.bfloat16
MESH = pl.DeviceIdType.MESH
WEIGHTS = ('self_q', 'self_k', 'self_v', 'self_o', 'cross_k', 'cross_v', 'cross_q', 'cross_o', 'mlp_gate', 'mlp_up', 'mlp_down')
HALVED = ('cross_k', 'cross_v')


def rms_norm(hidden, gain_row):
    hidden32 = hidden.astype(F32)
    inv_rms = lax.rsqrt(jnp.mean(hidden32 * hidden32, axis=-1, keepdims=True) + EPS)
    return (hidden32 * inv_rms * gain_row.astype(F32)).astype(BF16)


def mm(a, b):
    return jnp.dot(a, b, preferred_element_type=F32)


def mm_t(a, b):
    return lax.dot_general(a, b, (((1,), (1,)), ((), ())), preferred_element_type=F32)


def lane_groups(rows, lanes, head_dim):
    return lax.broadcasted_iota(jnp.int32, (rows, lanes), 1) // head_dim


def stack_heads(q, head_dim, scale):
    rows, lanes = q.shape
    scaled = q.astype(F32) * scale
    group = lane_groups(rows, lanes, head_dim)
    return jnp.concatenate([jnp.where(group == h, scaled, 0.0).astype(BF16) for h in range(lanes // head_dim)], axis=0)


def score_steps(q_stack, key_block, n_keys, allowed, scores_ref):
    def step(start):
        scores = mm_t(q_stack, key_block(start))
        scores_ref[:, start:start + KEY_BLOCK] = jnp.where(allowed(start), scores, NEG_BIG)
    return [functools.partial(step, start) for start in range(0, n_keys, KEY_BLOCK)]


def exponent_steps(n_keys, scores_ref, weights_ref, tops, dens, lag=0):
    sums = []

    def step(row):
        at = slice(row, row + ROW_BLOCK)
        tiles = [scores_ref[at, lane:lane + 128] for lane in range(0, n_keys, 128)]
        if lag and len(sums) >= lag:
            tiles.insert(0, jnp.minimum(sums[-lag], LOWEST))
        top = jnp.max(functools.reduce(jnp.maximum, tiles), axis=-1, keepdims=True)
        run_sum = None
        for lane in range(0, n_keys, 256):
            weights = jnp.exp(scores_ref[at, lane:lane + 256] - top)
            weights_ref[at, lane:lane + 256] = weights.astype(BF16)
            pair = weights[:, :128] + weights[:, 128:]
            run_sum = pair if run_sum is None else run_sum + pair
        sums.append(run_sum)
        tops.append(top)
        dens.append(jnp.sum(run_sum, axis=-1, keepdims=True))
    return [functools.partial(step, row) for row in range(0, scores_ref.shape[0], ROW_BLOCK)]


def value_steps(value_block, n_keys, weights_ref, parts):
    def step(start):
        part = mm(weights_ref[:, start:start + KEY_BLOCK], value_block(start))
        parts[:] = [part if not parts else parts[0] + part]
    return [functools.partial(step, start) for start in range(0, n_keys, KEY_BLOCK)]


def interleave(*lists):
    order = sorted(((i + 0.5) / len(steps), n, i) for n, steps in enumerate(lists) for i in range(len(steps)))
    for _, n, i in order:
        lists[n][i]()


def unstack_heads(stacked, rows, head_dim):
    lanes = stacked.shape[1]
    group = lane_groups(rows, lanes, head_dim)
    out = stacked[:rows]
    for h in range(1, lanes // head_dim):
        out = jnp.where(group == h, stacked[h * rows:(h + 1) * rows], out)
    return out


class Phase:
    def __init__(self):
        self.cur = None

    def __call__(self, name):
        if self.cur is not None:
            self.cur.__exit__(None, None, None)
        self.cur = jax.named_scope(name) if name else None
        if self.cur is not None:
            self.cur.__enter__()


def kernel(group, n_layers, head_dim, *refs):
    n_w = len(WEIGHTS)
    hidden_ref, memory_ref, mem_len_ref, norm_self, norm_cross, norm_mlp = refs[:6]
    w_hbm = dict(zip(WEIGHTS, refs[6:6 + n_w]))
    out_ref = refs[6 + n_w]
    scratch = refs[7 + n_w:]
    w = dict(zip(WEIGHTS, scratch[:n_w]))
    (mem_v, x_all, k_all, v_all, mem_k, mem_vals, q_send, q_all, part_send, part_recv, stat_send, stat_recv, hid, scores_a, scores_b, weights_a, weights_b,
     w_sem, mem_sem, mem_send, mem_recv, x_send, x_relay, x_recv, q_ssem, q_rsem, p_ssem, p_rsem, s_ssem, s_rsem) = scratch[n_w:]

    rows, width = hidden_ref.shape
    mem_rows = memory_ref.shape[0]
    chips = group // CORES
    mem_chips = -(-MEM_LEN_MAX // (CORES * mem_rows))
    half = q_send.shape[-1]
    hpg = half // head_dim
    scale = head_dim ** -0.5
    me = lax.axis_index('sp')
    chip, core = me // CORES, me % CORES
    partner = chip * CORES + (1 - core)

    def remote(src, dst, ssem, rsem, dev):
        return pltpu.make_async_remote_copy(src_ref=src, dst_ref=dst, send_sem=ssem, recv_sem=rsem, device_id={'sp': dev}, device_id_type=MESH)

    def weight_copy(name, layer):
        src = w_hbm[name].at[layer]
        if name in HALVED:
            src = w_hbm[name].at[layer, :, pl.ds(pl.multiple_of(core * half, half), half)]
        return pltpu.make_async_copy(src, w[name].at[layer], w_sem.at[WEIGHTS.index(name), layer])

    phase = Phase()
    phase('start')
    mem_copy = pltpu.make_async_copy(memory_ref, mem_v.at[core], mem_sem.at[0])

    for name in ('self_q', 'self_k', 'self_v'):
        weight_copy(name, 0).start()
    mem_copy.start()
    for layer in range(n_layers):
        for name in HALVED:
            weight_copy(name, layer).start()

    def start_weights(layer, names):
        for name in names:
            weight_copy(name, layer).start()

    phase('barrier')
    barrier = pltpu.get_barrier_semaphore()
    for step in range(1, group):
        pl.semaphore_signal(barrier, inc=1, device_id={'sp': lax.rem(me + step, group)}, device_id_type=MESH)
    pl.semaphore_wait(barrier, group - 1)

    top_chip = chip // (chips - 1)
    half_rows = rows // 2

    def x_copy(layer, src, part, ssem, dst):
        at = x_all.at[layer, src, pl.ds(pl.multiple_of(part * half_rows, half_rows), half_rows)]
        return remote(at, at, ssem, x_recv.at[layer, src, part], dst)

    def x_sends(layer):
        up = me + CORES
        across = (chips - 1) * CORES + core
        send = x_send.at
        return [
            (chip == 1, x_copy(layer, me, 1, send[layer, 2], core)),
            (chip < chips - 1, x_copy(layer, me, 0, send[layer, 0], up)),
            (chip == 0, x_copy(layer, me, 1, send[layer, 2], across)),
            (chip < chips - 1, x_copy(layer, me, 1, send[layer, 1], up)),
            (chip == 0, x_copy(layer, me, 0, send[layer, 3], across)),
            (core == 0, x_copy(layer, me, 0, send[layer, 4], partner)),
            (core == 0, x_copy(layer, me, 1, send[layer, 5], partner)),
        ]

    def x_source(turn):
        return top_chip * (turn * 2 - 3 * (turn // 2)) + (1 - top_chip) * (chip - 1 - turn)

    def x_forward(layer):
        src = x_source(0) * CORES + core
        return x_copy(layer, src, top_chip, x_send.at[layer, 6], me + CORES - 2 * CORES * top_chip)

    def x_forward_first(layer):
        return x_copy(layer, CORES + core, 1, x_send.at[layer, 6], (chips - 1) * CORES + core)

    def x_relay_copy(layer, turn, part):
        return x_copy(layer, x_source(turn) * CORES + core, part, x_relay.at[layer, turn, part], partner)

    def x_arrival(layer, src, part):
        return x_copy(layer, src, part, x_send.at[layer, 0], partner)

    def q_copy(layer, d, k):
        dst = lax.rem(chip + d, chips) * CORES + k
        return remote(q_send.at[layer, k], q_all.at[layer, me], q_ssem.at[layer, d * CORES + k], q_rsem.at[layer, me], dst)

    def q_to_partner(layer):
        return remote(q_send.at[layer, 1 - core], q_all.at[layer, me], q_ssem.at[layer, 0], q_rsem.at[layer, me], partner)

    def q_arrival(layer, src):
        return remote(q_send.at[layer, 0], q_all.at[layer, src], q_ssem.at[layer, 0], q_rsem.at[layer, src], partner)

    def part_copy(layer, src):
        return remote(part_send.at[layer, src], part_recv.at[layer, me], p_ssem.at[layer, src], p_rsem.at[layer, me], src)

    def stat_copy(layer, src):
        return remote(stat_send.at[layer, src], stat_recv.at[layer, me], s_ssem.at[layer, src], s_rsem.at[layer, me], src)

    def part_arrival(layer, src):
        return remote(part_send.at[layer, src], part_recv.at[layer, src], p_ssem.at[layer, src], p_rsem.at[layer, src], partner)

    def stat_arrival(layer, src):
        return remote(stat_send.at[layer, src], stat_recv.at[layer, src], s_ssem.at[layer, src], s_rsem.at[layer, src], partner)

    mem_out = remote(mem_v.at[core], mem_v.at[core], mem_send.at[0], mem_recv.at[0], partner)
    mem_in = remote(mem_v.at[1 - core], mem_v.at[1 - core], mem_send.at[0], mem_recv.at[0], partner)

    def project_memory(slot, layer):
        def body(i, carry):
            at = pl.ds(pl.multiple_of(i * MEM_BLOCK, MEM_BLOCK), MEM_BLOCK)
            to = pl.ds(pl.multiple_of(slot * mem_rows + i * MEM_BLOCK, MEM_BLOCK), MEM_BLOCK)
            block = mem_v[slot, at, :]
            mem_k[layer, to, :] = mm(block, w['cross_k'][layer]).astype(BF16)
            mem_vals[layer, to, :] = mm(block, w['cross_v'][layer]).astype(BF16)
            return carry
        lax.fori_loop(0, mem_rows // MEM_BLOCK, body, 0)

    phase('zero')
    hid[...] = hidden_ref[...]
    for src in range(group):
        @pl.when(src > me)
        def _():
            k_all[src] = jnp.zeros((rows, width), BF16)
            v_all[src] = jnp.zeros((rows, width), BF16)

    for layer in range(n_layers):
        phase(f'xnorm{layer}')
        x_all[layer, me] = rms_norm(hid[...], norm_self[layer:layer + 1, :])
        for condition, copy in x_sends(layer):
            pl.when(condition)(copy.start)
        if layer == 0:
            start_weights(0, ('self_o', 'cross_q', 'cross_o'))

        for name in ('self_q', 'self_k', 'self_v'):
            weight_copy(name, layer).wait()

        def project_rows(src):
            block = x_all[layer, src]
            k_all[src] = mm(block, w['self_k'][layer]).astype(BF16)
            v_all[src] = mm(block, w['self_v'][layer]).astype(BF16)

        phase(f'ownproj{layer}')
        project_rows(me)
        queries = mm(x_all[layer, me], w['self_q'][layer]).astype(BF16)

        phase(f'memproj{layer}')
        if layer == 0:
            mem_copy.wait()
            for other in range(n_layers):
                for name in HALVED:
                    weight_copy(name, other).wait()

            @pl.when(chip < mem_chips)
            def _():
                mem_out.start()
                for other in range(n_layers):
                    project_memory(core, other)
        phase(f'xwait{layer}')

        @pl.when(chip == 0)
        def _():
            x_arrival(layer, CORES + core, 1).wait_recv()
            x_forward_first(layer).start()

        for turn in range(chips - 1):
            @pl.when(turn < chip)
            def _():
                src = x_source(turn) * CORES + core
                first = top_chip if turn == 0 else 0
                for i, part in enumerate((first, 1 - first)):
                    x_arrival(layer, src, part).wait_recv()
                    if turn == 0 and i == 0:
                        pl.when(chip > 0)(x_forward(layer).start)
                    x_relay_copy(layer, turn, part).start()
                project_rows(src)

        phase(f'memproj2{layer}')

        @pl.when(chip < mem_chips)
        def _():
            if layer == 0:
                mem_in.wait_recv()
            project_memory(1 - core, layer)

        phase(f'xwait2{layer}')
        @pl.when(core == 1)
        def _():
            for part in (0, 1):
                x_arrival(layer, partner, part).wait_recv()
            project_rows(partner)

        for turn in range(chips - 1):
            @pl.when(turn < chip)
            def _():
                src = x_source(turn) * CORES + (1 - core)
                for part in (0, 1):
                    x_arrival(layer, src, part).wait_recv()
                project_rows(src)

        phase(f'selfatt{layer}')
        all_rows = group * rows
        query_at = me * rows + lax.rem(lax.broadcasted_iota(jnp.int32, (hpg * rows, KEY_BLOCK), 0), rows)
        key_at = lax.broadcasted_iota(jnp.int32, (hpg * rows, KEY_BLOCK), 1)
        per_block = KEY_BLOCK // rows
        stores = ((scores_a, weights_a), (scores_b, weights_b))
        tops, dens, parts = [[], []], [[], []], [[], []]

        def self_steps(g):
            lanes = slice(g * half, (g + 1) * half)
            s_ref, w_ref = stores[g]
            return (
                score_steps(stack_heads(queries[:, lanes], head_dim, scale),
                            lambda start: k_all[start // rows:start // rows + per_block, :, lanes].reshape(KEY_BLOCK, half),
                            all_rows, lambda start: key_at + start <= query_at, s_ref),
                exponent_steps(all_rows, s_ref, w_ref, tops[g], dens[g]),
                value_steps(lambda start: v_all[start // rows:start // rows + per_block, :, lanes].reshape(KEY_BLOCK, half),
                            all_rows, w_ref, parts[g]))

        steps = [self_steps(g) for g in range(CORES)]
        interleave(steps[0][0])
        interleave(steps[0][1], steps[1][0])
        interleave(steps[0][2], steps[1][1])
        interleave(steps[1][2])
        attended = [unstack_heads(parts[g][0] / jnp.concatenate(dens[g], axis=0), rows, head_dim).astype(BF16) for g in range(CORES)]
        attended = jnp.concatenate(attended, axis=-1)
        phase(f'oproj{layer}')
        weight_copy('self_o', layer).wait()
        hidden = (hid[...].astype(F32) + mm(attended, w['self_o'][layer])).astype(BF16)
        hid[...] = hidden

        phase(f'qproj{layer}')
        weight_copy('cross_q', layer).wait()
        queries = mm(rms_norm(hidden, norm_cross[layer:layer + 1, :]), w['cross_q'][layer]).astype(BF16)
        for g in range(CORES):
            q_send[layer, g] = queries[:, g * half:(g + 1) * half]
        q_order = [(d, k) for d in (1, 3, 2) if d < chips for k in range(CORES)]

        @pl.when(chip < mem_chips)
        def _():
            q_to_partner(layer).start()
        for d, k in q_order:
            @pl.when(lax.rem(chip + d, chips) < mem_chips)
            def _():
                q_copy(layer, d, k).start()
        q_all[layer, me] = q_send[layer, core]
        if layer == 0:
            start_weights(0, ('mlp_gate', 'mlp_up', 'mlp_down'))
            for other in range(1, n_layers):
                start_weights(other, [name for name in WEIGHTS if name not in HALVED])

        mem_at = chip * (CORES * mem_rows) + lax.broadcasted_iota(jnp.int32, (1, KEY_BLOCK), 1)
        n_keys = CORES * mem_rows

        def wait_queries(src):
            @pl.when(src != me)
            def _():
                q_arrival(layer, src).wait_recv()

        def score_of(src, scores_ref):
            return score_steps(stack_heads(q_all[layer, src], head_dim, scale), lambda start: mem_k[layer, start:start + KEY_BLOCK, :], n_keys,
                               lambda start: mem_at + start < mem_len_ref[0], scores_ref)

        def put_stats(src, tops, dens):
            top, den = jnp.concatenate(tops, axis=0), jnp.concatenate(dens, axis=0)
            lane = lax.broadcasted_iota(jnp.int32, (rows, 128), 1)
            stats = jnp.zeros((rows, 128), F32)
            for h in range(hpg):
                stats = jnp.where(lane == h, top[h * rows:(h + 1) * rows], stats)
                stats = jnp.where(lane == hpg + h, den[h * rows:(h + 1) * rows], stats)
            stat_send[layer, src] = jnp.transpose(stats)[:2 * hpg]

        def values_of(weights_ref, parts):
            return value_steps(lambda start: mem_vals[layer, start:start + KEY_BLOCK, :], n_keys, weights_ref, parts)

        def put_part(src, parts):
            part_send[layer, src] = unstack_heads(parts[0], rows, head_dim).astype(BF16)

        def stages(after, s_after, now, s_now, w_now, before, w_before):
            tops, dens, parts = [], [], []
            interleave(score_of(after, s_after), exponent_steps(n_keys, s_now, w_now, tops, dens, LAG), values_of(w_before, parts))
            put_stats(now, tops, dens)
            put_part(before, parts)

        def send(src, copy):
            @pl.when(src != me)
            def _():
                copy(layer, src).start()

        phase(f'cross{layer}')

        def turn_body(turn, carry):
            first = turn * 2
            second, before, after = first + 1, lax.rem(first + group - 1, group), jnp.minimum(first + 2, group - 1)
            wait_queries(second)
            stages(second, scores_b, first, scores_a, weights_a, before, weights_b)
            send(first, stat_copy)

            @pl.when(turn > 0)
            def _():
                send(before, part_copy)

            @pl.when(turn < group // 2 - 1)
            def _():
                wait_queries(first + 2)
            stages(after, scores_a, second, scores_b, weights_b, first, weights_a)
            send(second, stat_copy)
            send(first, part_copy)
            return carry

        @pl.when(chip < mem_chips)
        def _():
            wait_queries(0)
            interleave(score_of(0, scores_a))
            lax.fori_loop(0, group // 2, turn_body, 0)
            parts = []
            interleave(values_of(weights_b, parts))
            put_part(group - 1, parts)
            send(group - 1, part_copy)
            part_recv[layer, me] = part_send[layer, me]
            stat_recv[layer, me] = stat_send[layer, me]
        phase(f'arrived{layer}')

        for src in range(mem_chips * CORES):
            @pl.when(src != me)
            def _():
                stat_arrival(layer, src).wait_recv()
                part_arrival(layer, src).wait_recv()

        phase(f'combine{layer}')
        factors = [None] * (mem_chips * CORES)
        for g in range(CORES):
            members = [c * CORES + g for c in range(mem_chips)]
            tops = [stat_recv[layer, i, 0:hpg] for i in members]
            dens = [stat_recv[layer, i, hpg:2 * hpg] for i in members]
            best = functools.reduce(jnp.maximum, tops)
            shares = [jnp.exp(t - best) for t in tops]
            total = functools.reduce(jnp.add, [s * d for s, d in zip(shares, dens)])
            for i, s in zip(members, shares):
                factors[i] = s / total
        packed = jnp.concatenate(factors + [jnp.zeros((128 - mem_chips * CORES * hpg, rows), F32)], axis=0)
        packed = jnp.transpose(packed)
        lane_group = lane_groups(rows, half, head_dim)
        attended = []
        for g in range(CORES):
            total = jnp.zeros((rows, half), F32)
            for c in range(mem_chips):
                i = c * CORES + g
                factor = jnp.zeros((rows, half), F32)
                for h in range(hpg):
                    factor = jnp.where(lane_group == h, packed[:, i * hpg + h:i * hpg + h + 1], factor)
                total = total + part_recv[layer, i].astype(F32) * factor
            attended.append(total.astype(BF16))
        attended = jnp.concatenate(attended, axis=-1)
        phase(f'co{layer}')
        weight_copy('cross_o', layer).wait()
        hidden = (hid[...].astype(F32) + mm(attended, w['cross_o'][layer])).astype(BF16)

        phase(f'mlp{layer}')
        normed = rms_norm(hidden, norm_mlp[layer:layer + 1, :])
        for name in ('mlp_gate', 'mlp_up', 'mlp_down'):
            weight_copy(name, layer).wait()
        update = None
        for start in range(0, w['mlp_gate'].shape[-1], FF_BLOCK):
            cols = slice(start, start + FF_BLOCK)
            gate = mm(normed, w['mlp_gate'][layer, :, cols])
            up = mm(normed, w['mlp_up'][layer, :, cols])
            act = (gate * jax.nn.sigmoid(gate) * up).astype(BF16)
            part = mm(act, w['mlp_down'][layer, cols, :])
            update = part if update is None else update + part
        hidden = (hidden.astype(F32) + update).astype(BF16)
        hid[...] = hidden

    phase('end')
    out_ref[...] = hid[...]

    @pl.when(chip < mem_chips)
    def _():
        mem_out.wait_send()
    for layer in range(n_layers):
        for condition, copy in x_sends(layer):
            pl.when(condition)(copy.wait_send)
        pl.when(chip == 0)(x_forward_first(layer).wait_send)
        pl.when(chip > 0)(x_forward(layer).wait_send)
        for turn in range(chips - 1):
            @pl.when(turn < chip)
            def _():
                for part in (0, 1):
                    x_relay_copy(layer, turn, part).wait_send()
        for d in range(1, chips):
            @pl.when(lax.rem(chip + d, chips) < mem_chips)
            def _():
                for k in range(CORES):
                    q_copy(layer, d, k).wait_send()

        @pl.when(chip < mem_chips)
        def _():
            q_to_partner(layer).wait_send()
            for step in range(1, group):
                part_copy(layer, lax.rem(me + step, group)).wait_send()
                stat_copy(layer, lax.rem(me + step, group)).wait_send()
    phase(None)


def solution(mesh):
    group = mesh.shape['sp']
    row_spec = P(('dp', 'sp'), None)

    def local_step(hidden, memory, mem_len, norm_self, norm_cross, norm_mlp, self_q, self_k, self_v, self_o, cross_q, cross_k, cross_v, cross_o, mlp_gate, mlp_up, mlp_down):
        rows, width = hidden.shape
        mem_rows = memory.shape[0]
        n_layers, n_heads, head_dim = self_o.shape[:3]
        inner = n_heads * head_dim
        half = inner // CORES
        hpg = half // head_dim
        all_keys = max(group * rows, CORES * mem_rows)
        weights = dict(
            self_q=self_q, self_k=self_k, self_v=self_v, self_o=self_o.reshape(n_layers, inner, width), cross_k=cross_k, cross_v=cross_v,
            cross_q=cross_q, cross_o=cross_o.reshape(n_layers, inner, width), mlp_gate=mlp_gate, mlp_up=mlp_up, mlp_down=mlp_down)
        w_scratch = [
            pltpu.VMEM((n_layers, width, half) if name in HALVED else weights[name].shape, BF16) for name in WEIGHTS]
        dma = pltpu.SemaphoreType.DMA
        vmem = pl.BlockSpec(memory_space=pltpu.VMEM)
        hbm = pl.BlockSpec(memory_space=pl.ANY)
        return pl.pallas_call(
            functools.partial(kernel, group, n_layers, head_dim),
            out_shape=jax.ShapeDtypeStruct((rows, width), BF16),
            in_specs=[vmem, hbm, pl.BlockSpec(memory_space=pltpu.SMEM), vmem, vmem, vmem] + [hbm] * len(WEIGHTS),
            out_specs=vmem,
            scratch_shapes=w_scratch + [
                pltpu.VMEM((CORES, mem_rows, width), BF16),
                pltpu.VMEM((n_layers, group, rows, width), BF16),
                pltpu.VMEM((group, rows, width), BF16),
                pltpu.VMEM((group, rows, width), BF16),
                pltpu.VMEM((n_layers, CORES * mem_rows, half), BF16),
                pltpu.VMEM((n_layers, CORES * mem_rows, half), BF16),
                pltpu.VMEM((n_layers, CORES, rows, half), BF16),
                pltpu.VMEM((n_layers, group, rows, half), BF16),
                pltpu.VMEM((n_layers, group, rows, half), BF16),
                pltpu.VMEM((n_layers, group, rows, half), BF16),
                pltpu.VMEM((n_layers, group, 2 * hpg, rows), F32),
                pltpu.VMEM((n_layers, group, 2 * hpg, rows), F32),
                pltpu.VMEM((rows, width), BF16),
                pltpu.VMEM((hpg * rows, all_keys), F32),
                pltpu.VMEM((hpg * rows, all_keys), F32),
                pltpu.VMEM((hpg * rows, all_keys), BF16),
                pltpu.VMEM((hpg * rows, all_keys), BF16),
                dma((len(WEIGHTS), n_layers)),
                dma((1,)), dma((1,)), dma((1,)),
                dma((n_layers, 7)), dma((n_layers, group // CORES - 1, 2)), dma((n_layers, group, 2)),
                dma((n_layers, group)), dma((n_layers, group)),
                dma((n_layers, group)), dma((n_layers, group)),
                dma((n_layers, group)), dma((n_layers, group)),
            ],
            compiler_params=pltpu.CompilerParams(collective_id=0, has_side_effects=True, vmem_limit_bytes=60 * 1024 * 1024),
        )(hidden, memory, mem_len, norm_self, norm_cross, norm_mlp, *[weights[name] for name in WEIGHTS])

    return jax.shard_map(local_step, mesh=mesh, in_specs=(row_spec, row_spec, P('dp')) + (P(),) * 14, out_specs=row_spec, check_vma=False)
```

```python
import functools

import jax
import jax.numpy as jnp
from jax import lax
from jax.experimental import pallas as pl
from jax.experimental.pallas import tpu as pltpu
from jax.sharding import PartitionSpec as P

EPS = 1e-6
NEG_BIG = -1e30
CORES = 2
KEY_BLOCK = 512
FF_BLOCK = 512
MEM_BLOCK = 256
ROW_BLOCK = 64
LAG = 1
X_ORDER = (2, 3, 1)
LOWEST = -3.4e38
MEM_LEN_MAX = 6144
F32 = jnp.float32
BF16 = jnp.bfloat16
MESH = pl.DeviceIdType.MESH
WEIGHTS = ('self_q', 'self_k', 'self_v', 'self_o', 'cross_k', 'cross_v', 'cross_q', 'cross_o', 'mlp_gate', 'mlp_up', 'mlp_down')
HALVED = ('cross_k', 'cross_v')


def rms_norm(hidden, gain_row):
    hidden32 = hidden.astype(F32)
    inv_rms = lax.rsqrt(jnp.mean(hidden32 * hidden32, axis=-1, keepdims=True) + EPS)
    return (hidden32 * inv_rms * gain_row.astype(F32)).astype(BF16)


def mm(a, b):
    return jnp.dot(a, b, preferred_element_type=F32)


def mm_t(a, b):
    return lax.dot_general(a, b, (((1,), (1,)), ((), ())), preferred_element_type=F32)


def lane_groups(rows, lanes, head_dim):
    return lax.broadcasted_iota(jnp.int32, (rows, lanes), 1) // head_dim


def stack_heads(q, head_dim, scale):
    rows, lanes = q.shape
    scaled = q.astype(F32) * scale
    group = lane_groups(rows, lanes, head_dim)
    return jnp.concatenate([jnp.where(group == h, scaled, 0.0).astype(BF16) for h in range(lanes // head_dim)], axis=0)


def score_steps(q_stack, key_block, n_keys, allowed, scores_ref):
    def step(start):
        scores = mm_t(q_stack, key_block(start))
        scores_ref[:, start:start + KEY_BLOCK] = jnp.where(allowed(start), scores, NEG_BIG)
    return [functools.partial(step, start) for start in range(0, n_keys, KEY_BLOCK)]


def exponent_steps(n_keys, scores_ref, weights_ref, tops, dens, lag=0):
    sums = []

    def step(row):
        at = slice(row, row + ROW_BLOCK)
        tiles = [scores_ref[at, lane:lane + 128] for lane in range(0, n_keys, 128)]
        if lag and len(sums) >= lag:
            tiles.insert(0, jnp.minimum(sums[-lag], LOWEST))
        top = jnp.max(functools.reduce(jnp.maximum, tiles), axis=-1, keepdims=True)
        run_sum = None
        for lane in range(0, n_keys, 256):
            weights = jnp.exp(scores_ref[at, lane:lane + 256] - top)
            weights_ref[at, lane:lane + 256] = weights.astype(BF16)
            pair = weights[:, :128] + weights[:, 128:]
            run_sum = pair if run_sum is None else run_sum + pair
        sums.append(run_sum)
        tops.append(top)
        dens.append(jnp.sum(run_sum, axis=-1, keepdims=True))
    return [functools.partial(step, row) for row in range(0, scores_ref.shape[0], ROW_BLOCK)]


def value_steps(value_block, n_keys, weights_ref, parts):
    def step(start):
        part = mm(weights_ref[:, start:start + KEY_BLOCK], value_block(start))
        parts[:] = [part if not parts else parts[0] + part]
    return [functools.partial(step, start) for start in range(0, n_keys, KEY_BLOCK)]


def interleave(*lists):
    order = sorted(((i + 0.5) / len(steps), n, i) for n, steps in enumerate(lists) for i in range(len(steps)))
    for _, n, i in order:
        lists[n][i]()


def unstack_heads(stacked, rows, head_dim):
    lanes = stacked.shape[1]
    group = lane_groups(rows, lanes, head_dim)
    out = stacked[:rows]
    for h in range(1, lanes // head_dim):
        out = jnp.where(group == h, stacked[h * rows:(h + 1) * rows], out)
    return out


class Phase:
    def __init__(self):
        self.cur = None

    def __call__(self, name):
        if self.cur is not None:
            self.cur.__exit__(None, None, None)
        self.cur = jax.named_scope(name) if name else None
        if self.cur is not None:
            self.cur.__enter__()


def kernel(group, n_layers, head_dim, *refs):
    n_w = len(WEIGHTS)
    hidden_ref, memory_ref, mem_len_ref, norm_self, norm_cross, norm_mlp = refs[:6]
    w_hbm = dict(zip(WEIGHTS, refs[6:6 + n_w]))
    out_ref = refs[6 + n_w]
    scratch = refs[7 + n_w:]
    w = dict(zip(WEIGHTS, scratch[:n_w]))
    (mem_v, x_all, k_all, v_all, mem_k, mem_vals, q_send, q_all, part_send, part_recv, stat_send, stat_recv, hid, scores_a, scores_b, weights_a, weights_b,
     w_sem, mem_sem, mem_send, mem_recv, x_send, x_relay, x_recv, q_ssem, q_rsem, p_ssem, p_rsem, s_ssem, s_rsem) = scratch[n_w:]

    rows, width = hidden_ref.shape
    mem_rows = memory_ref.shape[0]
    chips = group // CORES
    mem_chips = -(-MEM_LEN_MAX // (CORES * mem_rows))
    half = q_send.shape[-1]
    hpg = half // head_dim
    scale = head_dim ** -0.5
    me = lax.axis_index('sp')
    chip, core = me // CORES, me % CORES
    partner = chip * CORES + (1 - core)

    def remote(src, dst, ssem, rsem, dev):
        return pltpu.make_async_remote_copy(src_ref=src, dst_ref=dst, send_sem=ssem, recv_sem=rsem, device_id={'sp': dev}, device_id_type=MESH)

    def weight_copy(name, layer):
        src = w_hbm[name].at[layer]
        if name in HALVED:
            src = w_hbm[name].at[layer, :, pl.ds(pl.multiple_of(core * half, half), half)]
        return pltpu.make_async_copy(src, w[name].at[layer], w_sem.at[WEIGHTS.index(name), layer])

    phase = Phase()
    phase('start')
    mem_copy = pltpu.make_async_copy(memory_ref, mem_v.at[core], mem_sem.at[0])

    for name in ('self_q', 'self_k', 'self_v'):
        weight_copy(name, 0).start()
    mem_copy.start()
    for layer in range(n_layers):
        for name in HALVED:
            weight_copy(name, layer).start()

    def start_weights(layer, names):
        for name in names:
            weight_copy(name, layer).start()

    phase('barrier')
    barrier = pltpu.get_barrier_semaphore()
    for step in range(1, group):
        pl.semaphore_signal(barrier, inc=1, device_id={'sp': lax.rem(me + step, group)}, device_id_type=MESH)
    pl.semaphore_wait(barrier, group - 1)

    top_chip = chip // (chips - 1)
    half_rows = rows // 2

    def x_copy(layer, src, part, ssem, dst):
        at = x_all.at[layer, src, pl.ds(pl.multiple_of(part * half_rows, half_rows), half_rows)]
        return remote(at, at, ssem, x_recv.at[layer, src, part], dst)

    def x_sends(layer):
        sends = []
        for d in X_ORDER:
            for part in (0, 1):
                sends.append((chip + d < chips, x_copy(layer, me, part, x_send.at[layer, d, part], me + d * CORES)))
        for part in (0, 1):
            sends.append((core == 0, x_copy(layer, me, part, x_send.at[layer, 0, part], partner)))
        return sends

    def x_source(turn):
        return top_chip * (turn * 2 - 3 * (turn // 2)) + (1 - top_chip) * (chip - 1 - turn)

    def x_relay_copy(layer, turn, part):
        return x_copy(layer, x_source(turn) * CORES + core, part, x_relay.at[layer, turn, part], partner)

    def x_arrival(layer, src, part):
        return x_copy(layer, src, part, x_send.at[layer, 0, part], partner)

    def q_copy(layer, d, k):
        dst = lax.rem(chip + d, chips) * CORES + k
        return remote(q_send.at[layer, k], q_all.at[layer, me], q_ssem.at[layer, d * CORES + k], q_rsem.at[layer, me], dst)

    def q_to_partner(layer):
        return remote(q_send.at[layer, 1 - core], q_all.at[layer, me], q_ssem.at[layer, 0], q_rsem.at[layer, me], partner)

    def q_arrival(layer, src):
        return remote(q_send.at[layer, 0], q_all.at[layer, src], q_ssem.at[layer, 0], q_rsem.at[layer, src], partner)

    def part_copy(layer, src):
        return remote(part_send.at[layer, src], part_recv.at[layer, me], p_ssem.at[layer, src], p_rsem.at[layer, me], src)

    def stat_copy(layer, src):
        return remote(stat_send.at[layer, src], stat_recv.at[layer, me], s_ssem.at[layer, src], s_rsem.at[layer, me], src)

    def part_arrival(layer, src):
        return remote(part_send.at[layer, src], part_recv.at[layer, src], p_ssem.at[layer, src], p_rsem.at[layer, src], partner)

    def stat_arrival(layer, src):
        return remote(stat_send.at[layer, src], stat_recv.at[layer, src], s_ssem.at[layer, src], s_rsem.at[layer, src], partner)

    mem_out = remote(mem_v.at[core], mem_v.at[core], mem_send.at[0], mem_recv.at[0], partner)
    mem_in = remote(mem_v.at[1 - core], mem_v.at[1 - core], mem_send.at[0], mem_recv.at[0], partner)

    def project_memory(slot, layer):
        def body(i, carry):
            at = pl.ds(pl.multiple_of(i * MEM_BLOCK, MEM_BLOCK), MEM_BLOCK)
            to = pl.ds(pl.multiple_of(slot * mem_rows + i * MEM_BLOCK, MEM_BLOCK), MEM_BLOCK)
            block = mem_v[slot, at, :]
            mem_k[layer, to, :] = mm(block, w['cross_k'][layer]).astype(BF16)
            mem_vals[layer, to, :] = mm(block, w['cross_v'][layer]).astype(BF16)
            return carry
        lax.fori_loop(0, mem_rows // MEM_BLOCK, body, 0)

    phase('zero')
    hid[...] = hidden_ref[...]
    for src in range(group):
        @pl.when(src > me)
        def _():
            k_all[src] = jnp.zeros((rows, width), BF16)
            v_all[src] = jnp.zeros((rows, width), BF16)

    for layer in range(n_layers):
        phase(f'xnorm{layer}')
        x_all[layer, me] = rms_norm(hid[...], norm_self[layer:layer + 1, :])
        for condition, copy in x_sends(layer):
            pl.when(condition)(copy.start)
        if layer == 0:
            start_weights(0, ('self_o', 'cross_q', 'cross_o'))

        for name in ('self_q', 'self_k', 'self_v'):
            weight_copy(name, layer).wait()

        def project_rows(src):
            block = x_all[layer, src]
            k_all[src] = mm(block, w['self_k'][layer]).astype(BF16)
            v_all[src] = mm(block, w['self_v'][layer]).astype(BF16)

        phase(f'ownproj{layer}')
        project_rows(me)
        queries = mm(x_all[layer, me], w['self_q'][layer]).astype(BF16)

        phase(f'memproj{layer}')
        if layer == 0:
            mem_copy.wait()
            for other in range(n_layers):
                for name in HALVED:
                    weight_copy(name, other).wait()

            @pl.when(chip < mem_chips)
            def _():
                mem_out.start()
                for other in range(n_layers):
                    project_memory(core, other)
        phase(f'xwait{layer}')

        for turn in range(chips - 1):
            @pl.when(turn < chip)
            def _():
                src = x_source(turn) * CORES + core
                for part in (0, 1):
                    x_arrival(layer, src, part).wait_recv()
                    x_relay_copy(layer, turn, part).start()
                project_rows(src)

        phase(f'memproj2{layer}')

        @pl.when(chip < mem_chips)
        def _():
            if layer == 0:
                mem_in.wait_recv()
            project_memory(1 - core, layer)

        phase(f'xwait2{layer}')
        @pl.when(core == 1)
        def _():
            for part in (0, 1):
                x_arrival(layer, partner, part).wait_recv()
            project_rows(partner)

        for turn in range(chips - 1):
            @pl.when(turn < chip)
            def _():
                src = x_source(turn) * CORES + (1 - core)
                for part in (0, 1):
                    x_arrival(layer, src, part).wait_recv()
                project_rows(src)

        phase(f'selfatt{layer}')
        all_rows = group * rows
        query_at = me * rows + lax.rem(lax.broadcasted_iota(jnp.int32, (hpg * rows, KEY_BLOCK), 0), rows)
        key_at = lax.broadcasted_iota(jnp.int32, (hpg * rows, KEY_BLOCK), 1)
        per_block = KEY_BLOCK // rows
        stores = ((scores_a, weights_a), (scores_b, weights_b))
        tops, dens, parts = [[], []], [[], []], [[], []]

        def self_steps(g):
            lanes = slice(g * half, (g + 1) * half)
            s_ref, w_ref = stores[g]
            return (
                score_steps(stack_heads(queries[:, lanes], head_dim, scale),
                            lambda start: k_all[start // rows:start // rows + per_block, :, lanes].reshape(KEY_BLOCK, half),
                            all_rows, lambda start: key_at + start <= query_at, s_ref),
                exponent_steps(all_rows, s_ref, w_ref, tops[g], dens[g]),
                value_steps(lambda start: v_all[start // rows:start // rows + per_block, :, lanes].reshape(KEY_BLOCK, half),
                            all_rows, w_ref, parts[g]))

        steps = [self_steps(g) for g in range(CORES)]
        interleave(steps[0][0])
        interleave(steps[0][1], steps[1][0])
        interleave(steps[0][2], steps[1][1])
        interleave(steps[1][2])
        attended = [unstack_heads(parts[g][0] / jnp.concatenate(dens[g], axis=0), rows, head_dim).astype(BF16) for g in range(CORES)]
        attended = jnp.concatenate(attended, axis=-1)
        phase(f'oproj{layer}')
        weight_copy('self_o', layer).wait()
        hidden = (hid[...].astype(F32) + mm(attended, w['self_o'][layer])).astype(BF16)
        hid[...] = hidden

        phase(f'qproj{layer}')
        weight_copy('cross_q', layer).wait()
        queries = mm(rms_norm(hidden, norm_cross[layer:layer + 1, :]), w['cross_q'][layer]).astype(BF16)
        for g in range(CORES):
            q_send[layer, g] = queries[:, g * half:(g + 1) * half]
        q_order = [(d, k) for d in (1, 3, 2) if d < chips for k in range(CORES)]

        @pl.when(chip < mem_chips)
        def _():
            q_to_partner(layer).start()
        for d, k in q_order:
            @pl.when(lax.rem(chip + d, chips) < mem_chips)
            def _():
                q_copy(layer, d, k).start()
        q_all[layer, me] = q_send[layer, core]
        if layer == 0:
            start_weights(0, ('mlp_gate', 'mlp_up', 'mlp_down'))
            for other in range(1, n_layers):
                start_weights(other, [name for name in WEIGHTS if name not in HALVED])

        mem_at = chip * (CORES * mem_rows) + lax.broadcasted_iota(jnp.int32, (1, KEY_BLOCK), 1)
        n_keys = CORES * mem_rows

        def wait_queries(src):
            @pl.when(src != me)
            def _():
                q_arrival(layer, src).wait_recv()

        def score_of(src, scores_ref):
            return score_steps(stack_heads(q_all[layer, src], head_dim, scale), lambda start: mem_k[layer, start:start + KEY_BLOCK, :], n_keys,
                               lambda start: mem_at + start < mem_len_ref[0], scores_ref)

        def put_stats(src, tops, dens):
            top, den = jnp.concatenate(tops, axis=0), jnp.concatenate(dens, axis=0)
            lane = lax.broadcasted_iota(jnp.int32, (rows, 128), 1)
            stats = jnp.zeros((rows, 128), F32)
            for h in range(hpg):
                stats = jnp.where(lane == h, top[h * rows:(h + 1) * rows], stats)
                stats = jnp.where(lane == hpg + h, den[h * rows:(h + 1) * rows], stats)
            stat_send[layer, src] = jnp.transpose(stats)[:2 * hpg]

        def values_of(weights_ref, parts):
            return value_steps(lambda start: mem_vals[layer, start:start + KEY_BLOCK, :], n_keys, weights_ref, parts)

        def put_part(src, parts):
            part_send[layer, src] = unstack_heads(parts[0], rows, head_dim).astype(BF16)

        def stages(after, s_after, now, s_now, w_now, before, w_before):
            tops, dens, parts = [], [], []
            interleave(score_of(after, s_after), exponent_steps(n_keys, s_now, w_now, tops, dens, LAG), values_of(w_before, parts))
            put_stats(now, tops, dens)
            put_part(before, parts)

        def send(src, copy):
            @pl.when(src != me)
            def _():
                copy(layer, src).start()

        phase(f'cross{layer}')

        def turn_body(turn, carry):
            first = turn * 2
            second, before, after = first + 1, lax.rem(first + group - 1, group), jnp.minimum(first + 2, group - 1)
            wait_queries(second)
            stages(second, scores_b, first, scores_a, weights_a, before, weights_b)
            send(first, stat_copy)

            @pl.when(turn > 0)
            def _():
                send(before, part_copy)

            @pl.when(turn < group // 2 - 1)
            def _():
                wait_queries(first + 2)
            stages(after, scores_a, second, scores_b, weights_b, first, weights_a)
            send(second, stat_copy)
            send(first, part_copy)
            return carry

        @pl.when(chip < mem_chips)
        def _():
            wait_queries(0)
            interleave(score_of(0, scores_a))
            lax.fori_loop(0, group // 2, turn_body, 0)
            parts = []
            interleave(values_of(weights_b, parts))
            put_part(group - 1, parts)
            send(group - 1, part_copy)
            part_recv[layer, me] = part_send[layer, me]
            stat_recv[layer, me] = stat_send[layer, me]
        phase(f'arrived{layer}')

        for src in range(mem_chips * CORES):
            @pl.when(src != me)
            def _():
                stat_arrival(layer, src).wait_recv()
                part_arrival(layer, src).wait_recv()

        phase(f'combine{layer}')
        factors = [None] * (mem_chips * CORES)
        for g in range(CORES):
            members = [c * CORES + g for c in range(mem_chips)]
            tops = [stat_recv[layer, i, 0:hpg] for i in members]
            dens = [stat_recv[layer, i, hpg:2 * hpg] for i in members]
            best = functools.reduce(jnp.maximum, tops)
            shares = [jnp.exp(t - best) for t in tops]
            total = functools.reduce(jnp.add, [s * d for s, d in zip(shares, dens)])
            for i, s in zip(members, shares):
                factors[i] = s / total
        packed = jnp.concatenate(factors + [jnp.zeros((128 - mem_chips * CORES * hpg, rows), F32)], axis=0)
        packed = jnp.transpose(packed)
        lane_group = lane_groups(rows, half, head_dim)
        attended = []
        for g in range(CORES):
            total = jnp.zeros((rows, half), F32)
            for c in range(mem_chips):
                i = c * CORES + g
                factor = jnp.zeros((rows, half), F32)
                for h in range(hpg):
                    factor = jnp.where(lane_group == h, packed[:, i * hpg + h:i * hpg + h + 1], factor)
                total = total + part_recv[layer, i].astype(F32) * factor
            attended.append(total.astype(BF16))
        attended = jnp.concatenate(attended, axis=-1)
        phase(f'co{layer}')
        weight_copy('cross_o', layer).wait()
        hidden = (hid[...].astype(F32) + mm(attended, w['cross_o'][layer])).astype(BF16)

        phase(f'mlp{layer}')
        normed = rms_norm(hidden, norm_mlp[layer:layer + 1, :])
        for name in ('mlp_gate', 'mlp_up', 'mlp_down'):
            weight_copy(name, layer).wait()
        update = None
        for start in range(0, w['mlp_gate'].shape[-1], FF_BLOCK):
            cols = slice(start, start + FF_BLOCK)
            gate = mm(normed, w['mlp_gate'][layer, :, cols])
            up = mm(normed, w['mlp_up'][layer, :, cols])
            act = (gate * jax.nn.sigmoid(gate) * up).astype(BF16)
            part = mm(act, w['mlp_down'][layer, cols, :])
            update = part if update is None else update + part
        hidden = (hidden.astype(F32) + update).astype(BF16)
        hid[...] = hidden

    phase('end')
    out_ref[...] = hid[...]

    @pl.when(chip < mem_chips)
    def _():
        mem_out.wait_send()
    for layer in range(n_layers):
        for condition, copy in x_sends(layer):
            pl.when(condition)(copy.wait_send)
        for turn in range(chips - 1):
            @pl.when(turn < chip)
            def _():
                for part in (0, 1):
                    x_relay_copy(layer, turn, part).wait_send()
        for d in range(1, chips):
            @pl.when(lax.rem(chip + d, chips) < mem_chips)
            def _():
                for k in range(CORES):
                    q_copy(layer, d, k).wait_send()

        @pl.when(chip < mem_chips)
        def _():
            q_to_partner(layer).wait_send()
            for step in range(1, group):
                part_copy(layer, lax.rem(me + step, group)).wait_send()
                stat_copy(layer, lax.rem(me + step, group)).wait_send()
    phase(None)


def solution(mesh):
    group = mesh.shape['sp']
    row_spec = P(('dp', 'sp'), None)

    def local_step(hidden, memory, mem_len, norm_self, norm_cross, norm_mlp, self_q, self_k, self_v, self_o, cross_q, cross_k, cross_v, cross_o, mlp_gate, mlp_up, mlp_down):
        rows, width = hidden.shape
        mem_rows = memory.shape[0]
        n_layers, n_heads, head_dim = self_o.shape[:3]
        inner = n_heads * head_dim
        half = inner // CORES
        hpg = half // head_dim
        all_keys = max(group * rows, CORES * mem_rows)
        weights = dict(
            self_q=self_q, self_k=self_k, self_v=self_v, self_o=self_o.reshape(n_layers, inner, width), cross_k=cross_k, cross_v=cross_v,
            cross_q=cross_q, cross_o=cross_o.reshape(n_layers, inner, width), mlp_gate=mlp_gate, mlp_up=mlp_up, mlp_down=mlp_down)
        w_scratch = [
            pltpu.VMEM((n_layers, width, half) if name in HALVED else weights[name].shape, BF16) for name in WEIGHTS]
        dma = pltpu.SemaphoreType.DMA
        vmem = pl.BlockSpec(memory_space=pltpu.VMEM)
        hbm = pl.BlockSpec(memory_space=pl.ANY)
        return pl.pallas_call(
            functools.partial(kernel, group, n_layers, head_dim),
            out_shape=jax.ShapeDtypeStruct((rows, width), BF16),
            in_specs=[vmem, hbm, pl.BlockSpec(memory_space=pltpu.SMEM), vmem, vmem, vmem] + [hbm] * len(WEIGHTS),
            out_specs=vmem,
            scratch_shapes=w_scratch + [
                pltpu.VMEM((CORES, mem_rows, width), BF16),
                pltpu.VMEM((n_layers, group, rows, width), BF16),
                pltpu.VMEM((group, rows, width), BF16),
                pltpu.VMEM((group, rows, width), BF16),
                pltpu.VMEM((n_layers, CORES * mem_rows, half), BF16),
                pltpu.VMEM((n_layers, CORES * mem_rows, half), BF16),
                pltpu.VMEM((n_layers, CORES, rows, half), BF16),
                pltpu.VMEM((n_layers, group, rows, half), BF16),
                pltpu.VMEM((n_layers, group, rows, half), BF16),
                pltpu.VMEM((n_layers, group, rows, half), BF16),
                pltpu.VMEM((n_layers, group, 2 * hpg, rows), F32),
                pltpu.VMEM((n_layers, group, 2 * hpg, rows), F32),
                pltpu.VMEM((rows, width), BF16),
                pltpu.VMEM((hpg * rows, all_keys), F32),
                pltpu.VMEM((hpg * rows, all_keys), F32),
                pltpu.VMEM((hpg * rows, all_keys), BF16),
                pltpu.VMEM((hpg * rows, all_keys), BF16),
                dma((len(WEIGHTS), n_layers)),
                dma((1,)), dma((1,)), dma((1,)),
                dma((n_layers, group // CORES, 2)), dma((n_layers, group // CORES - 1, 2)), dma((n_layers, group, 2)),
                dma((n_layers, group)), dma((n_layers, group)),
                dma((n_layers, group)), dma((n_layers, group)),
                dma((n_layers, group)), dma((n_layers, group)),
            ],
            compiler_params=pltpu.CompilerParams(collective_id=0, has_side_effects=True, vmem_limit_bytes=60 * 1024 * 1024),
        )(hidden, memory, mem_len, norm_self, norm_cross, norm_mlp, *[weights[name] for name in WEIGHTS])

    return jax.shard_map(local_step, mesh=mesh, in_specs=(row_spec, row_spec, P('dp')) + (P(),) * 14, out_specs=row_spec, check_vma=False)
```

```python
import functools

import jax
import jax.numpy as jnp
from jax import lax
from jax.experimental import pallas as pl
from jax.experimental.pallas import tpu as pltpu
from jax.sharding import PartitionSpec as P

EPS = 1e-6
NEG_BIG = -1e30
CORES = 2
KEY_BLOCK = 512
FF_BLOCK = 512
MEM_BLOCK = 256
ROW_BLOCK = 64
LAG = 1
LOWEST = -3.4e38
MEM_LEN_MAX = 6144
F32 = jnp.float32
BF16 = jnp.bfloat16
MESH = pl.DeviceIdType.MESH
WEIGHTS = ('self_q', 'self_k', 'self_v', 'self_o', 'cross_k', 'cross_v', 'cross_q', 'cross_o', 'mlp_gate', 'mlp_up', 'mlp_down')
HALVED = ('cross_k', 'cross_v')


def rms_norm(hidden, gain_row):
    hidden32 = hidden.astype(F32)
    inv_rms = lax.rsqrt(jnp.mean(hidden32 * hidden32, axis=-1, keepdims=True) + EPS)
    return (hidden32 * inv_rms * gain_row.astype(F32)).astype(BF16)


def mm(a, b):
    return jnp.dot(a, b, preferred_element_type=F32)


def mm_t(a, b):
    return lax.dot_general(a, b, (((1,), (1,)), ((), ())), preferred_element_type=F32)


def lane_groups(rows, lanes, head_dim):
    return lax.broadcasted_iota(jnp.int32, (rows, lanes), 1) // head_dim


def stack_heads(q, head_dim, scale):
    rows, lanes = q.shape
    scaled = q.astype(F32) * scale
    group = lane_groups(rows, lanes, head_dim)
    return jnp.concatenate([jnp.where(group == h, scaled, 0.0).astype(BF16) for h in range(lanes // head_dim)], axis=0)


def score_steps(q_stack, key_block, n_keys, allowed, scores_ref):
    def step(start):
        scores = mm_t(q_stack, key_block(start))
        scores_ref[:, start:start + KEY_BLOCK] = jnp.where(allowed(start), scores, NEG_BIG)
    return [functools.partial(step, start) for start in range(0, n_keys, KEY_BLOCK)]


def exponent_steps(n_keys, scores_ref, weights_ref, tops, dens, lag=0):
    sums = []

    def step(row):
        at = slice(row, row + ROW_BLOCK)
        tiles = [scores_ref[at, lane:lane + 128] for lane in range(0, n_keys, 128)]
        if lag and len(sums) >= lag:
            tiles.insert(0, jnp.minimum(sums[-lag], LOWEST))
        top = jnp.max(functools.reduce(jnp.maximum, tiles), axis=-1, keepdims=True)
        run_sum = None
        for lane in range(0, n_keys, 256):
            weights = jnp.exp(scores_ref[at, lane:lane + 256] - top)
            weights_ref[at, lane:lane + 256] = weights.astype(BF16)
            pair = weights[:, :128] + weights[:, 128:]
            run_sum = pair if run_sum is None else run_sum + pair
        sums.append(run_sum)
        tops.append(top)
        dens.append(jnp.sum(run_sum, axis=-1, keepdims=True))
    return [functools.partial(step, row) for row in range(0, scores_ref.shape[0], ROW_BLOCK)]


def value_steps(value_block, n_keys, weights_ref, parts):
    def step(start):
        part = mm(weights_ref[:, start:start + KEY_BLOCK], value_block(start))
        parts[:] = [part if not parts else parts[0] + part]
    return [functools.partial(step, start) for start in range(0, n_keys, KEY_BLOCK)]


def interleave(*lists):
    order = sorted(((i + 0.5) / len(steps), n, i) for n, steps in enumerate(lists) for i in range(len(steps)))
    for _, n, i in order:
        lists[n][i]()


def unstack_heads(stacked, rows, head_dim):
    lanes = stacked.shape[1]
    group = lane_groups(rows, lanes, head_dim)
    out = stacked[:rows]
    for h in range(1, lanes // head_dim):
        out = jnp.where(group == h, stacked[h * rows:(h + 1) * rows], out)
    return out


class Phase:
    def __init__(self):
        self.cur = None

    def __call__(self, name):
        if self.cur is not None:
            self.cur.__exit__(None, None, None)
        self.cur = jax.named_scope(name) if name else None
        if self.cur is not None:
            self.cur.__enter__()


def kernel(group, n_layers, head_dim, *refs):
    n_w = len(WEIGHTS)
    hidden_ref, memory_ref, mem_len_ref, norm_self, norm_cross, norm_mlp = refs[:6]
    w_hbm = dict(zip(WEIGHTS, refs[6:6 + n_w]))
    out_ref = refs[6 + n_w]
    scratch = refs[7 + n_w:]
    w = dict(zip(WEIGHTS, scratch[:n_w]))
    (mem_v, x_all, k_all, v_all, mem_k, mem_vals, q_send, q_all, part_send, part_recv, stat_send, stat_recv, hid, scores_a, scores_b, weights_a, weights_b,
     w_sem, mem_sem, mem_send, mem_recv, x_send, x_relay, x_recv, q_ssem, q_rsem, p_ssem, p_rsem, s_ssem, s_rsem) = scratch[n_w:]

    rows, width = hidden_ref.shape
    mem_rows = memory_ref.shape[0]
    chips = group // CORES
    mem_chips = -(-MEM_LEN_MAX // (CORES * mem_rows))
    half = q_send.shape[-1]
    hpg = half // head_dim
    scale = head_dim ** -0.5
    me = lax.axis_index('sp')
    chip, core = me // CORES, me % CORES
    partner = chip * CORES + (1 - core)

    def remote(src, dst, ssem, rsem, dev):
        return pltpu.make_async_remote_copy(src_ref=src, dst_ref=dst, send_sem=ssem, recv_sem=rsem, device_id={'sp': dev}, device_id_type=MESH)

    def weight_copy(name, layer):
        src = w_hbm[name].at[layer]
        if name in HALVED:
            src = w_hbm[name].at[layer, :, pl.ds(pl.multiple_of(core * half, half), half)]
        return pltpu.make_async_copy(src, w[name].at[layer], w_sem.at[WEIGHTS.index(name), layer])

    phase = Phase()
    phase('start')
    mem_copy = pltpu.make_async_copy(memory_ref, mem_v.at[core], mem_sem.at[0])

    for name in ('self_q', 'self_k', 'self_v'):
        weight_copy(name, 0).start()
    mem_copy.start()
    for layer in range(n_layers):
        for name in HALVED:
            weight_copy(name, layer).start()

    def start_weights(layer, names):
        for name in names:
            weight_copy(name, layer).start()

    phase('barrier')
    barrier = pltpu.get_barrier_semaphore()
    for step in range(1, group):
        pl.semaphore_signal(barrier, inc=1, device_id={'sp': lax.rem(me + step, group)}, device_id_type=MESH)
    pl.semaphore_wait(barrier, group - 1)

    top_chip = chip // (chips - 1)
    half_rows = rows // 2

    def x_copy(layer, src, part, ssem, dst):
        at = x_all.at[layer, src, pl.ds(pl.multiple_of(part * half_rows, half_rows), half_rows)]
        return remote(at, at, ssem, x_recv.at[layer, src, part], dst)

    def x_sends(layer):
        up = me + CORES
        across = (chips - 1) * CORES + core
        send = x_send.at
        return [
            (core == 0, x_copy(layer, me, 0, send[layer, 4], partner)),
            (core == 0, x_copy(layer, me, 1, send[layer, 5], partner)),
            (chip == 1, x_copy(layer, me, 1, send[layer, 2], core)),
            (chip < chips - 1, x_copy(layer, me, 0, send[layer, 0], up)),
            (chip == 0, x_copy(layer, me, 1, send[layer, 2], across)),
            (chip < chips - 1, x_copy(layer, me, 1, send[layer, 1], up)),
            (chip == 0, x_copy(layer, me, 0, send[layer, 3], across)),
        ]

    def x_source(turn):
        return top_chip * (turn * 2 - 3 * (turn // 2)) + (1 - top_chip) * (chip - 1 - turn)

    def x_forward(layer):
        src = x_source(0) * CORES + core
        return x_copy(layer, src, top_chip, x_send.at[layer, 6], me + CORES - 2 * CORES * top_chip)

    def x_forward_first(layer):
        return x_copy(layer, CORES + core, 1, x_send.at[layer, 6], (chips - 1) * CORES + core)

    def x_relay_copy(layer, turn, part):
        return x_copy(layer, x_source(turn) * CORES + core, part, x_relay.at[layer, turn, part], partner)

    def x_arrival(layer, src, part):
        return x_copy(layer, src, part, x_send.at[layer, 0], partner)

    def q_copy(layer, d, k):
        dst = lax.rem(chip + d, chips) * CORES + k
        return remote(q_send.at[layer, k], q_all.at[layer, me], q_ssem.at[layer, d * CORES + k], q_rsem.at[layer, me], dst)

    def q_to_partner(layer):
        return remote(q_send.at[layer, 1 - core], q_all.at[layer, me], q_ssem.at[layer, 0], q_rsem.at[layer, me], partner)

    def q_arrival(layer, src):
        return remote(q_send.at[layer, 0], q_all.at[layer, src], q_ssem.at[layer, 0], q_rsem.at[layer, src], partner)

    def part_copy(layer, src):
        return remote(part_send.at[layer, src], part_recv.at[layer, me], p_ssem.at[layer, src], p_rsem.at[layer, me], src)

    def stat_copy(layer, src):
        return remote(stat_send.at[layer, src], stat_recv.at[layer, me], s_ssem.at[layer, src], s_rsem.at[layer, me], src)

    def part_arrival(layer, src):
        return remote(part_send.at[layer, src], part_recv.at[layer, src], p_ssem.at[layer, src], p_rsem.at[layer, src], partner)

    def stat_arrival(layer, src):
        return remote(stat_send.at[layer, src], stat_recv.at[layer, src], s_ssem.at[layer, src], s_rsem.at[layer, src], partner)

    mem_out = remote(mem_v.at[core], mem_v.at[core], mem_send.at[0], mem_recv.at[0], partner)
    mem_in = remote(mem_v.at[1 - core], mem_v.at[1 - core], mem_send.at[0], mem_recv.at[0], partner)

    def project_memory(slot, layer):
        def body(i, carry):
            at = pl.ds(pl.multiple_of(i * MEM_BLOCK, MEM_BLOCK), MEM_BLOCK)
            to = pl.ds(pl.multiple_of(slot * mem_rows + i * MEM_BLOCK, MEM_BLOCK), MEM_BLOCK)
            block = mem_v[slot, at, :]
            mem_k[layer, to, :] = mm(block, w['cross_k'][layer]).astype(BF16)
            mem_vals[layer, to, :] = mm(block, w['cross_v'][layer]).astype(BF16)
            return carry
        lax.fori_loop(0, mem_rows // MEM_BLOCK, body, 0)

    phase('zero')
    hid[...] = hidden_ref[...]
    for src in range(group):
        @pl.when(src > me)
        def _():
            k_all[src] = jnp.zeros((rows, width), BF16)
            v_all[src] = jnp.zeros((rows, width), BF16)

    for layer in range(n_layers):
        phase(f'xnorm{layer}')
        x_all[layer, me] = rms_norm(hid[...], norm_self[layer:layer + 1, :])
        for condition, copy in x_sends(layer):
            pl.when(condition)(copy.start)
        if layer == 0:
            start_weights(0, ('self_o', 'cross_q', 'cross_o'))

        for name in ('self_q', 'self_k', 'self_v'):
            weight_copy(name, layer).wait()

        def project_rows(src):
            block = x_all[layer, src]
            k_all[src] = mm(block, w['self_k'][layer]).astype(BF16)
            v_all[src] = mm(block, w['self_v'][layer]).astype(BF16)

        phase(f'ownproj{layer}')
        project_rows(me)
        queries = mm(x_all[layer, me], w['self_q'][layer]).astype(BF16)

        phase(f'memproj{layer}')
        if layer == 0:
            mem_copy.wait()
            for other in range(n_layers):
                for name in HALVED:
                    weight_copy(name, other).wait()

            @pl.when(chip < mem_chips)
            def _():
                mem_out.start()
                for other in range(n_layers):
                    project_memory(core, other)
        phase(f'xwait{layer}')

        @pl.when(chip == 0)
        def _():
            x_arrival(layer, CORES + core, 1).wait_recv()
            x_forward_first(layer).start()

        for turn in range(chips - 1):
            @pl.when(turn < chip)
            def _():
                src = x_source(turn) * CORES + core
                first = top_chip if turn == 0 else 0
                for i, part in enumerate((first, 1 - first)):
                    x_arrival(layer, src, part).wait_recv()
                    if turn == 0 and i == 0:
                        pl.when(chip > 0)(x_forward(layer).start)
                    x_relay_copy(layer, turn, part).start()
                project_rows(src)

        phase(f'memproj2{layer}')

        @pl.when(chip < mem_chips)
        def _():
            if layer == 0:
                mem_in.wait_recv()
            project_memory(1 - core, layer)

        phase(f'xwait2{layer}')
        @pl.when(core == 1)
        def _():
            for part in (0, 1):
                x_arrival(layer, partner, part).wait_recv()
            project_rows(partner)

        for turn in range(chips - 1):
            @pl.when(turn < chip)
            def _():
                src = x_source(turn) * CORES + (1 - core)
                for part in (0, 1):
                    x_arrival(layer, src, part).wait_recv()
                project_rows(src)

        phase(f'selfatt{layer}')
        all_rows = group * rows
        query_at = me * rows + lax.rem(lax.broadcasted_iota(jnp.int32, (hpg * rows, KEY_BLOCK), 0), rows)
        key_at = lax.broadcasted_iota(jnp.int32, (hpg * rows, KEY_BLOCK), 1)
        per_block = KEY_BLOCK // rows
        stores = ((scores_a, weights_a), (scores_b, weights_b))
        tops, dens, parts = [[], []], [[], []], [[], []]

        def self_steps(g):
            lanes = slice(g * half, (g + 1) * half)
            s_ref, w_ref = stores[g]
            return (
                score_steps(stack_heads(queries[:, lanes], head_dim, scale),
                            lambda start: k_all[start // rows:start // rows + per_block, :, lanes].reshape(KEY_BLOCK, half),
                            all_rows, lambda start: key_at + start <= query_at, s_ref),
                exponent_steps(all_rows, s_ref, w_ref, tops[g], dens[g]),
                value_steps(lambda start: v_all[start // rows:start // rows + per_block, :, lanes].reshape(KEY_BLOCK, half),
                            all_rows, w_ref, parts[g]))

        steps = [self_steps(g) for g in range(CORES)]
        interleave(steps[0][0])
        interleave(steps[0][1], steps[1][0])
        interleave(steps[0][2], steps[1][1])
        interleave(steps[1][2])
        attended = [unstack_heads(parts[g][0] / jnp.concatenate(dens[g], axis=0), rows, head_dim).astype(BF16) for g in range(CORES)]
        attended = jnp.concatenate(attended, axis=-1)
        phase(f'oproj{layer}')
        weight_copy('self_o', layer).wait()
        hidden = (hid[...].astype(F32) + mm(attended, w['self_o'][layer])).astype(BF16)
        hid[...] = hidden

        phase(f'qproj{layer}')
        weight_copy('cross_q', layer).wait()
        queries = mm(rms_norm(hidden, norm_cross[layer:layer + 1, :]), w['cross_q'][layer]).astype(BF16)
        for g in range(CORES):
            q_send[layer, g] = queries[:, g * half:(g + 1) * half]
        q_order = [(d, k) for d in (1, 3, 2) if d < chips for k in range(CORES)]

        @pl.when(chip < mem_chips)
        def _():
            q_to_partner(layer).start()
        for d, k in q_order:
            @pl.when(lax.rem(chip + d, chips) < mem_chips)
            def _():
                q_copy(layer, d, k).start()
        q_all[layer, me] = q_send[layer, core]
        later = []
        if layer == 0:
            later = [(0, name) for name in ('mlp_gate', 'mlp_up', 'mlp_down')]
            later += [(other, name) for other in range(1, n_layers) for name in WEIGHTS if name not in HALVED]

        mem_at = chip * (CORES * mem_rows) + lax.broadcasted_iota(jnp.int32, (1, KEY_BLOCK), 1)
        n_keys = CORES * mem_rows

        def wait_queries(src):
            @pl.when(src != me)
            def _():
                q_arrival(layer, src).wait_recv()

        def score_of(src, scores_ref):
            return score_steps(stack_heads(q_all[layer, src], head_dim, scale), lambda start: mem_k[layer, start:start + KEY_BLOCK, :], n_keys,
                               lambda start: mem_at + start < mem_len_ref[0], scores_ref)

        def put_stats(src, tops, dens):
            top, den = jnp.concatenate(tops, axis=0), jnp.concatenate(dens, axis=0)
            lane = lax.broadcasted_iota(jnp.int32, (rows, 128), 1)
            stats = jnp.zeros((rows, 128), F32)
            for h in range(hpg):
                stats = jnp.where(lane == h, top[h * rows:(h + 1) * rows], stats)
                stats = jnp.where(lane == hpg + h, den[h * rows:(h + 1) * rows], stats)
            stat_send[layer, src] = jnp.transpose(stats)[:2 * hpg]

        def values_of(weights_ref, parts):
            return value_steps(lambda start: mem_vals[layer, start:start + KEY_BLOCK, :], n_keys, weights_ref, parts)

        def put_part(src, parts):
            part_send[layer, src] = unstack_heads(parts[0], rows, head_dim).astype(BF16)

        def stages(after, s_after, now, s_now, w_now, before, w_before):
            tops, dens, parts = [], [], []
            interleave(score_of(after, s_after), exponent_steps(n_keys, s_now, w_now, tops, dens, LAG), values_of(w_before, parts))
            put_stats(now, tops, dens)
            put_part(before, parts)

        def send(src, copy):
            @pl.when(src != me)
            def _():
                copy(layer, src).start()

        phase(f'cross{layer}')

        def turn_body(turn, carry):
            first = turn * 2
            for i in range(group // 2):
                if later:
                    @pl.when(turn == i)
                    def _():
                        for other, name in later[i::group // 2]:
                            weight_copy(name, other).start()
            second, before, after = first + 1, lax.rem(first + group - 1, group), jnp.minimum(first + 2, group - 1)
            wait_queries(second)
            stages(second, scores_b, first, scores_a, weights_a, before, weights_b)
            send(first, stat_copy)

            @pl.when(turn > 0)
            def _():
                send(before, part_copy)

            @pl.when(turn < group // 2 - 1)
            def _():
                wait_queries(first + 2)
            stages(after, scores_a, second, scores_b, weights_b, first, weights_a)
            send(second, stat_copy)
            send(first, part_copy)
            return carry

        @pl.when(chip < mem_chips)
        def _():
            wait_queries(0)
            interleave(score_of(0, scores_a))
            lax.fori_loop(0, group // 2, turn_body, 0)
            parts = []
            interleave(values_of(weights_b, parts))
            put_part(group - 1, parts)
            send(group - 1, part_copy)
            part_recv[layer, me] = part_send[layer, me]
            stat_recv[layer, me] = stat_send[layer, me]

        @pl.when(chip >= mem_chips)
        def _():
            for other, name in later:
                weight_copy(name, other).start()
        phase(f'arrived{layer}')

        for src in range(mem_chips * CORES):
            @pl.when(src != me)
            def _():
                stat_arrival(layer, src).wait_recv()
                part_arrival(layer, src).wait_recv()

        phase(f'combine{layer}')
        factors = [None] * (mem_chips * CORES)
        for g in range(CORES):
            members = [c * CORES + g for c in range(mem_chips)]
            tops = [stat_recv[layer, i, 0:hpg] for i in members]
            dens = [stat_recv[layer, i, hpg:2 * hpg] for i in members]
            best = functools.reduce(jnp.maximum, tops)
            shares = [jnp.exp(t - best) for t in tops]
            total = functools.reduce(jnp.add, [s * d for s, d in zip(shares, dens)])
            for i, s in zip(members, shares):
                factors[i] = s / total
        packed = jnp.concatenate(factors + [jnp.zeros((128 - mem_chips * CORES * hpg, rows), F32)], axis=0)
        packed = jnp.transpose(packed)
        lane_group = lane_groups(rows, half, head_dim)
        attended = []
        for g in range(CORES):
            total = jnp.zeros((rows, half), F32)
            for c in range(mem_chips):
                i = c * CORES + g
                factor = jnp.zeros((rows, half), F32)
                for h in range(hpg):
                    factor = jnp.where(lane_group == h, packed[:, i * hpg + h:i * hpg + h + 1], factor)
                total = total + part_recv[layer, i].astype(F32) * factor
            attended.append(total.astype(BF16))
        attended = jnp.concatenate(attended, axis=-1)
        phase(f'co{layer}')
        weight_copy('cross_o', layer).wait()
        hidden = (hid[...].astype(F32) + mm(attended, w['cross_o'][layer])).astype(BF16)

        phase(f'mlp{layer}')
        normed = rms_norm(hidden, norm_mlp[layer:layer + 1, :])
        for name in ('mlp_gate', 'mlp_up', 'mlp_down'):
            weight_copy(name, layer).wait()
        update = None
        for start in range(0, w['mlp_gate'].shape[-1], FF_BLOCK):
            cols = slice(start, start + FF_BLOCK)
            gate = mm(normed, w['mlp_gate'][layer, :, cols])
            up = mm(normed, w['mlp_up'][layer, :, cols])
            act = (gate * jax.nn.sigmoid(gate) * up).astype(BF16)
            part = mm(act, w['mlp_down'][layer, cols, :])
            update = part if update is None else update + part
        hidden = (hidden.astype(F32) + update).astype(BF16)
        hid[...] = hidden

    phase('end')
    out_ref[...] = hid[...]

    @pl.when(chip < mem_chips)
    def _():
        mem_out.wait_send()
    for layer in range(n_layers):
        for condition, copy in x_sends(layer):
            pl.when(condition)(copy.wait_send)
        pl.when(chip == 0)(x_forward_first(layer).wait_send)
        pl.when(chip > 0)(x_forward(layer).wait_send)
        for turn in range(chips - 1):
            @pl.when(turn < chip)
            def _():
                for part in (0, 1):
                    x_relay_copy(layer, turn, part).wait_send()
        for d in range(1, chips):
            @pl.when(lax.rem(chip + d, chips) < mem_chips)
            def _():
                for k in range(CORES):
                    q_copy(layer, d, k).wait_send()

        @pl.when(chip < mem_chips)
        def _():
            q_to_partner(layer).wait_send()
            for step in range(1, group):
                part_copy(layer, lax.rem(me + step, group)).wait_send()
                stat_copy(layer, lax.rem(me + step, group)).wait_send()
    phase(None)


def solution(mesh):
    group = mesh.shape['sp']
    row_spec = P(('dp', 'sp'), None)

    def local_step(hidden, memory, mem_len, norm_self, norm_cross, norm_mlp, self_q, self_k, self_v, self_o, cross_q, cross_k, cross_v, cross_o, mlp_gate, mlp_up, mlp_down):
        rows, width = hidden.shape
        mem_rows = memory.shape[0]
        n_layers, n_heads, head_dim = self_o.shape[:3]
        inner = n_heads * head_dim
        half = inner // CORES
        hpg = half // head_dim
        all_keys = max(group * rows, CORES * mem_rows)
        weights = dict(
            self_q=self_q, self_k=self_k, self_v=self_v, self_o=self_o.reshape(n_layers, inner, width), cross_k=cross_k, cross_v=cross_v,
            cross_q=cross_q, cross_o=cross_o.reshape(n_layers, inner, width), mlp_gate=mlp_gate, mlp_up=mlp_up, mlp_down=mlp_down)
        w_scratch = [
            pltpu.VMEM((n_layers, width, half) if name in HALVED else weights[name].shape, BF16) for name in WEIGHTS]
        dma = pltpu.SemaphoreType.DMA
        vmem = pl.BlockSpec(memory_space=pltpu.VMEM)
        hbm = pl.BlockSpec(memory_space=pl.ANY)
        return pl.pallas_call(
            functools.partial(kernel, group, n_layers, head_dim),
            out_shape=jax.ShapeDtypeStruct((rows, width), BF16),
            in_specs=[vmem, hbm, pl.BlockSpec(memory_space=pltpu.SMEM), vmem, vmem, vmem] + [hbm] * len(WEIGHTS),
            out_specs=vmem,
            scratch_shapes=w_scratch + [
                pltpu.VMEM((CORES, mem_rows, width), BF16),
                pltpu.VMEM((n_layers, group, rows, width), BF16),
                pltpu.VMEM((group, rows, width), BF16),
                pltpu.VMEM((group, rows, width), BF16),
                pltpu.VMEM((n_layers, CORES * mem_rows, half), BF16),
                pltpu.VMEM((n_layers, CORES * mem_rows, half), BF16),
                pltpu.VMEM((n_layers, CORES, rows, half), BF16),
                pltpu.VMEM((n_layers, group, rows, half), BF16),
                pltpu.VMEM((n_layers, group, rows, half), BF16),
                pltpu.VMEM((n_layers, group, rows, half), BF16),
                pltpu.VMEM((n_layers, group, 2 * hpg, rows), F32),
                pltpu.VMEM((n_layers, group, 2 * hpg, rows), F32),
                pltpu.VMEM((rows, width), BF16),
                pltpu.VMEM((hpg * rows, all_keys), F32),
                pltpu.VMEM((hpg * rows, all_keys), F32),
                pltpu.VMEM((hpg * rows, all_keys), BF16),
                pltpu.VMEM((hpg * rows, all_keys), BF16),
                dma((len(WEIGHTS), n_layers)),
                dma((1,)), dma((1,)), dma((1,)),
                dma((n_layers, 7)), dma((n_layers, group // CORES - 1, 2)), dma((n_layers, group, 2)),
                dma((n_layers, group)), dma((n_layers, group)),
                dma((n_layers, group)), dma((n_layers, group)),
                dma((n_layers, group)), dma((n_layers, group)),
            ],
            compiler_params=pltpu.CompilerParams(collective_id=0, has_side_effects=True, vmem_limit_bytes=60 * 1024 * 1024),
        )(hidden, memory, mem_len, norm_self, norm_cross, norm_mlp, *[weights[name] for name in WEIGHTS])

    return jax.shard_map(local_step, mesh=mesh, in_specs=(row_spec, row_spec, P('dp')) + (P(),) * 14, out_specs=row_spec, check_vma=False)
```

```python
import functools

import jax
import jax.numpy as jnp
from jax import lax
from jax.experimental import pallas as pl
from jax.experimental.pallas import tpu as pltpu
from jax.sharding import PartitionSpec as P

EPS = 1e-6
NEG_BIG = -1e30
CORES = 2
KEY_BLOCK = 512
VALUE_BLOCK = 2048
FF_BLOCK = 512
MEM_BLOCK = 256
ROW_BLOCK = 64
LAG = 1
LOWEST = -3.4e38
MEM_LEN_MAX = 6144
F32 = jnp.float32
BF16 = jnp.bfloat16
MESH = pl.DeviceIdType.MESH
WEIGHTS = ('self_q', 'self_k', 'self_v', 'self_o', 'cross_k', 'cross_v', 'cross_q', 'cross_o', 'mlp_gate', 'mlp_up', 'mlp_down')
HALVED = ('cross_k', 'cross_v')


def rms_norm(hidden, gain_row):
    hidden32 = hidden.astype(F32)
    inv_rms = lax.rsqrt(jnp.mean(hidden32 * hidden32, axis=-1, keepdims=True) + EPS)
    return (hidden32 * inv_rms * gain_row.astype(F32)).astype(BF16)


def mm(a, b):
    return jnp.dot(a, b, preferred_element_type=F32)


def mm_t(a, b):
    return lax.dot_general(a, b, (((1,), (1,)), ((), ())), preferred_element_type=F32)


def lane_groups(rows, lanes, head_dim):
    return lax.broadcasted_iota(jnp.int32, (rows, lanes), 1) // head_dim


def stack_heads(q, head_dim, scale):
    rows, lanes = q.shape
    scaled = q.astype(F32) * scale
    group = lane_groups(rows, lanes, head_dim)
    return jnp.concatenate([jnp.where(group == h, scaled, 0.0).astype(BF16) for h in range(lanes // head_dim)], axis=0)


def score_steps(q_stack, key_block, n_keys, allowed, scores_ref):
    def step(start):
        scores = mm_t(q_stack, key_block(start))
        scores_ref[:, start:start + KEY_BLOCK] = jnp.where(allowed(start), scores, NEG_BIG)
    return [functools.partial(step, start) for start in range(0, n_keys, KEY_BLOCK)]


def exponent_steps(n_keys, scores_ref, weights_ref, tops, dens, lag=0):
    sums = []

    def step(row):
        at = slice(row, row + ROW_BLOCK)
        tiles = [scores_ref[at, lane:lane + 128] for lane in range(0, n_keys, 128)]
        if lag and len(sums) >= lag:
            tiles.insert(0, jnp.minimum(sums[-lag], LOWEST))
        top = jnp.max(functools.reduce(jnp.maximum, tiles), axis=-1, keepdims=True)
        run_sum = None
        for lane in range(0, n_keys, 256):
            weights = jnp.exp(scores_ref[at, lane:lane + 256] - top)
            weights_ref[at, lane:lane + 256] = weights.astype(BF16)
            pair = weights[:, :128] + weights[:, 128:]
            run_sum = pair if run_sum is None else run_sum + pair
        sums.append(run_sum)
        tops.append(top)
        dens.append(jnp.sum(run_sum, axis=-1, keepdims=True))
    return [functools.partial(step, row) for row in range(0, scores_ref.shape[0], ROW_BLOCK)]


def value_steps(value_block, n_keys, weights_ref, parts):
    def step(start):
        stop = min(start + VALUE_BLOCK, n_keys)
        part = mm(weights_ref[:, start:stop], value_block(start, stop))
        parts[:] = [part if not parts else parts[0] + part]
    return [functools.partial(step, start) for start in range(0, n_keys, VALUE_BLOCK)]


def interleave(*lists):
    order = sorted(((i + 0.5) / len(steps), n, i) for n, steps in enumerate(lists) for i in range(len(steps)))
    for _, n, i in order:
        lists[n][i]()


def unstack_heads(stacked, rows, head_dim):
    lanes = stacked.shape[1]
    group = lane_groups(rows, lanes, head_dim)
    out = stacked[:rows]
    for h in range(1, lanes // head_dim):
        out = jnp.where(group == h, stacked[h * rows:(h + 1) * rows], out)
    return out


class Phase:
    def __init__(self):
        self.cur = None

    def __call__(self, name):
        if self.cur is not None:
            self.cur.__exit__(None, None, None)
        self.cur = jax.named_scope(name) if name else None
        if self.cur is not None:
            self.cur.__enter__()


def kernel(group, n_layers, head_dim, *refs):
    n_w = len(WEIGHTS)
    hidden_ref, memory_ref, mem_len_ref, norm_self, norm_cross, norm_mlp = refs[:6]
    w_hbm = dict(zip(WEIGHTS, refs[6:6 + n_w]))
    out_ref = refs[6 + n_w]
    scratch = refs[7 + n_w:]
    w = dict(zip(WEIGHTS, scratch[:n_w]))
    (mem_v, x_all, k_all, v_all, mem_k, mem_vals, q_send, q_all, part_send, part_recv, stat_send, stat_recv, hid, scores_a, scores_b, weights_a, weights_b,
     w_sem, mem_sem, mem_send, mem_recv, x_send, x_relay, x_recv, q_ssem, q_rsem, p_ssem, p_rsem, s_ssem, s_rsem) = scratch[n_w:]

    rows, width = hidden_ref.shape
    mem_rows = memory_ref.shape[0]
    chips = group // CORES
    mem_chips = -(-MEM_LEN_MAX // (CORES * mem_rows))
    half = q_send.shape[-1]
    hpg = half // head_dim
    scale = head_dim ** -0.5
    me = lax.axis_index('sp')
    chip, core = me // CORES, me % CORES
    partner = chip * CORES + (1 - core)

    def remote(src, dst, ssem, rsem, dev):
        return pltpu.make_async_remote_copy(src_ref=src, dst_ref=dst, send_sem=ssem, recv_sem=rsem, device_id={'sp': dev}, device_id_type=MESH)

    def weight_copy(name, layer):
        src = w_hbm[name].at[layer]
        if name in HALVED:
            src = w_hbm[name].at[layer, :, pl.ds(pl.multiple_of(core * half, half), half)]
        return pltpu.make_async_copy(src, w[name].at[layer], w_sem.at[WEIGHTS.index(name), layer])

    phase = Phase()
    phase('start')
    mem_copy = pltpu.make_async_copy(memory_ref, mem_v.at[core], mem_sem.at[0])

    for name in ('self_q', 'self_k', 'self_v'):
        weight_copy(name, 0).start()
    mem_copy.start()
    for layer in range(n_layers):
        for name in HALVED:
            weight_copy(name, layer).start()

    def start_weights(layer, names):
        for name in names:
            weight_copy(name, layer).start()

    phase('barrier')
    barrier = pltpu.get_barrier_semaphore()
    for step in range(1, group):
        pl.semaphore_signal(barrier, inc=1, device_id={'sp': lax.rem(me + step, group)}, device_id_type=MESH)
    pl.semaphore_wait(barrier, group - 1)

    top_chip = chip // (chips - 1)
    half_rows = rows // 2

    def x_copy(layer, src, part, ssem, dst):
        at = x_all.at[layer, src, pl.ds(pl.multiple_of(part * half_rows, half_rows), half_rows)]
        return remote(at, at, ssem, x_recv.at[layer, src, part], dst)

    def x_sends(layer):
        up = me + CORES
        across = (chips - 1) * CORES + core
        send = x_send.at
        return [
            (core == 0, x_copy(layer, me, 0, send[layer, 4], partner)),
            (core == 0, x_copy(layer, me, 1, send[layer, 5], partner)),
            (chip == 1, x_copy(layer, me, 1, send[layer, 2], core)),
            (chip < chips - 1, x_copy(layer, me, 0, send[layer, 0], up)),
            (chip == 0, x_copy(layer, me, 1, send[layer, 2], across)),
            (chip < chips - 1, x_copy(layer, me, 1, send[layer, 1], up)),
            (chip == 0, x_copy(layer, me, 0, send[layer, 3], across)),
        ]

    def x_source(turn):
        return top_chip * (turn * 2 - 3 * (turn // 2)) + (1 - top_chip) * (chip - 1 - turn)

    def x_forward(layer):
        src = x_source(0) * CORES + core
        return x_copy(layer, src, top_chip, x_send.at[layer, 6], me + CORES - 2 * CORES * top_chip)

    def x_forward_first(layer):
        return x_copy(layer, CORES + core, 1, x_send.at[layer, 6], (chips - 1) * CORES + core)

    def x_relay_copy(layer, turn, part):
        return x_copy(layer, x_source(turn) * CORES + core, part, x_relay.at[layer, turn, part], partner)

    def x_arrival(layer, src, part):
        return x_copy(layer, src, part, x_send.at[layer, 0], partner)

    def q_copy(layer, d, k):
        dst = lax.rem(chip + d, chips) * CORES + k
        return remote(q_send.at[layer, k], q_all.at[layer, me], q_ssem.at[layer, d * CORES + k], q_rsem.at[layer, me], dst)

    def q_to_partner(layer):
        return remote(q_send.at[layer, 1 - core], q_all.at[layer, me], q_ssem.at[layer, 0], q_rsem.at[layer, me], partner)

    def q_arrival(layer, src):
        return remote(q_send.at[layer, 0], q_all.at[layer, src], q_ssem.at[layer, 0], q_rsem.at[layer, src], partner)

    def part_copy(layer, src):
        return remote(part_send.at[layer, src], part_recv.at[layer, me], p_ssem.at[layer, src], p_rsem.at[layer, me], src)

    def stat_copy(layer, src):
        return remote(stat_send.at[layer, src], stat_recv.at[layer, me], s_ssem.at[layer, src], s_rsem.at[layer, me], src)

    def part_arrival(layer, src):
        return remote(part_send.at[layer, src], part_recv.at[layer, src], p_ssem.at[layer, src], p_rsem.at[layer, src], partner)

    def stat_arrival(layer, src):
        return remote(stat_send.at[layer, src], stat_recv.at[layer, src], s_ssem.at[layer, src], s_rsem.at[layer, src], partner)

    mem_out = remote(mem_v.at[core], mem_v.at[core], mem_send.at[0], mem_recv.at[0], partner)
    mem_in = remote(mem_v.at[1 - core], mem_v.at[1 - core], mem_send.at[0], mem_recv.at[0], partner)

    def project_memory(slot, layer):
        def body(i, carry):
            at = pl.ds(pl.multiple_of(i * MEM_BLOCK, MEM_BLOCK), MEM_BLOCK)
            to = pl.ds(pl.multiple_of(slot * mem_rows + i * MEM_BLOCK, MEM_BLOCK), MEM_BLOCK)
            block = mem_v[slot, at, :]
            mem_k[layer, to, :] = mm(block, w['cross_k'][layer]).astype(BF16)
            mem_vals[layer, to, :] = mm(block, w['cross_v'][layer]).astype(BF16)
            return carry
        lax.fori_loop(0, mem_rows // MEM_BLOCK, body, 0)

    phase('zero')
    hid[...] = hidden_ref[...]
    for src in range(group):
        @pl.when(src > me)
        def _():
            k_all[src] = jnp.zeros((rows, width), BF16)
            v_all[src] = jnp.zeros((rows, width), BF16)

    for layer in range(n_layers):
        phase(f'xnorm{layer}')
        x_all[layer, me] = rms_norm(hid[...], norm_self[layer:layer + 1, :])
        for condition, copy in x_sends(layer):
            pl.when(condition)(copy.start)
        if layer == 0:
            start_weights(0, ('self_o', 'cross_q', 'cross_o'))

        for name in ('self_q', 'self_k', 'self_v'):
            weight_copy(name, layer).wait()

        def project_rows(src):
            block = x_all[layer, src]
            k_all[src] = mm(block, w['self_k'][layer]).astype(BF16)
            v_all[src] = mm(block, w['self_v'][layer]).astype(BF16)

        phase(f'ownproj{layer}')
        project_rows(me)
        queries = mm(x_all[layer, me], w['self_q'][layer]).astype(BF16)

        phase(f'memproj{layer}')
        if layer == 0:
            mem_copy.wait()
            for other in range(n_layers):
                for name in HALVED:
                    weight_copy(name, other).wait()

            @pl.when(chip < mem_chips)
            def _():
                mem_out.start()
                for other in range(n_layers):
                    project_memory(core, other)
        phase(f'xwait{layer}')

        @pl.when(chip == 0)
        def _():
            x_arrival(layer, CORES + core, 1).wait_recv()
            x_forward_first(layer).start()

        for turn in range(chips - 1):
            @pl.when(turn < chip)
            def _():
                src = x_source(turn) * CORES + core
                first = top_chip if turn == 0 else 0
                for i, part in enumerate((first, 1 - first)):
                    x_arrival(layer, src, part).wait_recv()
                    if turn == 0 and i == 0:
                        pl.when(chip > 0)(x_forward(layer).start)
                    x_relay_copy(layer, turn, part).start()
                project_rows(src)

        phase(f'memproj2{layer}')

        @pl.when(chip < mem_chips)
        def _():
            if layer == 0:
                mem_in.wait_recv()
            project_memory(1 - core, layer)

        phase(f'xwait2{layer}')
        @pl.when(core == 1)
        def _():
            for part in (0, 1):
                x_arrival(layer, partner, part).wait_recv()
            project_rows(partner)

        for turn in range(chips - 1):
            @pl.when(turn < chip)
            def _():
                src = x_source(turn) * CORES + (1 - core)
                for part in (0, 1):
                    x_arrival(layer, src, part).wait_recv()
                project_rows(src)

        phase(f'selfatt{layer}')
        all_rows = group * rows
        query_at = me * rows + lax.rem(lax.broadcasted_iota(jnp.int32, (hpg * rows, KEY_BLOCK), 0), rows)
        key_at = lax.broadcasted_iota(jnp.int32, (hpg * rows, KEY_BLOCK), 1)
        per_block = KEY_BLOCK // rows
        stores = ((scores_a, weights_a), (scores_b, weights_b))
        tops, dens, parts = [[], []], [[], []], [[], []]

        def self_steps(g):
            lanes = slice(g * half, (g + 1) * half)
            s_ref, w_ref = stores[g]
            return (
                score_steps(stack_heads(queries[:, lanes], head_dim, scale),
                            lambda start: k_all[start // rows:start // rows + per_block, :, lanes].reshape(KEY_BLOCK, half),
                            all_rows, lambda start: key_at + start <= query_at, s_ref),
                exponent_steps(all_rows, s_ref, w_ref, tops[g], dens[g]),
                value_steps(lambda start, stop: v_all[start // rows:stop // rows, :, lanes].reshape(stop - start, half),
                            all_rows, w_ref, parts[g]))

        steps = [self_steps(g) for g in range(CORES)]
        interleave(steps[0][0])
        interleave(steps[0][1], steps[1][0])
        interleave(steps[0][2], steps[1][1])
        interleave(steps[1][2])
        attended = [unstack_heads(parts[g][0] / jnp.concatenate(dens[g], axis=0), rows, head_dim).astype(BF16) for g in range(CORES)]
        attended = jnp.concatenate(attended, axis=-1)
        phase(f'oproj{layer}')
        weight_copy('self_o', layer).wait()
        hidden = (hid[...].astype(F32) + mm(attended, w['self_o'][layer])).astype(BF16)
        hid[...] = hidden

        phase(f'qproj{layer}')
        weight_copy('cross_q', layer).wait()
        queries = mm(rms_norm(hidden, norm_cross[layer:layer + 1, :]), w['cross_q'][layer]).astype(BF16)
        for g in range(CORES):
            q_send[layer, g] = queries[:, g * half:(g + 1) * half]
        q_order = [(d, k) for d in (1, 3, 2) if d < chips for k in range(CORES)]

        @pl.when(chip < mem_chips)
        def _():
            q_to_partner(layer).start()
        for d, k in q_order:
            @pl.when(lax.rem(chip + d, chips) < mem_chips)
            def _():
                q_copy(layer, d, k).start()
        q_all[layer, me] = q_send[layer, core]
        later = []
        if layer == 0:
            later = [(0, name) for name in ('mlp_gate', 'mlp_up', 'mlp_down')]
            later += [(other, name) for other in range(1, n_layers) for name in WEIGHTS if name not in HALVED]

        mem_at = chip * (CORES * mem_rows) + lax.broadcasted_iota(jnp.int32, (1, KEY_BLOCK), 1)
        n_keys = CORES * mem_rows

        def wait_queries(src):
            @pl.when(src != me)
            def _():
                q_arrival(layer, src).wait_recv()

        def score_of(src, scores_ref):
            return score_steps(stack_heads(q_all[layer, src], head_dim, scale), lambda start: mem_k[layer, start:start + KEY_BLOCK, :], n_keys,
                               lambda start: mem_at + start < mem_len_ref[0], scores_ref)

        def put_stats(src, tops, dens):
            top, den = jnp.concatenate(tops, axis=0), jnp.concatenate(dens, axis=0)
            lane = lax.broadcasted_iota(jnp.int32, (rows, 128), 1)
            stats = jnp.zeros((rows, 128), F32)
            for h in range(hpg):
                stats = jnp.where(lane == h, top[h * rows:(h + 1) * rows], stats)
                stats = jnp.where(lane == hpg + h, den[h * rows:(h + 1) * rows], stats)
            stat_send[layer, src] = jnp.transpose(stats)[:2 * hpg]

        def values_of(weights_ref, parts):
            return value_steps(lambda start, stop: mem_vals[layer, start:stop, :], n_keys, weights_ref, parts)

        def put_part(src, parts):
            part_send[layer, src] = unstack_heads(parts[0], rows, head_dim).astype(BF16)

        def stages(after, s_after, now, s_now, w_now, before, w_before):
            tops, dens, parts = [], [], []
            interleave(score_of(after, s_after), exponent_steps(n_keys, s_now, w_now, tops, dens, LAG), values_of(w_before, parts))
            put_stats(now, tops, dens)
            put_part(before, parts)

        def send(src, copy):
            @pl.when(src != me)
            def _():
                copy(layer, src).start()

        phase(f'cross{layer}')

        def turn_body(turn, carry):
            first = turn * 2
            for i in range(group // 2):
                if later:
                    @pl.when(turn == i)
                    def _():
                        for other, name in later[i::group // 2]:
                            weight_copy(name, other).start()
            second, before, after = first + 1, lax.rem(first + group - 1, group), jnp.minimum(first + 2, group - 1)
            wait_queries(second)
            stages(second, scores_b, first, scores_a, weights_a, before, weights_b)
            send(first, stat_copy)

            @pl.when(turn > 0)
            def _():
                send(before, part_copy)

            @pl.when(turn < group // 2 - 1)
            def _():
                wait_queries(first + 2)
            stages(after, scores_a, second, scores_b, weights_b, first, weights_a)
            send(second, stat_copy)
            send(first, part_copy)
            return carry

        @pl.when(chip < mem_chips)
        def _():
            wait_queries(0)
            interleave(score_of(0, scores_a))
            lax.fori_loop(0, group // 2, turn_body, 0)
            parts = []
            interleave(values_of(weights_b, parts))
            put_part(group - 1, parts)
            send(group - 1, part_copy)
            part_recv[layer, me] = part_send[layer, me]
            stat_recv[layer, me] = stat_send[layer, me]

        @pl.when(chip >= mem_chips)
        def _():
            for other, name in later:
                weight_copy(name, other).start()
        phase(f'arrived{layer}')

        for src in range(mem_chips * CORES):
            @pl.when(src != me)
            def _():
                stat_arrival(layer, src).wait_recv()
                part_arrival(layer, src).wait_recv()

        phase(f'combine{layer}')
        factors = [None] * (mem_chips * CORES)
        for g in range(CORES):
            members = [c * CORES + g for c in range(mem_chips)]
            tops = [stat_recv[layer, i, 0:hpg] for i in members]
            dens = [stat_recv[layer, i, hpg:2 * hpg] for i in members]
            best = functools.reduce(jnp.maximum, tops)
            shares = [jnp.exp(t - best) for t in tops]
            total = functools.reduce(jnp.add, [s * d for s, d in zip(shares, dens)])
            for i, s in zip(members, shares):
                factors[i] = s / total
        packed = jnp.concatenate(factors + [jnp.zeros((128 - mem_chips * CORES * hpg, rows), F32)], axis=0)
        packed = jnp.transpose(packed)
        lane_group = lane_groups(rows, half, head_dim)
        attended = []
        for g in range(CORES):
            total = jnp.zeros((rows, half), F32)
            for c in range(mem_chips):
                i = c * CORES + g
                factor = jnp.zeros((rows, half), F32)
                for h in range(hpg):
                    factor = jnp.where(lane_group == h, packed[:, i * hpg + h:i * hpg + h + 1], factor)
                total = total + part_recv[layer, i].astype(F32) * factor
            attended.append(total.astype(BF16))
        attended = jnp.concatenate(attended, axis=-1)
        phase(f'co{layer}')
        weight_copy('cross_o', layer).wait()
        hidden = (hid[...].astype(F32) + mm(attended, w['cross_o'][layer])).astype(BF16)

        phase(f'mlp{layer}')
        normed = rms_norm(hidden, norm_mlp[layer:layer + 1, :])
        for name in ('mlp_gate', 'mlp_up', 'mlp_down'):
            weight_copy(name, layer).wait()
        update = None
        for start in range(0, w['mlp_gate'].shape[-1], FF_BLOCK):
            cols = slice(start, start + FF_BLOCK)
            gate = mm(normed, w['mlp_gate'][layer, :, cols])
            up = mm(normed, w['mlp_up'][layer, :, cols])
            act = (gate * jax.nn.sigmoid(gate) * up).astype(BF16)
            part = mm(act, w['mlp_down'][layer, cols, :])
            update = part if update is None else update + part
        hidden = (hidden.astype(F32) + update).astype(BF16)
        hid[...] = hidden

    phase('end')
    out_ref[...] = hid[...]

    @pl.when(chip < mem_chips)
    def _():
        mem_out.wait_send()
    for layer in range(n_layers):
        for condition, copy in x_sends(layer):
            pl.when(condition)(copy.wait_send)
        pl.when(chip == 0)(x_forward_first(layer).wait_send)
        pl.when(chip > 0)(x_forward(layer).wait_send)
        for turn in range(chips - 1):
            @pl.when(turn < chip)
            def _():
                for part in (0, 1):
                    x_relay_copy(layer, turn, part).wait_send()
        for d in range(1, chips):
            @pl.when(lax.rem(chip + d, chips) < mem_chips)
            def _():
                for k in range(CORES):
                    q_copy(layer, d, k).wait_send()

        @pl.when(chip < mem_chips)
        def _():
            q_to_partner(layer).wait_send()
            for step in range(1, group):
                part_copy(layer, lax.rem(me + step, group)).wait_send()
                stat_copy(layer, lax.rem(me + step, group)).wait_send()
    phase(None)


def solution(mesh):
    group = mesh.shape['sp']
    row_spec = P(('dp', 'sp'), None)

    def local_step(hidden, memory, mem_len, norm_self, norm_cross, norm_mlp, self_q, self_k, self_v, self_o, cross_q, cross_k, cross_v, cross_o, mlp_gate, mlp_up, mlp_down):
        rows, width = hidden.shape
        mem_rows = memory.shape[0]
        n_layers, n_heads, head_dim = self_o.shape[:3]
        inner = n_heads * head_dim
        half = inner // CORES
        hpg = half // head_dim
        all_keys = max(group * rows, CORES * mem_rows)
        weights = dict(
            self_q=self_q, self_k=self_k, self_v=self_v, self_o=self_o.reshape(n_layers, inner, width), cross_k=cross_k, cross_v=cross_v,
            cross_q=cross_q, cross_o=cross_o.reshape(n_layers, inner, width), mlp_gate=mlp_gate, mlp_up=mlp_up, mlp_down=mlp_down)
        w_scratch = [
            pltpu.VMEM((n_layers, width, half) if name in HALVED else weights[name].shape, BF16) for name in WEIGHTS]
        dma = pltpu.SemaphoreType.DMA
        vmem = pl.BlockSpec(memory_space=pltpu.VMEM)
        hbm = pl.BlockSpec(memory_space=pl.ANY)
        return pl.pallas_call(
            functools.partial(kernel, group, n_layers, head_dim),
            out_shape=jax.ShapeDtypeStruct((rows, width), BF16),
            in_specs=[vmem, hbm, pl.BlockSpec(memory_space=pltpu.SMEM), vmem, vmem, vmem] + [hbm] * len(WEIGHTS),
            out_specs=vmem,
            scratch_shapes=w_scratch + [
                pltpu.VMEM((CORES, mem_rows, width), BF16),
                pltpu.VMEM((n_layers, group, rows, width), BF16),
                pltpu.VMEM((group, rows, width), BF16),
                pltpu.VMEM((group, rows, width), BF16),
                pltpu.VMEM((n_layers, CORES * mem_rows, half), BF16),
                pltpu.VMEM((n_layers, CORES * mem_rows, half), BF16),
                pltpu.VMEM((n_layers, CORES, rows, half), BF16),
                pltpu.VMEM((n_layers, group, rows, half), BF16),
                pltpu.VMEM((n_layers, group, rows, half), BF16),
                pltpu.VMEM((n_layers, group, rows, half), BF16),
                pltpu.VMEM((n_layers, group, 2 * hpg, rows), F32),
                pltpu.VMEM((n_layers, group, 2 * hpg, rows), F32),
                pltpu.VMEM((rows, width), BF16),
                pltpu.VMEM((hpg * rows, all_keys), F32),
                pltpu.VMEM((hpg * rows, all_keys), F32),
                pltpu.VMEM((hpg * rows, all_keys), BF16),
                pltpu.VMEM((hpg * rows, all_keys), BF16),
                dma((len(WEIGHTS), n_layers)),
                dma((1,)), dma((1,)), dma((1,)),
                dma((n_layers, 7)), dma((n_layers, group // CORES - 1, 2)), dma((n_layers, group, 2)),
                dma((n_layers, group)), dma((n_layers, group)),
                dma((n_layers, group)), dma((n_layers, group)),
                dma((n_layers, group)), dma((n_layers, group)),
            ],
            compiler_params=pltpu.CompilerParams(collective_id=0, has_side_effects=True, vmem_limit_bytes=60 * 1024 * 1024),
        )(hidden, memory, mem_len, norm_self, norm_cross, norm_mlp, *[weights[name] for name in WEIGHTS])

    return jax.shard_map(local_step, mesh=mesh, in_specs=(row_spec, row_spec, P('dp')) + (P(),) * 14, out_specs=row_spec, check_vma=False)
```

```python
import functools

import jax
import jax.numpy as jnp
from jax import lax
from jax.experimental import pallas as pl
from jax.experimental.pallas import tpu as pltpu
from jax.sharding import PartitionSpec as P

EPS = 1e-6
NEG_BIG = -1e30
CORES = 2
KEY_BLOCK = 512
VALUE_BLOCK = 2048
FF_BLOCK = 512
MEM_BLOCK = 256
ROW_BLOCK = 64
LAG = 1
LOWEST = -3.4e38
MEM_LEN_MAX = 6144
F32 = jnp.float32
BF16 = jnp.bfloat16
MESH = pl.DeviceIdType.MESH
WEIGHTS = ('self_q', 'self_k', 'self_v', 'self_o', 'cross_k', 'cross_v', 'cross_q', 'cross_o', 'mlp_gate', 'mlp_up', 'mlp_down')
HALVED = ('cross_k', 'cross_v')


def rms_norm(hidden, gain_row):
    hidden32 = hidden.astype(F32)
    inv_rms = lax.rsqrt(jnp.mean(hidden32 * hidden32, axis=-1, keepdims=True) + EPS)
    return (hidden32 * inv_rms * gain_row.astype(F32)).astype(BF16)


def mm(a, b):
    return jnp.dot(a, b, preferred_element_type=F32)


def mm_t(a, b):
    return lax.dot_general(a, b, (((1,), (1,)), ((), ())), preferred_element_type=F32)


def lane_groups(rows, lanes, head_dim):
    return lax.broadcasted_iota(jnp.int32, (rows, lanes), 1) // head_dim


def stack_heads(q, head_dim, scale):
    rows, lanes = q.shape
    scaled = q.astype(F32) * scale
    group = lane_groups(rows, lanes, head_dim)
    return jnp.concatenate([jnp.where(group == h, scaled, 0.0).astype(BF16) for h in range(lanes // head_dim)], axis=0)


def score_steps(q_stack, key_block, n_keys, allowed, scores_ref):
    def step(start):
        scores = mm_t(q_stack, key_block(start))
        scores_ref[:, start:start + KEY_BLOCK] = jnp.where(allowed(start), scores, NEG_BIG)
    return [functools.partial(step, start) for start in range(0, n_keys, KEY_BLOCK)]


def exponent_steps(n_keys, scores_ref, weights_ref, tops, dens, lag=0):
    sums = []

    def step(row):
        at = slice(row, row + ROW_BLOCK)
        tiles = [scores_ref[at, lane:lane + 128] for lane in range(0, n_keys, 128)]
        if lag and len(sums) >= lag:
            tiles.insert(0, jnp.minimum(sums[-lag], LOWEST))
        top = jnp.max(functools.reduce(jnp.maximum, tiles), axis=-1, keepdims=True)
        run_sum = None
        for lane in range(0, n_keys, 256):
            weights = jnp.exp(scores_ref[at, lane:lane + 256] - top)
            weights_ref[at, lane:lane + 256] = weights.astype(BF16)
            pair = weights[:, :128] + weights[:, 128:]
            run_sum = pair if run_sum is None else run_sum + pair
        sums.append(run_sum)
        tops.append(top)
        dens.append(jnp.sum(run_sum, axis=-1, keepdims=True))
    return [functools.partial(step, row) for row in range(0, scores_ref.shape[0], ROW_BLOCK)]


def value_steps(value_block, n_keys, weights_ref, parts):
    def step(start):
        stop = min(start + VALUE_BLOCK, n_keys)
        part = mm(weights_ref[:, start:stop], value_block(start, stop))
        parts[:] = [part if not parts else parts[0] + part]
    return [functools.partial(step, start) for start in range(0, n_keys, VALUE_BLOCK)]


def interleave(*lists):
    order = sorted(((i + 0.5) / len(steps), n, i) for n, steps in enumerate(lists) for i in range(len(steps)))
    for _, n, i in order:
        lists[n][i]()


def unstack_heads(stacked, rows, head_dim):
    lanes = stacked.shape[1]
    group = lane_groups(rows, lanes, head_dim)
    out = stacked[:rows]
    for h in range(1, lanes // head_dim):
        out = jnp.where(group == h, stacked[h * rows:(h + 1) * rows], out)
    return out


class Phase:
    def __init__(self):
        self.cur = None

    def __call__(self, name):
        if self.cur is not None:
            self.cur.__exit__(None, None, None)
        self.cur = jax.named_scope(name) if name else None
        if self.cur is not None:
            self.cur.__enter__()


def kernel(group, n_layers, head_dim, *refs):
    n_w = len(WEIGHTS)
    hidden_ref, memory_ref, mem_len_ref, norm_self, norm_cross, norm_mlp = refs[:6]
    w_hbm = dict(zip(WEIGHTS, refs[6:6 + n_w]))
    out_ref = refs[6 + n_w]
    scratch = refs[7 + n_w:]
    w = dict(zip(WEIGHTS, scratch[:n_w]))
    (mem_v, x_all, k_all, v_all, mem_k, mem_vals, q_send, q_all, part_send, part_recv, stat_send, stat_recv, hid, scores_a, scores_b, weights_a, weights_b,
     w_sem, mem_sem, mem_send, mem_recv, x_send, x_relay, x_recv, q_ssem, q_rsem, p_ssem, p_rsem, s_ssem, s_rsem) = scratch[n_w:]

    rows, width = hidden_ref.shape
    mem_rows = memory_ref.shape[0]
    chips = group // CORES
    mem_chips = -(-MEM_LEN_MAX // (CORES * mem_rows))
    half = q_send.shape[-1]
    hpg = half // head_dim
    scale = head_dim ** -0.5
    me = lax.axis_index('sp')
    chip, core = me // CORES, me % CORES
    partner = chip * CORES + (1 - core)

    def remote(src, dst, ssem, rsem, dev):
        return pltpu.make_async_remote_copy(src_ref=src, dst_ref=dst, send_sem=ssem, recv_sem=rsem, device_id={'sp': dev}, device_id_type=MESH)

    def weight_copy(name, layer):
        src = w_hbm[name].at[layer]
        if name in HALVED:
            src = w_hbm[name].at[layer, :, pl.ds(pl.multiple_of(core * half, half), half)]
        return pltpu.make_async_copy(src, w[name].at[layer], w_sem.at[WEIGHTS.index(name), layer])

    phase = Phase()
    phase('start')
    mem_copy = pltpu.make_async_copy(memory_ref, mem_v.at[core], mem_sem.at[0])

    for name in ('self_q', 'self_k', 'self_v'):
        weight_copy(name, 0).start()
    mem_copy.start()
    for layer in range(n_layers):
        for name in HALVED:
            weight_copy(name, layer).start()

    def start_weights(layer, names):
        for name in names:
            weight_copy(name, layer).start()

    phase('barrier')
    barrier = pltpu.get_barrier_semaphore()
    for step in range(1, group):
        pl.semaphore_signal(barrier, inc=1, device_id={'sp': lax.rem(me + step, group)}, device_id_type=MESH)
    pl.semaphore_wait(barrier, group - 1)

    top_chip = chip // (chips - 1)
    half_rows = rows // 2

    def x_copy(layer, src, part, ssem, dst):
        at = x_all.at[layer, src, pl.ds(pl.multiple_of(part * half_rows, half_rows), half_rows)]
        return remote(at, at, ssem, x_recv.at[layer, src, part], dst)

    def x_sends(layer):
        up = me + CORES
        across = (chips - 1) * CORES + core
        send = x_send.at
        return [
            (core == 0, x_copy(layer, me, 0, send[layer, 4], partner)),
            (core == 0, x_copy(layer, me, 1, send[layer, 5], partner)),
            (chip == 1, x_copy(layer, me, 1, send[layer, 2], core)),
            (chip < chips - 1, x_copy(layer, me, 0, send[layer, 0], up)),
            (chip == 0, x_copy(layer, me, 1, send[layer, 2], across)),
            (chip < chips - 1, x_copy(layer, me, 1, send[layer, 1], up)),
            (chip == 0, x_copy(layer, me, 0, send[layer, 3], across)),
        ]

    def x_source(turn):
        return top_chip * (turn * 2 - 3 * (turn // 2)) + (1 - top_chip) * (chip - 1 - turn)

    def x_forward(layer):
        src = x_source(0) * CORES + core
        return x_copy(layer, src, top_chip, x_send.at[layer, 6], me + CORES - 2 * CORES * top_chip)

    def x_forward_first(layer):
        return x_copy(layer, CORES + core, 1, x_send.at[layer, 6], (chips - 1) * CORES + core)

    def x_relay_copy(layer, turn, part):
        return x_copy(layer, x_source(turn) * CORES + core, part, x_relay.at[layer, turn, part], partner)

    def x_arrival(layer, src, part):
        return x_copy(layer, src, part, x_send.at[layer, 0], partner)

    def q_copy(layer, d, k):
        dst = lax.rem(chip + d, chips) * CORES + k
        return remote(q_send.at[layer, k], q_all.at[layer, me], q_ssem.at[layer, d * CORES + k], q_rsem.at[layer, me], dst)

    def q_to_partner(layer):
        return remote(q_send.at[layer, 1 - core], q_all.at[layer, me], q_ssem.at[layer, 0], q_rsem.at[layer, me], partner)

    def q_arrival(layer, src):
        return remote(q_send.at[layer, 0], q_all.at[layer, src], q_ssem.at[layer, 0], q_rsem.at[layer, src], partner)

    def part_copy(layer, src):
        return remote(part_send.at[layer, src], part_recv.at[layer, me], p_ssem.at[layer, src], p_rsem.at[layer, me], src)

    def stat_copy(layer, src):
        return remote(stat_send.at[layer, src], stat_recv.at[layer, me], s_ssem.at[layer, src], s_rsem.at[layer, me], src)

    def part_arrival(layer, src):
        return remote(part_send.at[layer, src], part_recv.at[layer, src], p_ssem.at[layer, src], p_rsem.at[layer, src], partner)

    def stat_arrival(layer, src):
        return remote(stat_send.at[layer, src], stat_recv.at[layer, src], s_ssem.at[layer, src], s_rsem.at[layer, src], partner)

    mem_out = remote(mem_v.at[core], mem_v.at[core], mem_send.at[0], mem_recv.at[0], partner)
    mem_in = remote(mem_v.at[1 - core], mem_v.at[1 - core], mem_send.at[0], mem_recv.at[0], partner)

    def project_memory(slot, layer):
        def body(i, carry):
            at = pl.ds(pl.multiple_of(i * MEM_BLOCK, MEM_BLOCK), MEM_BLOCK)
            to = pl.ds(pl.multiple_of(slot * mem_rows + i * MEM_BLOCK, MEM_BLOCK), MEM_BLOCK)
            block = mem_v[slot, at, :]
            mem_k[layer, to, :] = mm(block, w['cross_k'][layer]).astype(BF16)
            mem_vals[layer, to, :] = mm(block, w['cross_v'][layer]).astype(BF16)
            return carry
        lax.fori_loop(0, mem_rows // MEM_BLOCK, body, 0)

    phase('zero')
    hid[...] = hidden_ref[...]
    for src in range(group):
        @pl.when(src > me)
        def _():
            k_all[src] = jnp.zeros((rows, width), BF16)
            v_all[src] = jnp.zeros((rows, width), BF16)

    for layer in range(n_layers):
        phase(f'xnorm{layer}')
        x_all[layer, me] = rms_norm(hid[...], norm_self[layer:layer + 1, :])
        for condition, copy in x_sends(layer):
            pl.when(condition)(copy.start)
        if layer == 0:
            start_weights(0, ('self_o', 'cross_q', 'cross_o'))

        for name in ('self_q', 'self_k', 'self_v'):
            weight_copy(name, layer).wait()

        def project_rows(src):
            block = x_all[layer, src]
            k_all[src] = mm(block, w['self_k'][layer]).astype(BF16)
            v_all[src] = mm(block, w['self_v'][layer]).astype(BF16)

        phase(f'ownproj{layer}')
        project_rows(me)
        queries = mm(x_all[layer, me], w['self_q'][layer]).astype(BF16)

        phase(f'memproj{layer}')
        if layer == 0:
            mem_copy.wait()
            for other in range(n_layers):
                for name in HALVED:
                    weight_copy(name, other).wait()

            @pl.when(chip < mem_chips)
            def _():
                mem_out.start()
                for other in range(n_layers):
                    project_memory(core, other)
        phase(f'xwait{layer}')

        @pl.when(chip == 0)
        def _():
            x_arrival(layer, CORES + core, 1).wait_recv()
            x_forward_first(layer).start()

        for turn in range(chips - 1):
            @pl.when(turn < chip)
            def _():
                src = x_source(turn) * CORES + core
                first = top_chip if turn == 0 else 0
                for i, part in enumerate((first, 1 - first)):
                    x_arrival(layer, src, part).wait_recv()
                    if turn == 0 and i == 0:
                        pl.when(chip > 0)(x_forward(layer).start)
                    x_relay_copy(layer, turn, part).start()
                project_rows(src)

        phase(f'memproj2{layer}')

        @pl.when(chip < mem_chips)
        def _():
            if layer == 0:
                mem_in.wait_recv()
            project_memory(1 - core, layer)

        phase(f'xwait2{layer}')
        @pl.when(core == 1)
        def _():
            for part in (0, 1):
                x_arrival(layer, partner, part).wait_recv()
            project_rows(partner)

        for turn in range(chips - 1):
            @pl.when(turn < chip)
            def _():
                src = x_source(turn) * CORES + (1 - core)
                for part in (0, 1):
                    x_arrival(layer, src, part).wait_recv()
                project_rows(src)

        phase(f'selfatt{layer}')
        all_rows = group * rows
        query_at = me * rows + lax.rem(lax.broadcasted_iota(jnp.int32, (hpg * rows, KEY_BLOCK), 0), rows)
        key_at = lax.broadcasted_iota(jnp.int32, (hpg * rows, KEY_BLOCK), 1)
        per_block = KEY_BLOCK // rows
        stores = ((scores_a, weights_a), (scores_b, weights_b))
        tops, dens, parts = [[], []], [[], []], [[], []]

        def self_steps(g):
            lanes = slice(g * half, (g + 1) * half)
            s_ref, w_ref = stores[g]
            return (
                score_steps(stack_heads(queries[:, lanes], head_dim, scale),
                            lambda start: k_all[start // rows:start // rows + per_block, :, lanes].reshape(KEY_BLOCK, half),
                            all_rows, lambda start: key_at + start <= query_at, s_ref),
                exponent_steps(all_rows, s_ref, w_ref, tops[g], dens[g]),
                value_steps(lambda start, stop: v_all[start // rows:stop // rows, :, lanes].reshape(stop - start, half),
                            all_rows, w_ref, parts[g]))

        steps = [self_steps(g) for g in range(CORES)]
        interleave(steps[0][0])
        interleave(steps[0][1], steps[1][0])
        interleave(steps[0][2], steps[1][1])
        interleave(steps[1][2])
        attended = [unstack_heads(parts[g][0] / jnp.concatenate(dens[g], axis=0), rows, head_dim).astype(BF16) for g in range(CORES)]
        attended = jnp.concatenate(attended, axis=-1)
        phase(f'oproj{layer}')
        weight_copy('self_o', layer).wait()
        hidden = (hid[...].astype(F32) + mm(attended, w['self_o'][layer])).astype(BF16)
        hid[...] = hidden

        phase(f'qproj{layer}')
        weight_copy('cross_q', layer).wait()
        queries = mm(rms_norm(hidden, norm_cross[layer:layer + 1, :]), w['cross_q'][layer]).astype(BF16)
        for g in range(CORES):
            q_send[layer, g] = queries[:, g * half:(g + 1) * half]
        q_order = [(d, k) for d in (1, 3, 2) if d < chips for k in range(CORES)]

        @pl.when(chip < mem_chips)
        def _():
            q_to_partner(layer).start()
        for d, k in q_order:
            @pl.when(lax.rem(chip + d, chips) < mem_chips)
            def _():
                q_copy(layer, d, k).start()
        q_all[layer, me] = q_send[layer, core]
        later = []
        if layer == 0:
            later = [(0, name) for name in ('mlp_gate', 'mlp_up', 'mlp_down')]
            later += [(other, name) for other in range(1, n_layers) for name in WEIGHTS if name not in HALVED]

        mem_at = chip * (CORES * mem_rows) + lax.broadcasted_iota(jnp.int32, (1, KEY_BLOCK), 1)
        n_keys = CORES * mem_rows

        def wait_queries(src):
            @pl.when(src != me)
            def _():
                q_arrival(layer, src).wait_recv()

        def score_of(src, scores_ref):
            return score_steps(stack_heads(q_all[layer, src], head_dim, scale), lambda start: mem_k[layer, start:start + KEY_BLOCK, :], n_keys,
                               lambda start: mem_at + start < mem_len_ref[0], scores_ref)

        def put_stats(src, tops, dens):
            top, den = jnp.concatenate(tops, axis=0), jnp.concatenate(dens, axis=0)
            lane = lax.broadcasted_iota(jnp.int32, (rows, 128), 1)
            stats = jnp.zeros((rows, 128), F32)
            for h in range(hpg):
                stats = jnp.where(lane == h, top[h * rows:(h + 1) * rows], stats)
                stats = jnp.where(lane == hpg + h, den[h * rows:(h + 1) * rows], stats)
            stat_send[layer, src] = jnp.transpose(stats)[:2 * hpg]

        def values_of(weights_ref, parts):
            return value_steps(lambda start, stop: mem_vals[layer, start:stop, :], n_keys, weights_ref, parts)

        def put_part(src, parts):
            part_send[layer, src] = unstack_heads(parts[0], rows, head_dim).astype(BF16)

        def stages(after, s_after, now, s_now, w_now, before, w_before):
            tops, dens, parts = [], [], []
            interleave(score_of(after, s_after), exponent_steps(n_keys, s_now, w_now, tops, dens, LAG), values_of(w_before, parts))
            put_stats(now, tops, dens)
            put_part(before, parts)

        def send(src, copy):
            @pl.when(src != me)
            def _():
                copy(layer, src).start()

        phase(f'cross{layer}')

        def pair(turn):
            return turn + (chip // (mem_chips - 1)) * (turn // 2) * (1 - 2 * lax.rem(turn, 2))

        def turn_body(turn, carry):
            first = pair(turn) * CORES
            for i in range(group // 2):
                if later:
                    @pl.when(turn == i)
                    def _():
                        for other, name in later[i::group // 2]:
                            weight_copy(name, other).start()
            second = first + 1
            before = pair(lax.rem(turn + chips - 1, chips)) * CORES + 1
            after = pair(lax.rem(turn + 1, chips)) * CORES
            wait_queries(second)
            stages(second, scores_b, first, scores_a, weights_a, before, weights_b)
            send(first, stat_copy)

            @pl.when(turn > 0)
            def _():
                send(before, part_copy)

            @pl.when(turn < chips - 1)
            def _():
                wait_queries(after)
            stages(after, scores_a, second, scores_b, weights_b, first, weights_a)
            send(second, stat_copy)
            send(first, part_copy)
            return carry

        @pl.when(chip < mem_chips)
        def _():
            wait_queries(0)
            interleave(score_of(0, scores_a))
            lax.fori_loop(0, chips, turn_body, 0)
            parts = []
            interleave(values_of(weights_b, parts))
            last = pair(jnp.int32(chips - 1)) * CORES + 1
            put_part(last, parts)
            send(last, part_copy)
            part_recv[layer, me] = part_send[layer, me]
            stat_recv[layer, me] = stat_send[layer, me]

        @pl.when(chip >= mem_chips)
        def _():
            for other, name in later:
                weight_copy(name, other).start()
        phase(f'arrived{layer}')

        for src in range(mem_chips * CORES):
            @pl.when(src != me)
            def _():
                stat_arrival(layer, src).wait_recv()
                part_arrival(layer, src).wait_recv()

        phase(f'combine{layer}')
        factors = [None] * (mem_chips * CORES)
        for g in range(CORES):
            members = [c * CORES + g for c in range(mem_chips)]
            tops = [stat_recv[layer, i, 0:hpg] for i in members]
            dens = [stat_recv[layer, i, hpg:2 * hpg] for i in members]
            best = functools.reduce(jnp.maximum, tops)
            shares = [jnp.exp(t - best) for t in tops]
            total = functools.reduce(jnp.add, [s * d for s, d in zip(shares, dens)])
            for i, s in zip(members, shares):
                factors[i] = s / total
        packed = jnp.concatenate(factors + [jnp.zeros((128 - mem_chips * CORES * hpg, rows), F32)], axis=0)
        packed = jnp.transpose(packed)
        lane_group = lane_groups(rows, half, head_dim)
        attended = []
        for g in range(CORES):
            total = jnp.zeros((rows, half), F32)
            for c in range(mem_chips):
                i = c * CORES + g
                factor = jnp.zeros((rows, half), F32)
                for h in range(hpg):
                    factor = jnp.where(lane_group == h, packed[:, i * hpg + h:i * hpg + h + 1], factor)
                total = total + part_recv[layer, i].astype(F32) * factor
            attended.append(total.astype(BF16))
        attended = jnp.concatenate(attended, axis=-1)
        phase(f'co{layer}')
        weight_copy('cross_o', layer).wait()
        hidden = (hid[...].astype(F32) + mm(attended, w['cross_o'][layer])).astype(BF16)

        phase(f'mlp{layer}')
        normed = rms_norm(hidden, norm_mlp[layer:layer + 1, :])
        for name in ('mlp_gate', 'mlp_up', 'mlp_down'):
            weight_copy(name, layer).wait()
        update = None
        for start in range(0, w['mlp_gate'].shape[-1], FF_BLOCK):
            cols = slice(start, start + FF_BLOCK)
            gate = mm(normed, w['mlp_gate'][layer, :, cols])
            up = mm(normed, w['mlp_up'][layer, :, cols])
            act = (gate * jax.nn.sigmoid(gate) * up).astype(BF16)
            part = mm(act, w['mlp_down'][layer, cols, :])
            update = part if update is None else update + part
        hidden = (hidden.astype(F32) + update).astype(BF16)
        hid[...] = hidden

    phase('end')
    out_ref[...] = hid[...]

    @pl.when(chip < mem_chips)
    def _():
        mem_out.wait_send()
    for layer in range(n_layers):
        for condition, copy in x_sends(layer):
            pl.when(condition)(copy.wait_send)
        pl.when(chip == 0)(x_forward_first(layer).wait_send)
        pl.when(chip > 0)(x_forward(layer).wait_send)
        for turn in range(chips - 1):
            @pl.when(turn < chip)
            def _():
                for part in (0, 1):
                    x_relay_copy(layer, turn, part).wait_send()
        for d in range(1, chips):
            @pl.when(lax.rem(chip + d, chips) < mem_chips)
            def _():
                for k in range(CORES):
                    q_copy(layer, d, k).wait_send()

        @pl.when(chip < mem_chips)
        def _():
            q_to_partner(layer).wait_send()
            for step in range(1, group):
                part_copy(layer, lax.rem(me + step, group)).wait_send()
                stat_copy(layer, lax.rem(me + step, group)).wait_send()
    phase(None)


def solution(mesh):
    group = mesh.shape['sp']
    row_spec = P(('dp', 'sp'), None)

    def local_step(hidden, memory, mem_len, norm_self, norm_cross, norm_mlp, self_q, self_k, self_v, self_o, cross_q, cross_k, cross_v, cross_o, mlp_gate, mlp_up, mlp_down):
        rows, width = hidden.shape
        mem_rows = memory.shape[0]
        n_layers, n_heads, head_dim = self_o.shape[:3]
        inner = n_heads * head_dim
        half = inner // CORES
        hpg = half // head_dim
        all_keys = max(group * rows, CORES * mem_rows)
        weights = dict(
            self_q=self_q, self_k=self_k, self_v=self_v, self_o=self_o.reshape(n_layers, inner, width), cross_k=cross_k, cross_v=cross_v,
            cross_q=cross_q, cross_o=cross_o.reshape(n_layers, inner, width), mlp_gate=mlp_gate, mlp_up=mlp_up, mlp_down=mlp_down)
        w_scratch = [
            pltpu.VMEM((n_layers, width, half) if name in HALVED else weights[name].shape, BF16) for name in WEIGHTS]
        dma = pltpu.SemaphoreType.DMA
        vmem = pl.BlockSpec(memory_space=pltpu.VMEM)
        hbm = pl.BlockSpec(memory_space=pl.ANY)
        return pl.pallas_call(
            functools.partial(kernel, group, n_layers, head_dim),
            out_shape=jax.ShapeDtypeStruct((rows, width), BF16),
            in_specs=[vmem, hbm, pl.BlockSpec(memory_space=pltpu.SMEM), vmem, vmem, vmem] + [hbm] * len(WEIGHTS),
            out_specs=vmem,
            scratch_shapes=w_scratch + [
                pltpu.VMEM((CORES, mem_rows, width), BF16),
                pltpu.VMEM((n_layers, group, rows, width), BF16),
                pltpu.VMEM((group, rows, width), BF16),
                pltpu.VMEM((group, rows, width), BF16),
                pltpu.VMEM((n_layers, CORES * mem_rows, half), BF16),
                pltpu.VMEM((n_layers, CORES * mem_rows, half), BF16),
                pltpu.VMEM((n_layers, CORES, rows, half), BF16),
                pltpu.VMEM((n_layers, group, rows, half), BF16),
                pltpu.VMEM((n_layers, group, rows, half), BF16),
                pltpu.VMEM((n_layers, group, rows, half), BF16),
                pltpu.VMEM((n_layers, group, 2 * hpg, rows), F32),
                pltpu.VMEM((n_layers, group, 2 * hpg, rows), F32),
                pltpu.VMEM((rows, width), BF16),
                pltpu.VMEM((hpg * rows, all_keys), F32),
                pltpu.VMEM((hpg * rows, all_keys), F32),
                pltpu.VMEM((hpg * rows, all_keys), BF16),
                pltpu.VMEM((hpg * rows, all_keys), BF16),
                dma((len(WEIGHTS), n_layers)),
                dma((1,)), dma((1,)), dma((1,)),
                dma((n_layers, 7)), dma((n_layers, group // CORES - 1, 2)), dma((n_layers, group, 2)),
                dma((n_layers, group)), dma((n_layers, group)),
                dma((n_layers, group)), dma((n_layers, group)),
                dma((n_layers, group)), dma((n_layers, group)),
            ],
            compiler_params=pltpu.CompilerParams(collective_id=0, has_side_effects=True, vmem_limit_bytes=60 * 1024 * 1024),
        )(hidden, memory, mem_len, norm_self, norm_cross, norm_mlp, *[weights[name] for name in WEIGHTS])

    return jax.shard_map(local_step, mesh=mesh, in_specs=(row_spec, row_spec, P('dp')) + (P(),) * 14, out_specs=row_spec, check_vma=False)
```

```python
import functools

import jax
import jax.numpy as jnp
from jax import lax
from jax.experimental import pallas as pl
from jax.experimental.pallas import tpu as pltpu
from jax.sharding import PartitionSpec as P

EPS = 1e-6
NEG_BIG = -1e30
CORES = 2
KEY_BLOCK = 512
VALUE_BLOCK = 2048
FF_BLOCK = 512
MEM_BLOCK = 256
ROW_BLOCK = 64
LAG = 1
LOWEST = -3.4e38
MEM_LEN_MAX = 6144
F32 = jnp.float32
BF16 = jnp.bfloat16
MESH = pl.DeviceIdType.MESH
WEIGHTS = ('self_q', 'self_k', 'self_v', 'self_o', 'cross_k', 'cross_v', 'cross_q', 'cross_o', 'mlp_gate', 'mlp_up', 'mlp_down')
HALVED = ('cross_k', 'cross_v')


def rms_norm(hidden, gain_row):
    hidden32 = hidden.astype(F32)
    inv_rms = lax.rsqrt(jnp.mean(hidden32 * hidden32, axis=-1, keepdims=True) + EPS)
    return (hidden32 * inv_rms * gain_row.astype(F32)).astype(BF16)


def mm(a, b):
    return jnp.dot(a, b, preferred_element_type=F32)


def mm_t(a, b):
    return lax.dot_general(a, b, (((1,), (1,)), ((), ())), preferred_element_type=F32)


def lane_groups(rows, lanes, head_dim):
    return lax.broadcasted_iota(jnp.int32, (rows, lanes), 1) // head_dim


def stack_heads(q, head_dim, scale):
    rows, lanes = q.shape
    scaled = q.astype(F32) * scale
    group = lane_groups(rows, lanes, head_dim)
    return jnp.concatenate([jnp.where(group == h, scaled, 0.0).astype(BF16) for h in range(lanes // head_dim)], axis=0)


def score_steps(q_stack, key_block, n_keys, allowed, scores_ref):
    def step(start):
        scores = mm_t(q_stack, key_block(start))
        scores_ref[:, start:start + KEY_BLOCK] = jnp.where(allowed(start), scores, NEG_BIG)
    return [functools.partial(step, start) for start in range(0, n_keys, KEY_BLOCK)]


def exponent_steps(n_keys, scores_ref, weights_ref, tops, dens, lag=0):
    sums = []

    def step(row):
        at = slice(row, row + ROW_BLOCK)
        tiles = [scores_ref[at, lane:lane + 128] for lane in range(0, n_keys, 128)]
        if lag and len(sums) >= lag:
            tiles.insert(0, jnp.minimum(sums[-lag], LOWEST))
        top = jnp.max(functools.reduce(jnp.maximum, tiles), axis=-1, keepdims=True)
        run_sum = None
        for lane in range(0, n_keys, 256):
            weights = jnp.exp(scores_ref[at, lane:lane + 256] - top)
            weights_ref[at, lane:lane + 256] = weights.astype(BF16)
            pair = weights[:, :128] + weights[:, 128:]
            run_sum = pair if run_sum is None else run_sum + pair
        sums.append(run_sum)
        tops.append(top)
        dens.append(jnp.sum(run_sum, axis=-1, keepdims=True))
    return [functools.partial(step, row) for row in range(0, scores_ref.shape[0], ROW_BLOCK)]


def value_steps(value_block, n_keys, weights_ref, parts):
    def step(start):
        stop = min(start + VALUE_BLOCK, n_keys)
        part = mm(weights_ref[:, start:stop], value_block(start, stop))
        parts[:] = [part if not parts else parts[0] + part]
    return [functools.partial(step, start) for start in range(0, n_keys, VALUE_BLOCK)]


def interleave(*lists):
    order = sorted(((i + 0.5) / len(steps), n, i) for n, steps in enumerate(lists) for i in range(len(steps)))
    for _, n, i in order:
        lists[n][i]()


def unstack_heads(stacked, rows, head_dim):
    lanes = stacked.shape[1]
    group = lane_groups(rows, lanes, head_dim)
    out = stacked[:rows]
    for h in range(1, lanes // head_dim):
        out = jnp.where(group == h, stacked[h * rows:(h + 1) * rows], out)
    return out


class Phase:
    def __init__(self):
        self.cur = None

    def __call__(self, name):
        if self.cur is not None:
            self.cur.__exit__(None, None, None)
        self.cur = jax.named_scope(name) if name else None
        if self.cur is not None:
            self.cur.__enter__()


def kernel(group, n_layers, head_dim, *refs):
    n_w = len(WEIGHTS)
    hidden_ref, memory_ref, mem_len_ref, norm_self, norm_cross, norm_mlp = refs[:6]
    w_hbm = dict(zip(WEIGHTS, refs[6:6 + n_w]))
    out_ref = refs[6 + n_w]
    scratch = refs[7 + n_w:]
    w = dict(zip(WEIGHTS, scratch[:n_w]))
    (mem_v, x_all, k_all, v_all, mem_k, mem_vals, q_send, q_all, part_send, part_recv, stat_send, stat_recv, hid, scores_a, scores_b, weights_a, weights_b,
     w_sem, mem_sem, mem_send, mem_recv, x_send, x_relay, x_recv, q_ssem, q_rsem, p_ssem, p_rsem, s_ssem, s_rsem) = scratch[n_w:]

    rows, width = hidden_ref.shape
    mem_rows = memory_ref.shape[0]
    chips = group // CORES
    mem_chips = -(-MEM_LEN_MAX // (CORES * mem_rows))
    half = q_send.shape[-1]
    hpg = half // head_dim
    scale = head_dim ** -0.5
    me = lax.axis_index('sp')
    chip, core = me // CORES, me % CORES
    partner = chip * CORES + (1 - core)

    def remote(src, dst, ssem, rsem, dev):
        return pltpu.make_async_remote_copy(src_ref=src, dst_ref=dst, send_sem=ssem, recv_sem=rsem, device_id={'sp': dev}, device_id_type=MESH)

    def weight_copy(name, layer):
        src = w_hbm[name].at[layer]
        if name in HALVED:
            src = w_hbm[name].at[layer, :, pl.ds(pl.multiple_of(core * half, half), half)]
        return pltpu.make_async_copy(src, w[name].at[layer], w_sem.at[WEIGHTS.index(name), layer])

    phase = Phase()
    phase('start')
    mem_copy = pltpu.make_async_copy(memory_ref, mem_v.at[core], mem_sem.at[0])

    for name in ('self_q', 'self_k', 'self_v'):
        weight_copy(name, 0).start()
    mem_copy.start()
    for layer in range(n_layers):
        for name in HALVED:
            weight_copy(name, layer).start()

    def start_weights(layer, names):
        for name in names:
            weight_copy(name, layer).start()

    phase('barrier')
    barrier = pltpu.get_barrier_semaphore()
    for step in range(1, group):
        pl.semaphore_signal(barrier, inc=1, device_id={'sp': lax.rem(me + step, group)}, device_id_type=MESH)
    pl.semaphore_wait(barrier, group - 1)

    top_chip = chip // (chips - 1)
    half_rows = rows // 2

    def x_copy(layer, src, part, ssem, dst):
        at = x_all.at[layer, src, pl.ds(pl.multiple_of(part * half_rows, half_rows), half_rows)]
        return remote(at, at, ssem, x_recv.at[layer, src, part], dst)

    def x_sends(layer):
        up = me + CORES
        across = (chips - 1) * CORES + core
        send = x_send.at
        return [
            (core == 0, x_copy(layer, me, 0, send[layer, 4], partner)),
            (core == 0, x_copy(layer, me, 1, send[layer, 5], partner)),
            (chip == 1, x_copy(layer, me, 1, send[layer, 2], core)),
            (chip < chips - 1, x_copy(layer, me, 0, send[layer, 0], up)),
            (chip == 0, x_copy(layer, me, 1, send[layer, 2], across)),
            (chip < chips - 1, x_copy(layer, me, 1, send[layer, 1], up)),
            (chip == 0, x_copy(layer, me, 0, send[layer, 3], across)),
        ]

    def x_source(turn):
        return top_chip * (turn * 2 - 3 * (turn // 2)) + (1 - top_chip) * (chip - 1 - turn)

    def x_forward(layer, part):
        return x_copy(layer, x_source(0) * CORES + core, part, x_send.at[layer, 6 + part], me + CORES)

    def x_forward_first(layer):
        return x_copy(layer, CORES + core, 1, x_send.at[layer, 6], (chips - 1) * CORES + core)

    def x_relay_copy(layer, turn, part):
        return x_copy(layer, x_source(turn) * CORES + core, part, x_relay.at[layer, turn, part], partner)

    def x_arrival(layer, src, part):
        return x_copy(layer, src, part, x_send.at[layer, 0], partner)

    def q_copy(layer, d, k):
        dst = lax.rem(chip + d, chips) * CORES + k
        return remote(q_send.at[layer, k], q_all.at[layer, me], q_ssem.at[layer, d * CORES + k], q_rsem.at[layer, me], dst)

    def q_to_partner(layer):
        return remote(q_send.at[layer, 1 - core], q_all.at[layer, me], q_ssem.at[layer, 0], q_rsem.at[layer, me], partner)

    def q_arrival(layer, src):
        return remote(q_send.at[layer, 0], q_all.at[layer, src], q_ssem.at[layer, 0], q_rsem.at[layer, src], partner)

    def part_copy(layer, src):
        return remote(part_send.at[layer, src], part_recv.at[layer, me], p_ssem.at[layer, src], p_rsem.at[layer, me], src)

    def stat_copy(layer, src):
        return remote(stat_send.at[layer, src], stat_recv.at[layer, me], s_ssem.at[layer, src], s_rsem.at[layer, me], src)

    def part_arrival(layer, src):
        return remote(part_send.at[layer, src], part_recv.at[layer, src], p_ssem.at[layer, src], p_rsem.at[layer, src], partner)

    def stat_arrival(layer, src):
        return remote(stat_send.at[layer, src], stat_recv.at[layer, src], s_ssem.at[layer, src], s_rsem.at[layer, src], partner)

    mem_out = remote(mem_v.at[core], mem_v.at[core], mem_send.at[0], mem_recv.at[0], partner)
    mem_in = remote(mem_v.at[1 - core], mem_v.at[1 - core], mem_send.at[0], mem_recv.at[0], partner)

    def project_memory(slot, layer):
        def body(i, carry):
            at = pl.ds(pl.multiple_of(i * MEM_BLOCK, MEM_BLOCK), MEM_BLOCK)
            to = pl.ds(pl.multiple_of(slot * mem_rows + i * MEM_BLOCK, MEM_BLOCK), MEM_BLOCK)
            block = mem_v[slot, at, :]
            mem_k[layer, to, :] = mm(block, w['cross_k'][layer]).astype(BF16)
            mem_vals[layer, to, :] = mm(block, w['cross_v'][layer]).astype(BF16)
            return carry
        lax.fori_loop(0, mem_rows // MEM_BLOCK, body, 0)

    phase('zero')
    hid[...] = hidden_ref[...]
    for src in range(group):
        @pl.when(src > me)
        def _():
            k_all[src] = jnp.zeros((rows, width), BF16)
            v_all[src] = jnp.zeros((rows, width), BF16)

    for layer in range(n_layers):
        phase(f'xnorm{layer}')
        x_all[layer, me] = rms_norm(hid[...], norm_self[layer:layer + 1, :])
        for condition, copy in x_sends(layer):
            pl.when(condition)(copy.start)
        if layer == 0:
            start_weights(0, ('self_o', 'cross_q', 'cross_o'))

        for name in ('self_q', 'self_k', 'self_v'):
            weight_copy(name, layer).wait()

        def project_rows(src):
            block = x_all[layer, src]
            k_all[src] = mm(block, w['self_k'][layer]).astype(BF16)
            v_all[src] = mm(block, w['self_v'][layer]).astype(BF16)

        phase(f'ownproj{layer}')
        project_rows(me)
        queries = mm(x_all[layer, me], w['self_q'][layer]).astype(BF16)

        phase(f'memproj{layer}')
        if layer == 0:
            mem_copy.wait()
            for other in range(n_layers):
                for name in HALVED:
                    weight_copy(name, other).wait()

            @pl.when(chip < mem_chips)
            def _():
                mem_out.start()
                for other in range(n_layers):
                    project_memory(core, other)

        def project_partner_memory():
            if layer == 0:
                mem_in.wait_recv()
            project_memory(1 - core, layer)

        @pl.when(chip == mem_chips - 1)
        def _():
            project_partner_memory()
        phase(f'xwait{layer}')

        @pl.when(chip == 0)
        def _():
            x_arrival(layer, CORES + core, 1).wait_recv()
            x_forward_first(layer).start()

        for turn in range(chips - 1):
            @pl.when(turn < chip)
            def _():
                src = x_source(turn) * CORES + core
                for part in (0, 1):
                    x_arrival(layer, src, part).wait_recv()
                    if turn == 0:
                        pl.when(chip == 1 if part else chip < chips - 1)(x_forward(layer, part).start)
                    x_relay_copy(layer, turn, part).start()
                project_rows(src)

        phase(f'memproj2{layer}')

        @pl.when(chip < mem_chips - 1)
        def _():
            project_partner_memory()

        phase(f'xwait2{layer}')
        @pl.when(core == 1)
        def _():
            for part in (0, 1):
                x_arrival(layer, partner, part).wait_recv()
            project_rows(partner)

        for turn in range(chips - 1):
            @pl.when(turn < chip)
            def _():
                src = x_source(turn) * CORES + (1 - core)
                for part in (0, 1):
                    x_arrival(layer, src, part).wait_recv()
                project_rows(src)

        phase(f'selfatt{layer}')
        all_rows = group * rows
        query_at = me * rows + lax.rem(lax.broadcasted_iota(jnp.int32, (hpg * rows, KEY_BLOCK), 0), rows)
        key_at = lax.broadcasted_iota(jnp.int32, (hpg * rows, KEY_BLOCK), 1)
        per_block = KEY_BLOCK // rows
        stores = ((scores_a, weights_a), (scores_b, weights_b))
        tops, dens, parts = [[], []], [[], []], [[], []]

        def self_steps(g):
            lanes = slice(g * half, (g + 1) * half)
            s_ref, w_ref = stores[g]
            return (
                score_steps(stack_heads(queries[:, lanes], head_dim, scale),
                            lambda start: k_all[start // rows:start // rows + per_block, :, lanes].reshape(KEY_BLOCK, half),
                            all_rows, lambda start: key_at + start <= query_at, s_ref),
                exponent_steps(all_rows, s_ref, w_ref, tops[g], dens[g]),
                value_steps(lambda start, stop: v_all[start // rows:stop // rows, :, lanes].reshape(stop - start, half),
                            all_rows, w_ref, parts[g]))

        steps = [self_steps(g) for g in range(CORES)]
        interleave(steps[0][0])
        interleave(steps[0][1], steps[1][0])
        interleave(steps[0][2], steps[1][1])
        interleave(steps[1][2])
        attended = [unstack_heads(parts[g][0] / jnp.concatenate(dens[g], axis=0), rows, head_dim).astype(BF16) for g in range(CORES)]
        attended = jnp.concatenate(attended, axis=-1)
        phase(f'oproj{layer}')
        weight_copy('self_o', layer).wait()
        hidden = (hid[...].astype(F32) + mm(attended, w['self_o'][layer])).astype(BF16)
        hid[...] = hidden

        phase(f'qproj{layer}')
        weight_copy('cross_q', layer).wait()
        queries = mm(rms_norm(hidden, norm_cross[layer:layer + 1, :]), w['cross_q'][layer]).astype(BF16)
        for g in range(CORES):
            q_send[layer, g] = queries[:, g * half:(g + 1) * half]
        q_order = [(d, k) for d in (2, 1, 3) if d < chips for k in range(CORES)]

        @pl.when(chip < mem_chips)
        def _():
            q_to_partner(layer).start()
        for d, k in q_order:
            @pl.when(lax.rem(chip + d, chips) < mem_chips)
            def _():
                q_copy(layer, d, k).start()
        q_all[layer, me] = q_send[layer, core]
        later = []
        if layer == 0:
            later = [(0, name) for name in ('mlp_gate', 'mlp_up', 'mlp_down')]
            later += [(other, name) for other in range(1, n_layers) for name in WEIGHTS if name not in HALVED]

        mem_at = chip * (CORES * mem_rows) + lax.broadcasted_iota(jnp.int32, (1, KEY_BLOCK), 1)
        n_keys = CORES * mem_rows

        def wait_queries(src):
            @pl.when(src != me)
            def _():
                q_arrival(layer, src).wait_recv()

        def score_of(src, scores_ref):
            return score_steps(stack_heads(q_all[layer, src], head_dim, scale), lambda start: mem_k[layer, start:start + KEY_BLOCK, :], n_keys,
                               lambda start: mem_at + start < mem_len_ref[0], scores_ref)

        def put_stats(src, tops, dens):
            top, den = jnp.concatenate(tops, axis=0), jnp.concatenate(dens, axis=0)
            lane = lax.broadcasted_iota(jnp.int32, (rows, 128), 1)
            stats = jnp.zeros((rows, 128), F32)
            for h in range(hpg):
                stats = jnp.where(lane == h, top[h * rows:(h + 1) * rows], stats)
                stats = jnp.where(lane == hpg + h, den[h * rows:(h + 1) * rows], stats)
            stat_send[layer, src] = jnp.transpose(stats)[:2 * hpg]

        def values_of(weights_ref, parts):
            return value_steps(lambda start, stop: mem_vals[layer, start:stop, :], n_keys, weights_ref, parts)

        def put_part(src, parts):
            part_send[layer, src] = unstack_heads(parts[0], rows, head_dim).astype(BF16)

        def stages(after, s_after, now, s_now, w_now, before, w_before):
            tops, dens, parts = [], [], []
            interleave(score_of(after, s_after), exponent_steps(n_keys, s_now, w_now, tops, dens, LAG), values_of(w_before, parts))
            put_stats(now, tops, dens)
            put_part(before, parts)

        def send(src, copy):
            @pl.when(src != me)
            def _():
                copy(layer, src).start()

        phase(f'cross{layer}')

        def pair(turn):
            return turn + (chip // (mem_chips - 1)) * (turn // 2) * (1 - 2 * lax.rem(turn, 2))

        def turn_body(turn, carry):
            first = pair(turn) * CORES
            for i in range(group // 2):
                if later:
                    @pl.when(turn == i)
                    def _():
                        for other, name in later[i::group // 2]:
                            weight_copy(name, other).start()
            second = first + 1
            before = pair(lax.rem(turn + chips - 1, chips)) * CORES + 1
            after = pair(lax.rem(turn + 1, chips)) * CORES
            wait_queries(second)
            stages(second, scores_b, first, scores_a, weights_a, before, weights_b)
            send(first, stat_copy)

            @pl.when(turn > 0)
            def _():
                send(before, part_copy)

            @pl.when(turn < chips - 1)
            def _():
                wait_queries(after)
            stages(after, scores_a, second, scores_b, weights_b, first, weights_a)
            send(second, stat_copy)
            send(first, part_copy)
            return carry

        @pl.when(chip < mem_chips)
        def _():
            wait_queries(0)
            interleave(score_of(0, scores_a))
            lax.fori_loop(0, chips, turn_body, 0)
            parts = []
            interleave(values_of(weights_b, parts))
            last = pair(jnp.int32(chips - 1)) * CORES + 1
            put_part(last, parts)
            send(last, part_copy)
            part_recv[layer, me] = part_send[layer, me]
            stat_recv[layer, me] = stat_send[layer, me]

        @pl.when(chip >= mem_chips)
        def _():
            for other, name in later:
                weight_copy(name, other).start()
        phase(f'arrived{layer}')

        for src in range(mem_chips * CORES):
            @pl.when(src != me)
            def _():
                stat_arrival(layer, src).wait_recv()
                part_arrival(layer, src).wait_recv()

        phase(f'combine{layer}')
        factors = [None] * (mem_chips * CORES)
        for g in range(CORES):
            members = [c * CORES + g for c in range(mem_chips)]
            tops = [stat_recv[layer, i, 0:hpg] for i in members]
            dens = [stat_recv[layer, i, hpg:2 * hpg] for i in members]
            best = functools.reduce(jnp.maximum, tops)
            shares = [jnp.exp(t - best) for t in tops]
            total = functools.reduce(jnp.add, [s * d for s, d in zip(shares, dens)])
            for i, s in zip(members, shares):
                factors[i] = s / total
        packed = jnp.concatenate(factors + [jnp.zeros((128 - mem_chips * CORES * hpg, rows), F32)], axis=0)
        packed = jnp.transpose(packed)
        lane_group = lane_groups(rows, half, head_dim)
        attended = []
        for g in range(CORES):
            total = jnp.zeros((rows, half), F32)
            for c in range(mem_chips):
                i = c * CORES + g
                factor = jnp.zeros((rows, half), F32)
                for h in range(hpg):
                    factor = jnp.where(lane_group == h, packed[:, i * hpg + h:i * hpg + h + 1], factor)
                total = total + part_recv[layer, i].astype(F32) * factor
            attended.append(total.astype(BF16))
        attended = jnp.concatenate(attended, axis=-1)
        phase(f'co{layer}')
        weight_copy('cross_o', layer).wait()
        hidden = (hid[...].astype(F32) + mm(attended, w['cross_o'][layer])).astype(BF16)

        phase(f'mlp{layer}')
        normed = rms_norm(hidden, norm_mlp[layer:layer + 1, :])
        for name in ('mlp_gate', 'mlp_up', 'mlp_down'):
            weight_copy(name, layer).wait()
        update = None
        for start in range(0, w['mlp_gate'].shape[-1], FF_BLOCK):
            cols = slice(start, start + FF_BLOCK)
            gate = mm(normed, w['mlp_gate'][layer, :, cols])
            up = mm(normed, w['mlp_up'][layer, :, cols])
            act = (gate * jax.nn.sigmoid(gate) * up).astype(BF16)
            part = mm(act, w['mlp_down'][layer, cols, :])
            update = part if update is None else update + part
        hidden = (hidden.astype(F32) + update).astype(BF16)
        hid[...] = hidden

    phase('end')
    out_ref[...] = hid[...]

    @pl.when(chip < mem_chips)
    def _():
        mem_out.wait_send()
    for layer in range(n_layers):
        for condition, copy in x_sends(layer):
            pl.when(condition)(copy.wait_send)
        pl.when(chip == 0)(x_forward_first(layer).wait_send)
        for part in (0, 1):
            pl.when((chip == 1) if part else (chip > 0) & (chip < chips - 1))(x_forward(layer, part).wait_send)
        for turn in range(chips - 1):
            @pl.when(turn < chip)
            def _():
                for part in (0, 1):
                    x_relay_copy(layer, turn, part).wait_send()
        for d in range(1, chips):
            @pl.when(lax.rem(chip + d, chips) < mem_chips)
            def _():
                for k in range(CORES):
                    q_copy(layer, d, k).wait_send()

        @pl.when(chip < mem_chips)
        def _():
            q_to_partner(layer).wait_send()
            for step in range(1, group):
                part_copy(layer, lax.rem(me + step, group)).wait_send()
                stat_copy(layer, lax.rem(me + step, group)).wait_send()
    phase(None)


def solution(mesh):
    group = mesh.shape['sp']
    row_spec = P(('dp', 'sp'), None)

    def local_step(hidden, memory, mem_len, norm_self, norm_cross, norm_mlp, self_q, self_k, self_v, self_o, cross_q, cross_k, cross_v, cross_o, mlp_gate, mlp_up, mlp_down):
        rows, width = hidden.shape
        mem_rows = memory.shape[0]
        n_layers, n_heads, head_dim = self_o.shape[:3]
        inner = n_heads * head_dim
        half = inner // CORES
        hpg = half // head_dim
        all_keys = max(group * rows, CORES * mem_rows)
        weights = dict(
            self_q=self_q, self_k=self_k, self_v=self_v, self_o=self_o.reshape(n_layers, inner, width), cross_k=cross_k, cross_v=cross_v,
            cross_q=cross_q, cross_o=cross_o.reshape(n_layers, inner, width), mlp_gate=mlp_gate, mlp_up=mlp_up, mlp_down=mlp_down)
        w_scratch = [
            pltpu.VMEM((n_layers, width, half) if name in HALVED else weights[name].shape, BF16) for name in WEIGHTS]
        dma = pltpu.SemaphoreType.DMA
        vmem = pl.BlockSpec(memory_space=pltpu.VMEM)
        hbm = pl.BlockSpec(memory_space=pl.ANY)
        return pl.pallas_call(
            functools.partial(kernel, group, n_layers, head_dim),
            out_shape=jax.ShapeDtypeStruct((rows, width), BF16),
            in_specs=[vmem, hbm, pl.BlockSpec(memory_space=pltpu.SMEM), vmem, vmem, vmem] + [hbm] * len(WEIGHTS),
            out_specs=vmem,
            scratch_shapes=w_scratch + [
                pltpu.VMEM((CORES, mem_rows, width), BF16),
                pltpu.VMEM((n_layers, group, rows, width), BF16),
                pltpu.VMEM((group, rows, width), BF16),
                pltpu.VMEM((group, rows, width), BF16),
                pltpu.VMEM((n_layers, CORES * mem_rows, half), BF16),
                pltpu.VMEM((n_layers, CORES * mem_rows, half), BF16),
                pltpu.VMEM((n_layers, CORES, rows, half), BF16),
                pltpu.VMEM((n_layers, group, rows, half), BF16),
                pltpu.VMEM((n_layers, group, rows, half), BF16),
                pltpu.VMEM((n_layers, group, rows, half), BF16),
                pltpu.VMEM((n_layers, group, 2 * hpg, rows), F32),
                pltpu.VMEM((n_layers, group, 2 * hpg, rows), F32),
                pltpu.VMEM((rows, width), BF16),
                pltpu.VMEM((hpg * rows, all_keys), F32),
                pltpu.VMEM((hpg * rows, all_keys), F32),
                pltpu.VMEM((hpg * rows, all_keys), BF16),
                pltpu.VMEM((hpg * rows, all_keys), BF16),
                dma((len(WEIGHTS), n_layers)),
                dma((1,)), dma((1,)), dma((1,)),
                dma((n_layers, 8)), dma((n_layers, group // CORES - 1, 2)), dma((n_layers, group, 2)),
                dma((n_layers, group)), dma((n_layers, group)),
                dma((n_layers, group)), dma((n_layers, group)),
                dma((n_layers, group)), dma((n_layers, group)),
            ],
            compiler_params=pltpu.CompilerParams(collective_id=0, has_side_effects=True, vmem_limit_bytes=60 * 1024 * 1024),
        )(hidden, memory, mem_len, norm_self, norm_cross, norm_mlp, *[weights[name] for name in WEIGHTS])

    return jax.shard_map(local_step, mesh=mesh, in_specs=(row_spec, row_spec, P('dp')) + (P(),) * 14, out_specs=row_spec, check_vma=False)
```

```python
import functools

import jax
import jax.numpy as jnp
from jax import lax
from jax.experimental import pallas as pl
from jax.experimental.pallas import tpu as pltpu
from jax.sharding import PartitionSpec as P

EPS = 1e-6
NEG_BIG = -1e30
CORES = 2
KEY_BLOCK = 512
VALUE_BLOCK = 2048
FF_BLOCK = 512
MEM_BLOCK = 256
ROW_BLOCK = 64
LAG = 1
LOWEST = -3.4e38
MEM_LEN_MAX = 6144
F32 = jnp.float32
BF16 = jnp.bfloat16
MESH = pl.DeviceIdType.MESH
WEIGHTS = ('self_q', 'self_k', 'self_v', 'self_o', 'cross_k', 'cross_v', 'cross_q', 'cross_o', 'mlp_gate', 'mlp_up', 'mlp_down')
HALVED = ('cross_k', 'cross_v')


def rms_norm(hidden, gain_row):
    hidden32 = hidden.astype(F32)
    inv_rms = lax.rsqrt(jnp.mean(hidden32 * hidden32, axis=-1, keepdims=True) + EPS)
    return (hidden32 * inv_rms * gain_row.astype(F32)).astype(BF16)


def mm(a, b):
    return jnp.dot(a, b, preferred_element_type=F32)


def mm_t(a, b):
    return lax.dot_general(a, b, (((1,), (1,)), ((), ())), preferred_element_type=F32)


def lane_groups(rows, lanes, head_dim):
    return lax.broadcasted_iota(jnp.int32, (rows, lanes), 1) // head_dim


def stack_heads(q, head_dim, scale):
    rows, lanes = q.shape
    scaled = q.astype(F32) * scale
    group = lane_groups(rows, lanes, head_dim)
    return jnp.concatenate([jnp.where(group == h, scaled, 0.0).astype(BF16) for h in range(lanes // head_dim)], axis=0)


def score_steps(q_stack, key_block, n_keys, allowed, scores_ref):
    def step(start):
        scores = mm_t(q_stack, key_block(start))
        scores_ref[:, start:start + KEY_BLOCK] = jnp.where(allowed(start), scores, NEG_BIG)
    return [functools.partial(step, start) for start in range(0, n_keys, KEY_BLOCK)]


def exponent_steps(n_keys, scores_ref, weights_ref, tops, dens, lag=0):
    sums = []

    def step(row):
        at = slice(row, row + ROW_BLOCK)
        tiles = [scores_ref[at, lane:lane + 128] for lane in range(0, n_keys, 128)]
        if lag and len(sums) >= lag:
            tiles.insert(0, jnp.minimum(sums[-lag], LOWEST))
        top = jnp.max(functools.reduce(jnp.maximum, tiles), axis=-1, keepdims=True)
        run_sum = None
        for lane in range(0, n_keys, 256):
            weights = jnp.exp(scores_ref[at, lane:lane + 256] - top)
            weights_ref[at, lane:lane + 256] = weights.astype(BF16)
            pair = weights[:, :128] + weights[:, 128:]
            run_sum = pair if run_sum is None else run_sum + pair
        sums.append(run_sum)
        tops.append(top)
        dens.append(jnp.sum(run_sum, axis=-1, keepdims=True))
    return [functools.partial(step, row) for row in range(0, scores_ref.shape[0], ROW_BLOCK)]


def value_steps(value_block, n_keys, weights_ref, parts):
    def step(start):
        stop = min(start + VALUE_BLOCK, n_keys)
        part = mm(weights_ref[:, start:stop], value_block(start, stop))
        parts[:] = [part if not parts else parts[0] + part]
    return [functools.partial(step, start) for start in range(0, n_keys, VALUE_BLOCK)]


def interleave(*lists):
    order = sorted(((i + 0.5) / len(steps), n, i) for n, steps in enumerate(lists) for i in range(len(steps)))
    for _, n, i in order:
        lists[n][i]()


def unstack_heads(stacked, rows, head_dim):
    lanes = stacked.shape[1]
    group = lane_groups(rows, lanes, head_dim)
    out = stacked[:rows]
    for h in range(1, lanes // head_dim):
        out = jnp.where(group == h, stacked[h * rows:(h + 1) * rows], out)
    return out


class Phase:
    def __init__(self):
        self.cur = None

    def __call__(self, name):
        if self.cur is not None:
            self.cur.__exit__(None, None, None)
        self.cur = jax.named_scope(name) if name else None
        if self.cur is not None:
            self.cur.__enter__()


def kernel(group, n_layers, head_dim, *refs):
    n_w = len(WEIGHTS)
    hidden_ref, memory_ref, mem_len_ref, norm_self, norm_cross, norm_mlp = refs[:6]
    w_hbm = dict(zip(WEIGHTS, refs[6:6 + n_w]))
    out_ref = refs[6 + n_w]
    scratch = refs[7 + n_w:]
    w = dict(zip(WEIGHTS, scratch[:n_w]))
    (mem_v, x_all, k_all, v_all, mem_k, mem_vals, q_send, q_all, part_send, part_recv, stat_send, stat_recv, hid, scores_a, scores_b, weights_a, weights_b,
     w_sem, mem_sem, mem_send, mem_recv, x_send, x_relay, x_recv, q_ssem, q_rsem, p_ssem, p_rsem, s_ssem, s_rsem) = scratch[n_w:]

    rows, width = hidden_ref.shape
    mem_rows = memory_ref.shape[0]
    chips = group // CORES
    mem_chips = -(-MEM_LEN_MAX // (CORES * mem_rows))
    half = q_send.shape[-1]
    hpg = half // head_dim
    scale = head_dim ** -0.5
    me = lax.axis_index('sp')
    chip, core = me // CORES, me % CORES
    partner = chip * CORES + (1 - core)

    def remote(src, dst, ssem, rsem, dev):
        return pltpu.make_async_remote_copy(src_ref=src, dst_ref=dst, send_sem=ssem, recv_sem=rsem, device_id={'sp': dev}, device_id_type=MESH)

    def weight_copy(name, layer):
        src = w_hbm[name].at[layer]
        if name in HALVED:
            src = w_hbm[name].at[layer, :, pl.ds(pl.multiple_of(core * half, half), half)]
        return pltpu.make_async_copy(src, w[name].at[layer], w_sem.at[WEIGHTS.index(name), layer])

    phase = Phase()
    phase('start')
    mem_copy = pltpu.make_async_copy(memory_ref, mem_v.at[core], mem_sem.at[0])

    for name in ('self_q', 'self_k', 'self_v'):
        weight_copy(name, 0).start()
    mem_copy.start()
    for layer in range(n_layers):
        for name in HALVED:
            weight_copy(name, layer).start()

    def start_weights(layer, names):
        for name in names:
            weight_copy(name, layer).start()

    phase('barrier')
    barrier = pltpu.get_barrier_semaphore()
    for step in range(1, group):
        pl.semaphore_signal(barrier, inc=1, device_id={'sp': lax.rem(me + step, group)}, device_id_type=MESH)
    pl.semaphore_wait(barrier, group - 1)

    top_chip = chip // (chips - 1)
    half_rows = rows // 2

    def x_copy(layer, src, part, ssem, dst):
        at = x_all.at[layer, src, pl.ds(pl.multiple_of(part * half_rows, half_rows), half_rows)]
        return remote(at, at, ssem, x_recv.at[layer, src, part], dst)

    def x_sends(layer):
        up = me + CORES
        across = (chips - 1) * CORES + core
        send = x_send.at
        return [
            (core == 0, x_copy(layer, me, 0, send[layer, 4], partner)),
            (core == 0, x_copy(layer, me, 1, send[layer, 5], partner)),
            (chip == 1, x_copy(layer, me, 1, send[layer, 2], core)),
            (chip < chips - 1, x_copy(layer, me, 0, send[layer, 0], up)),
            (chip == 0, x_copy(layer, me, 1, send[layer, 2], across)),
            (chip < chips - 1, x_copy(layer, me, 1, send[layer, 1], up)),
            (chip == 0, x_copy(layer, me, 0, send[layer, 3], across)),
        ]

    def x_source(turn):
        return top_chip * (turn * 2 - 3 * (turn // 2)) + (1 - top_chip) * (chip - 1 - turn)

    def x_forward(layer, part):
        return x_copy(layer, x_source(0) * CORES + core, part, x_send.at[layer, 6 + part], me + CORES)

    def x_forward_first(layer):
        return x_copy(layer, CORES + core, 1, x_send.at[layer, 6], (chips - 1) * CORES + core)

    def x_relay_copy(layer, turn, part):
        return x_copy(layer, x_source(turn) * CORES + core, part, x_relay.at[layer, turn, part], partner)

    def x_arrival(layer, src, part):
        return x_copy(layer, src, part, x_send.at[layer, 0], partner)

    def q_copy(layer, d, k):
        dst = lax.rem(chip + d, chips) * CORES + k
        return remote(q_send.at[layer, k], q_all.at[layer, me], q_ssem.at[layer, d * CORES + k], q_rsem.at[layer, me], dst)

    def q_to_partner(layer):
        return remote(q_send.at[layer, 1 - core], q_all.at[layer, me], q_ssem.at[layer, 0], q_rsem.at[layer, me], partner)

    def q_arrival(layer, src):
        return remote(q_send.at[layer, 0], q_all.at[layer, src], q_ssem.at[layer, 0], q_rsem.at[layer, src], partner)

    def part_copy(layer, src):
        return remote(part_send.at[layer, src], part_recv.at[layer, me], p_ssem.at[layer, src], p_rsem.at[layer, me], src)

    def stat_copy(layer, src):
        return remote(stat_send.at[layer, src], stat_recv.at[layer, me], s_ssem.at[layer, src], s_rsem.at[layer, me], src)

    def part_arrival(layer, src):
        return remote(part_send.at[layer, src], part_recv.at[layer, src], p_ssem.at[layer, src], p_rsem.at[layer, src], partner)

    def stat_arrival(layer, src):
        return remote(stat_send.at[layer, src], stat_recv.at[layer, src], s_ssem.at[layer, src], s_rsem.at[layer, src], partner)

    mem_out = remote(mem_v.at[core], mem_v.at[core], mem_send.at[0], mem_recv.at[0], partner)
    mem_in = remote(mem_v.at[1 - core], mem_v.at[1 - core], mem_send.at[0], mem_recv.at[0], partner)

    def project_memory(slot, layer):
        def body(i, carry):
            at = pl.ds(pl.multiple_of(i * MEM_BLOCK, MEM_BLOCK), MEM_BLOCK)
            to = pl.ds(pl.multiple_of(slot * mem_rows + i * MEM_BLOCK, MEM_BLOCK), MEM_BLOCK)
            block = mem_v[slot, at, :]
            mem_k[layer, to, :] = mm(block, w['cross_k'][layer]).astype(BF16)
            mem_vals[layer, to, :] = mm(block, w['cross_v'][layer]).astype(BF16)
            return carry
        lax.fori_loop(0, mem_rows // MEM_BLOCK, body, 0)

    phase('zero')
    hid[...] = hidden_ref[...]
    for src in range(group):
        @pl.when(src > me)
        def _():
            k_all[src] = jnp.zeros((rows, width), BF16)
            v_all[src] = jnp.zeros((rows, width), BF16)

    for layer in range(n_layers):
        phase(f'xnorm{layer}')
        x_all[layer, me] = rms_norm(hid[...], norm_self[layer:layer + 1, :])
        for condition, copy in x_sends(layer):
            pl.when(condition)(copy.start)
        if layer == 0:
            start_weights(0, ('self_o', 'cross_q', 'cross_o'))

        for name in ('self_q', 'self_k', 'self_v'):
            weight_copy(name, layer).wait()

        def project_rows(src):
            block = x_all[layer, src]
            k_all[src] = mm(block, w['self_k'][layer]).astype(BF16)
            v_all[src] = mm(block, w['self_v'][layer]).astype(BF16)

        phase(f'ownproj{layer}')
        project_rows(me)
        queries = mm(x_all[layer, me], w['self_q'][layer]).astype(BF16)

        phase(f'memproj{layer}')
        if layer == 0:
            mem_copy.wait()
            for other in range(n_layers):
                for name in HALVED:
                    weight_copy(name, other).wait()

            @pl.when(chip < mem_chips)
            def _():
                mem_out.start()
                for other in range(n_layers):
                    project_memory(core, other)

        def project_partner_memory():
            if layer == 0:
                mem_in.wait_recv()
            project_memory(1 - core, layer)

        @pl.when(chip == mem_chips - 1)
        def _():
            project_partner_memory()
        phase(f'xwait{layer}')

        @pl.when(chip == 0)
        def _():
            x_arrival(layer, CORES + core, 1).wait_recv()
            x_forward_first(layer).start()

        for turn in range(chips - 1):
            @pl.when(turn < chip)
            def _():
                src = x_source(turn) * CORES + core
                for part in (0, 1):
                    x_arrival(layer, src, part).wait_recv()
                    if turn == 0:
                        pl.when(chip == 1 if part else chip < chips - 1)(x_forward(layer, part).start)
                    x_relay_copy(layer, turn, part).start()
                project_rows(src)

        phase(f'memproj2{layer}')

        @pl.when(chip < mem_chips - 1)
        def _():
            project_partner_memory()

        phase(f'xwait2{layer}')
        @pl.when(core == 1)
        def _():
            for part in (0, 1):
                x_arrival(layer, partner, part).wait_recv()
            project_rows(partner)

        for turn in range(chips - 1):
            @pl.when(turn < chip)
            def _():
                src = x_source(turn) * CORES + (1 - core)
                for part in (0, 1):
                    x_arrival(layer, src, part).wait_recv()
                project_rows(src)

        phase(f'selfatt{layer}')
        all_rows = group * rows
        query_at = me * rows + lax.rem(lax.broadcasted_iota(jnp.int32, (hpg * rows, KEY_BLOCK), 0), rows)
        key_at = lax.broadcasted_iota(jnp.int32, (hpg * rows, KEY_BLOCK), 1)
        per_block = KEY_BLOCK // rows
        stores = ((scores_a, weights_a), (scores_b, weights_b))
        tops, dens, parts = [[], []], [[], []], [[], []]

        def self_steps(g):
            lanes = slice(g * half, (g + 1) * half)
            s_ref, w_ref = stores[g]
            return (
                score_steps(stack_heads(queries[:, lanes], head_dim, scale),
                            lambda start: k_all[start // rows:start // rows + per_block, :, lanes].reshape(KEY_BLOCK, half),
                            all_rows, lambda start: key_at + start <= query_at, s_ref),
                exponent_steps(all_rows, s_ref, w_ref, tops[g], dens[g]),
                value_steps(lambda start, stop: v_all[start // rows:stop // rows, :, lanes].reshape(stop - start, half),
                            all_rows, w_ref, parts[g]))

        steps = [self_steps(g) for g in range(CORES)]
        interleave(steps[0][0])
        interleave(steps[0][1], steps[1][0])
        interleave(steps[0][2], steps[1][1])
        interleave(steps[1][2])
        attended = [unstack_heads(parts[g][0] / jnp.concatenate(dens[g], axis=0), rows, head_dim).astype(BF16) for g in range(CORES)]
        attended = jnp.concatenate(attended, axis=-1)
        phase(f'oproj{layer}')
        weight_copy('self_o', layer).wait()
        hidden = (hid[...].astype(F32) + mm(attended, w['self_o'][layer])).astype(BF16)
        hid[...] = hidden

        phase(f'qproj{layer}')
        weight_copy('cross_q', layer).wait()
        queries = mm(rms_norm(hidden, norm_cross[layer:layer + 1, :]), w['cross_q'][layer]).astype(BF16)
        for g in range(CORES):
            q_send[layer, g] = queries[:, g * half:(g + 1) * half]
        q_order = [(d, k) for d in (1, 3, 2) if d < chips for k in range(CORES)]

        @pl.when(chip < mem_chips)
        def _():
            q_to_partner(layer).start()
        for d, k in q_order:
            @pl.when(lax.rem(chip + d, chips) < mem_chips)
            def _():
                q_copy(layer, d, k).start()
        q_all[layer, me] = q_send[layer, core]
        later = []
        if layer == 0:
            later = [(0, name) for name in ('mlp_gate', 'mlp_up', 'mlp_down')]
            later += [(other, name) for other in range(1, n_layers) for name in WEIGHTS if name not in HALVED]

        mem_at = chip * (CORES * mem_rows) + lax.broadcasted_iota(jnp.int32, (1, KEY_BLOCK), 1)
        n_keys = CORES * mem_rows

        def wait_queries(src):
            @pl.when(src != me)
            def _():
                q_arrival(layer, src).wait_recv()

        def score_of(src, scores_ref):
            return score_steps(stack_heads(q_all[layer, src], head_dim, scale), lambda start: mem_k[layer, start:start + KEY_BLOCK, :], n_keys,
                               lambda start: mem_at + start < mem_len_ref[0], scores_ref)

        def put_stats(src, tops, dens):
            top, den = jnp.concatenate(tops, axis=0), jnp.concatenate(dens, axis=0)
            lane = lax.broadcasted_iota(jnp.int32, (rows, 128), 1)
            stats = jnp.zeros((rows, 128), F32)
            for h in range(hpg):
                stats = jnp.where(lane == h, top[h * rows:(h + 1) * rows], stats)
                stats = jnp.where(lane == hpg + h, den[h * rows:(h + 1) * rows], stats)
            stat_send[layer, src] = jnp.transpose(stats)[:2 * hpg]

        def values_of(weights_ref, parts):
            return value_steps(lambda start, stop: mem_vals[layer, start:stop, :], n_keys, weights_ref, parts)

        def put_part(src, parts):
            part_send[layer, src] = unstack_heads(parts[0], rows, head_dim).astype(BF16)

        def stages(after, s_after, now, s_now, w_now, before, w_before):
            tops, dens, parts = [], [], []
            interleave(score_of(after, s_after), exponent_steps(n_keys, s_now, w_now, tops, dens, LAG), values_of(w_before, parts))
            put_stats(now, tops, dens)
            put_part(before, parts)

        def send(src, copy):
            @pl.when(src != me)
            def _():
                copy(layer, src).start()

        phase(f'cross{layer}')

        def pair(turn):
            return turn + (chip // (mem_chips - 1)) * (turn // 2) * (1 - 2 * lax.rem(turn, 2))

        def turn_body(turn, carry):
            first = pair(turn) * CORES
            for i in range(group // 2):
                if later:
                    @pl.when(turn == i)
                    def _():
                        for other, name in later[i::group // 2]:
                            weight_copy(name, other).start()
            second = first + 1
            before = pair(lax.rem(turn + chips - 1, chips)) * CORES + 1
            after = pair(lax.rem(turn + 1, chips)) * CORES
            wait_queries(second)
            stages(second, scores_b, first, scores_a, weights_a, before, weights_b)
            send(first, stat_copy)

            @pl.when(turn > 0)
            def _():
                send(before, part_copy)

            @pl.when(turn < chips - 1)
            def _():
                wait_queries(after)
            stages(after, scores_a, second, scores_b, weights_b, first, weights_a)
            send(second, stat_copy)
            send(first, part_copy)
            return carry

        @pl.when(chip < mem_chips)
        def _():
            wait_queries(0)
            interleave(score_of(0, scores_a))
            lax.fori_loop(0, chips, turn_body, 0)
            parts = []
            interleave(values_of(weights_b, parts))
            last = pair(jnp.int32(chips - 1)) * CORES + 1
            put_part(last, parts)
            send(last, part_copy)
            part_recv[layer, me] = part_send[layer, me]
            stat_recv[layer, me] = stat_send[layer, me]

        @pl.when(chip >= mem_chips)
        def _():
            for other, name in later:
                weight_copy(name, other).start()
        phase(f'arrived{layer}')

        for src in range(mem_chips * CORES):
            @pl.when(src != me)
            def _():
                stat_arrival(layer, src).wait_recv()
                part_arrival(layer, src).wait_recv()

        phase(f'combine{layer}')
        factors = [None] * (mem_chips * CORES)
        for g in range(CORES):
            members = [c * CORES + g for c in range(mem_chips)]
            tops = [stat_recv[layer, i, 0:hpg] for i in members]
            dens = [stat_recv[layer, i, hpg:2 * hpg] for i in members]
            best = functools.reduce(jnp.maximum, tops)
            shares = [jnp.exp(t - best) for t in tops]
            total = functools.reduce(jnp.add, [s * d for s, d in zip(shares, dens)])
            for i, s in zip(members, shares):
                factors[i] = s / total
        packed = jnp.concatenate(factors + [jnp.zeros((128 - mem_chips * CORES * hpg, rows), F32)], axis=0)
        packed = jnp.transpose(packed)
        lane_group = lane_groups(rows, half, head_dim)
        attended = []
        for g in range(CORES):
            total = jnp.zeros((rows, half), F32)
            for c in range(mem_chips):
                i = c * CORES + g
                factor = jnp.zeros((rows, half), F32)
                for h in range(hpg):
                    factor = jnp.where(lane_group == h, packed[:, i * hpg + h:i * hpg + h + 1], factor)
                total = total + part_recv[layer, i].astype(F32) * factor
            attended.append(total.astype(BF16))
        attended = jnp.concatenate(attended, axis=-1)
        phase(f'co{layer}')
        weight_copy('cross_o', layer).wait()
        hidden = (hid[...].astype(F32) + mm(attended, w['cross_o'][layer])).astype(BF16)

        phase(f'mlp{layer}')
        normed = rms_norm(hidden, norm_mlp[layer:layer + 1, :])
        for name in ('mlp_gate', 'mlp_up', 'mlp_down'):
            weight_copy(name, layer).wait()
        update = None
        for start in range(0, w['mlp_gate'].shape[-1], FF_BLOCK):
            cols = slice(start, start + FF_BLOCK)
            gate = mm(normed, w['mlp_gate'][layer, :, cols])
            up = mm(normed, w['mlp_up'][layer, :, cols])
            act = (gate * jax.nn.sigmoid(gate) * up).astype(BF16)
            part = mm(act, w['mlp_down'][layer, cols, :])
            update = part if update is None else update + part
        hidden = (hidden.astype(F32) + update).astype(BF16)
        hid[...] = hidden

    phase('end')
    out_ref[...] = hid[...]

    @pl.when(chip < mem_chips)
    def _():
        mem_out.wait_send()
    for layer in range(n_layers):
        for condition, copy in x_sends(layer):
            pl.when(condition)(copy.wait_send)
        pl.when(chip == 0)(x_forward_first(layer).wait_send)
        for part in (0, 1):
            pl.when((chip == 1) if part else (chip > 0) & (chip < chips - 1))(x_forward(layer, part).wait_send)
        for turn in range(chips - 1):
            @pl.when(turn < chip)
            def _():
                for part in (0, 1):
                    x_relay_copy(layer, turn, part).wait_send()
        for d in range(1, chips):
            @pl.when(lax.rem(chip + d, chips) < mem_chips)
            def _():
                for k in range(CORES):
                    q_copy(layer, d, k).wait_send()

        @pl.when(chip < mem_chips)
        def _():
            q_to_partner(layer).wait_send()
            for step in range(1, group):
                part_copy(layer, lax.rem(me + step, group)).wait_send()
                stat_copy(layer, lax.rem(me + step, group)).wait_send()
    phase(None)


def solution(mesh):
    group = mesh.shape['sp']
    row_spec = P(('dp', 'sp'), None)

    def local_step(hidden, memory, mem_len, norm_self, norm_cross, norm_mlp, self_q, self_k, self_v, self_o, cross_q, cross_k, cross_v, cross_o, mlp_gate, mlp_up, mlp_down):
        rows, width = hidden.shape
        mem_rows = memory.shape[0]
        n_layers, n_heads, head_dim = self_o.shape[:3]
        inner = n_heads * head_dim
        half = inner // CORES
        hpg = half // head_dim
        all_keys = max(group * rows, CORES * mem_rows)
        weights = dict(
            self_q=self_q, self_k=self_k, self_v=self_v, self_o=self_o.reshape(n_layers, inner, width), cross_k=cross_k, cross_v=cross_v,
            cross_q=cross_q, cross_o=cross_o.reshape(n_layers, inner, width), mlp_gate=mlp_gate, mlp_up=mlp_up, mlp_down=mlp_down)
        w_scratch = [
            pltpu.VMEM((n_layers, width, half) if name in HALVED else weights[name].shape, BF16) for name in WEIGHTS]
        dma = pltpu.SemaphoreType.DMA
        vmem = pl.BlockSpec(memory_space=pltpu.VMEM)
        hbm = pl.BlockSpec(memory_space=pl.ANY)
        return pl.pallas_call(
            functools.partial(kernel, group, n_layers, head_dim),
            out_shape=jax.ShapeDtypeStruct((rows, width), BF16),
            in_specs=[vmem, hbm, pl.BlockSpec(memory_space=pltpu.SMEM), vmem, vmem, vmem] + [hbm] * len(WEIGHTS),
            out_specs=vmem,
            scratch_shapes=w_scratch + [
                pltpu.VMEM((CORES, mem_rows, width), BF16),
                pltpu.VMEM((n_layers, group, rows, width), BF16),
                pltpu.VMEM((group, rows, width), BF16),
                pltpu.VMEM((group, rows, width), BF16),
                pltpu.VMEM((n_layers, CORES * mem_rows, half), BF16),
                pltpu.VMEM((n_layers, CORES * mem_rows, half), BF16),
                pltpu.VMEM((n_layers, CORES, rows, half), BF16),
                pltpu.VMEM((n_layers, group, rows, half), BF16),
                pltpu.VMEM((n_layers, group, rows, half), BF16),
                pltpu.VMEM((n_layers, group, rows, half), BF16),
                pltpu.VMEM((n_layers, group, 2 * hpg, rows), F32),
                pltpu.VMEM((n_layers, group, 2 * hpg, rows), F32),
                pltpu.VMEM((rows, width), BF16),
                pltpu.VMEM((hpg * rows, all_keys), F32),
                pltpu.VMEM((hpg * rows, all_keys), F32),
                pltpu.VMEM((hpg * rows, all_keys), BF16),
                pltpu.VMEM((hpg * rows, all_keys), BF16),
                dma((len(WEIGHTS), n_layers)),
                dma((1,)), dma((1,)), dma((1,)),
                dma((n_layers, 8)), dma((n_layers, group // CORES - 1, 2)), dma((n_layers, group, 2)),
                dma((n_layers, group)), dma((n_layers, group)),
                dma((n_layers, group)), dma((n_layers, group)),
                dma((n_layers, group)), dma((n_layers, group)),
            ],
            compiler_params=pltpu.CompilerParams(collective_id=0, has_side_effects=True, vmem_limit_bytes=60 * 1024 * 1024),
        )(hidden, memory, mem_len, norm_self, norm_cross, norm_mlp, *[weights[name] for name in WEIGHTS])

    return jax.shard_map(local_step, mesh=mesh, in_specs=(row_spec, row_spec, P('dp')) + (P(),) * 14, out_specs=row_spec, check_vma=False)
```

```python
import functools

import jax
import jax.numpy as jnp
from jax import lax
from jax.experimental import pallas as pl
from jax.experimental.pallas import tpu as pltpu
from jax.sharding import PartitionSpec as P

EPS = 1e-6
NEG_BIG = -1e30
CORES = 2
KEY_BLOCK = 512
VALUE_BLOCK = 2048
FF_BLOCK = 512
MEM_BLOCK = 256
ROW_BLOCK = 64
LAG = 1
LOWEST = -3.4e38
MEM_LEN_MAX = 6144
F32 = jnp.float32
BF16 = jnp.bfloat16
MESH = pl.DeviceIdType.MESH
WEIGHTS = ('self_q', 'self_k', 'self_v', 'self_o', 'cross_k', 'cross_v', 'cross_q', 'cross_o', 'mlp_gate', 'mlp_up', 'mlp_down')
HALVED = ('cross_k', 'cross_v')


def rms_norm(hidden, gain_row):
    hidden32 = hidden.astype(F32)
    inv_rms = lax.rsqrt(jnp.mean(hidden32 * hidden32, axis=-1, keepdims=True) + EPS)
    return (hidden32 * inv_rms * gain_row.astype(F32)).astype(BF16)


def mm(a, b):
    return jnp.dot(a, b, preferred_element_type=F32)


def mm_t(a, b):
    return lax.dot_general(a, b, (((1,), (1,)), ((), ())), preferred_element_type=F32)


def lane_groups(rows, lanes, head_dim):
    return lax.broadcasted_iota(jnp.int32, (rows, lanes), 1) // head_dim


def stack_heads(q, head_dim, scale):
    rows, lanes = q.shape
    scaled = q.astype(F32) * scale
    group = lane_groups(rows, lanes, head_dim)
    return jnp.concatenate([jnp.where(group == h, scaled, 0.0).astype(BF16) for h in range(lanes // head_dim)], axis=0)


def score_steps(q_stack, key_block, n_keys, allowed, scores_ref):
    def step(start):
        scores = mm_t(q_stack, key_block(start))
        scores_ref[:, start:start + KEY_BLOCK] = jnp.where(allowed(start), scores, NEG_BIG)
    return [functools.partial(step, start) for start in range(0, n_keys, KEY_BLOCK)]


def exponent_steps(n_keys, scores_ref, weights_ref, tops, dens, lag=0):
    sums = []

    def step(row):
        at = slice(row, row + ROW_BLOCK)
        tiles = [scores_ref[at, lane:lane + 128] for lane in range(0, n_keys, 128)]
        if lag and len(sums) >= lag:
            tiles.insert(0, jnp.minimum(sums[-lag], LOWEST))
        top = jnp.max(functools.reduce(jnp.maximum, tiles), axis=-1, keepdims=True)
        run_sum = None
        for lane in range(0, n_keys, 256):
            weights = jnp.exp(scores_ref[at, lane:lane + 256] - top)
            weights_ref[at, lane:lane + 256] = weights.astype(BF16)
            pair = weights[:, :128] + weights[:, 128:]
            run_sum = pair if run_sum is None else run_sum + pair
        sums.append(run_sum)
        tops.append(top)
        dens.append(jnp.sum(run_sum, axis=-1, keepdims=True))
    return [functools.partial(step, row) for row in range(0, scores_ref.shape[0], ROW_BLOCK)]


def value_steps(value_block, n_keys, weights_ref, parts):
    def step(start):
        stop = min(start + VALUE_BLOCK, n_keys)
        part = mm(weights_ref[:, start:stop], value_block(start, stop))
        parts[:] = [part if not parts else parts[0] + part]
    return [functools.partial(step, start) for start in range(0, n_keys, VALUE_BLOCK)]


def interleave(*lists):
    order = sorted(((i + 0.5) / len(steps), n, i) for n, steps in enumerate(lists) for i in range(len(steps)))
    for _, n, i in order:
        lists[n][i]()


def unstack_heads(stacked, rows, head_dim):
    lanes = stacked.shape[1]
    group = lane_groups(rows, lanes, head_dim)
    out = stacked[:rows]
    for h in range(1, lanes // head_dim):
        out = jnp.where(group == h, stacked[h * rows:(h + 1) * rows], out)
    return out


class Phase:
    def __init__(self):
        self.cur = None

    def __call__(self, name):
        if self.cur is not None:
            self.cur.__exit__(None, None, None)
        self.cur = jax.named_scope(name) if name else None
        if self.cur is not None:
            self.cur.__enter__()


def kernel(group, n_layers, head_dim, *refs):
    n_w = len(WEIGHTS)
    hidden_ref, memory_ref, mem_len_ref, norm_self, norm_cross, norm_mlp = refs[:6]
    w_hbm = dict(zip(WEIGHTS, refs[6:6 + n_w]))
    out_ref = refs[6 + n_w]
    scratch = refs[7 + n_w:]
    w = dict(zip(WEIGHTS, scratch[:n_w]))
    (mem_v, x_all, k_all, v_all, mem_k, mem_vals, q_send, q_all, part_send, part_recv, stat_send, stat_recv, hid, scores_a, scores_b, weights_a, weights_b,
     w_sem, mem_sem, mem_send, mem_recv, x_send, x_relay, x_recv, q_ssem, q_rsem, p_ssem, p_rsem, s_ssem, s_rsem) = scratch[n_w:]

    rows, width = hidden_ref.shape
    mem_rows = memory_ref.shape[0]
    chips = group // CORES
    mem_chips = -(-MEM_LEN_MAX // (CORES * mem_rows))
    half = q_send.shape[-1]
    hpg = half // head_dim
    scale = head_dim ** -0.5
    me = lax.axis_index('sp')
    chip, core = me // CORES, me % CORES
    partner = chip * CORES + (1 - core)

    def remote(src, dst, ssem, rsem, dev):
        return pltpu.make_async_remote_copy(src_ref=src, dst_ref=dst, send_sem=ssem, recv_sem=rsem, device_id={'sp': dev}, device_id_type=MESH)

    def weight_copy(name, layer):
        src = w_hbm[name].at[layer]
        if name in HALVED:
            src = w_hbm[name].at[layer, :, pl.ds(pl.multiple_of(core * half, half), half)]
        return pltpu.make_async_copy(src, w[name].at[layer], w_sem.at[WEIGHTS.index(name), layer])

    phase = Phase()
    phase('start')
    mem_copy = pltpu.make_async_copy(memory_ref, mem_v.at[core], mem_sem.at[0])

    for name in ('self_q', 'self_k', 'self_v'):
        weight_copy(name, 0).start()
    mem_copy.start()
    for layer in range(n_layers):
        for name in HALVED:
            weight_copy(name, layer).start()

    def start_weights(layer, names):
        for name in names:
            weight_copy(name, layer).start()

    phase('barrier')
    barrier = pltpu.get_barrier_semaphore()
    for step in range(1, group):
        pl.semaphore_signal(barrier, inc=1, device_id={'sp': lax.rem(me + step, group)}, device_id_type=MESH)
    pl.semaphore_wait(barrier, group - 1)

    top_chip = chip // (chips - 1)
    half_rows = rows // 2

    def x_copy(layer, src, part, ssem, dst):
        at = x_all.at[layer, src, pl.ds(pl.multiple_of(part * half_rows, half_rows), half_rows)]
        return remote(at, at, ssem, x_recv.at[layer, src, part], dst)

    def x_sends(layer):
        up = me + CORES
        across = (chips - 1) * CORES + core
        send = x_send.at
        return [
            (core == 0, x_copy(layer, me, 0, send[layer, 4], partner)),
            (core == 0, x_copy(layer, me, 1, send[layer, 5], partner)),
            (chip == 1, x_copy(layer, me, 1, send[layer, 2], core)),
            (chip < chips - 1, x_copy(layer, me, 0, send[layer, 0], up)),
            (chip == 0, x_copy(layer, me, 1, send[layer, 2], across)),
            (chip < chips - 1, x_copy(layer, me, 1, send[layer, 1], up)),
            (chip == 0, x_copy(layer, me, 0, send[layer, 3], across)),
        ]

    def x_source(turn):
        return top_chip * (turn * 2 - 3 * (turn // 2)) + (1 - top_chip) * (chip - 1 - turn)

    def x_forward(layer, part):
        return x_copy(layer, x_source(0) * CORES + core, part, x_send.at[layer, 6 + part], me + CORES)

    def x_forward_first(layer):
        return x_copy(layer, CORES + core, 1, x_send.at[layer, 6], (chips - 1) * CORES + core)

    def x_relay_copy(layer, turn, part):
        return x_copy(layer, x_source(turn) * CORES + core, part, x_relay.at[layer, turn, part], partner)

    def x_arrival(layer, src, part):
        return x_copy(layer, src, part, x_send.at[layer, 0], partner)

    def q_copy(layer, d, k):
        dst = lax.rem(chip + d, chips) * CORES + k
        return remote(q_send.at[layer, k], q_all.at[layer, me], q_ssem.at[layer, d * CORES + k], q_rsem.at[layer, me], dst)

    def q_to_partner(layer):
        return remote(q_send.at[layer, 1 - core], q_all.at[layer, me], q_ssem.at[layer, 0], q_rsem.at[layer, me], partner)

    def q_arrival(layer, src):
        return remote(q_send.at[layer, 0], q_all.at[layer, src], q_ssem.at[layer, 0], q_rsem.at[layer, src], partner)

    def part_copy(layer, src):
        return remote(part_send.at[layer, src], part_recv.at[layer, me], p_ssem.at[layer, src], p_rsem.at[layer, me], src)

    def stat_copy(layer, src):
        return remote(stat_send.at[layer, src], stat_recv.at[layer, me], s_ssem.at[layer, src], s_rsem.at[layer, me], src)

    def part_arrival(layer, src):
        return remote(part_send.at[layer, src], part_recv.at[layer, src], p_ssem.at[layer, src], p_rsem.at[layer, src], partner)

    def stat_arrival(layer, src):
        return remote(stat_send.at[layer, src], stat_recv.at[layer, src], s_ssem.at[layer, src], s_rsem.at[layer, src], partner)

    mem_out = remote(mem_v.at[core], mem_v.at[core], mem_send.at[0], mem_recv.at[0], partner)
    mem_in = remote(mem_v.at[1 - core], mem_v.at[1 - core], mem_send.at[0], mem_recv.at[0], partner)

    def project_memory(slot, layer):
        def body(i, carry):
            at = pl.ds(pl.multiple_of(i * MEM_BLOCK, MEM_BLOCK), MEM_BLOCK)
            to = pl.ds(pl.multiple_of(slot * mem_rows + i * MEM_BLOCK, MEM_BLOCK), MEM_BLOCK)
            block = mem_v[slot, at, :]
            mem_k[layer, to, :] = mm(block, w['cross_k'][layer]).astype(BF16)
            mem_vals[layer, to, :] = mm(block, w['cross_v'][layer]).astype(BF16)
            return carry
        lax.fori_loop(0, mem_rows // MEM_BLOCK, body, 0)

    phase('zero')
    hid[...] = hidden_ref[...]
    for src in range(group):
        @pl.when(src > me)
        def _():
            k_all[src] = jnp.zeros((rows, width), BF16)
            v_all[src] = jnp.zeros((rows, width), BF16)

    for layer in range(n_layers):
        phase(f'xnorm{layer}')
        x_all[layer, me] = rms_norm(hid[...], norm_self[layer:layer + 1, :])
        for condition, copy in x_sends(layer):
            pl.when(condition)(copy.start)
        if layer == 0:
            start_weights(0, ('self_o', 'cross_q', 'cross_o'))

        for name in ('self_q', 'self_k', 'self_v'):
            weight_copy(name, layer).wait()

        def project_rows(src):
            block = x_all[layer, src]
            k_all[src] = mm(block, w['self_k'][layer]).astype(BF16)
            v_all[src] = mm(block, w['self_v'][layer]).astype(BF16)

        phase(f'ownproj{layer}')
        project_rows(me)
        queries = mm(x_all[layer, me], w['self_q'][layer]).astype(BF16)

        phase(f'memproj{layer}')
        if layer == 0:
            mem_copy.wait()
            for other in range(n_layers):
                for name in HALVED:
                    weight_copy(name, other).wait()

            @pl.when(chip < mem_chips)
            def _():
                mem_out.start()
                for other in range(n_layers):
                    project_memory(core, other)

        def project_partner_memory():
            if layer == 0:
                mem_in.wait_recv()
            project_memory(1 - core, layer)

        @pl.when(chip == mem_chips - 1)
        def _():
            project_partner_memory()
        phase(f'xwait{layer}')

        def forward_first():
            x_arrival(layer, CORES + core, 1).wait_recv()
            x_forward_first(layer).start()

        if layer == 0:
            pl.when(chip == 0)(forward_first)

        for turn in range(chips - 1):
            @pl.when(turn < chip)
            def _():
                src = x_source(turn) * CORES + core
                for part in (0, 1):
                    x_arrival(layer, src, part).wait_recv()
                    if turn == 0:
                        pl.when(chip == 1 if part else chip < chips - 1)(x_forward(layer, part).start)
                    x_relay_copy(layer, turn, part).start()
                project_rows(src)

        phase(f'memproj2{layer}')

        @pl.when(chip < mem_chips - 1)
        def _():
            project_partner_memory()

        phase(f'xwait2{layer}')
        @pl.when(core == 1)
        def _():
            for part in (0, 1):
                x_arrival(layer, partner, part).wait_recv()
            project_rows(partner)

        for turn in range(chips - 1):
            @pl.when(turn < chip)
            def _():
                src = x_source(turn) * CORES + (1 - core)
                for part in (0, 1):
                    x_arrival(layer, src, part).wait_recv()
                project_rows(src)

        phase(f'selfatt{layer}')
        all_rows = group * rows
        query_at = me * rows + lax.rem(lax.broadcasted_iota(jnp.int32, (hpg * rows, KEY_BLOCK), 0), rows)
        key_at = lax.broadcasted_iota(jnp.int32, (hpg * rows, KEY_BLOCK), 1)
        per_block = KEY_BLOCK // rows
        stores = ((scores_a, weights_a), (scores_b, weights_b))
        tops, dens, parts = [[], []], [[], []], [[], []]

        def self_steps(g):
            lanes = slice(g * half, (g + 1) * half)
            s_ref, w_ref = stores[g]
            return (
                score_steps(stack_heads(queries[:, lanes], head_dim, scale),
                            lambda start: k_all[start // rows:start // rows + per_block, :, lanes].reshape(KEY_BLOCK, half),
                            all_rows, lambda start: key_at + start <= query_at, s_ref),
                exponent_steps(all_rows, s_ref, w_ref, tops[g], dens[g]),
                value_steps(lambda start, stop: v_all[start // rows:stop // rows, :, lanes].reshape(stop - start, half),
                            all_rows, w_ref, parts[g]))

        steps = [self_steps(g) for g in range(CORES)]
        interleave(steps[0][0])
        interleave(steps[0][1], steps[1][0])
        interleave(steps[0][2], steps[1][1])
        interleave(steps[1][2])
        attended = [unstack_heads(parts[g][0] / jnp.concatenate(dens[g], axis=0), rows, head_dim).astype(BF16) for g in range(CORES)]
        attended = jnp.concatenate(attended, axis=-1)
        phase(f'oproj{layer}')
        weight_copy('self_o', layer).wait()
        hidden = (hid[...].astype(F32) + mm(attended, w['self_o'][layer])).astype(BF16)
        hid[...] = hidden

        phase(f'qproj{layer}')
        weight_copy('cross_q', layer).wait()
        queries = mm(rms_norm(hidden, norm_cross[layer:layer + 1, :]), w['cross_q'][layer]).astype(BF16)
        for g in range(CORES):
            q_send[layer, g] = queries[:, g * half:(g + 1) * half]
        q_order = [(d, k) for d in (1, 3, 2) if d < chips for k in range(CORES)]

        @pl.when(chip < mem_chips)
        def _():
            q_to_partner(layer).start()
        for d, k in q_order:
            @pl.when(lax.rem(chip + d, chips) < mem_chips)
            def _():
                q_copy(layer, d, k).start()
        q_all[layer, me] = q_send[layer, core]
        if layer > 0:
            pl.when(chip == 0)(forward_first)
        later = []
        if layer == 0:
            later = [(0, name) for name in ('mlp_gate', 'mlp_up', 'mlp_down')]
            later += [(other, name) for other in range(1, n_layers) for name in WEIGHTS if name not in HALVED]

        mem_at = chip * (CORES * mem_rows) + lax.broadcasted_iota(jnp.int32, (1, KEY_BLOCK), 1)
        n_keys = CORES * mem_rows

        def wait_queries(src):
            @pl.when(src != me)
            def _():
                q_arrival(layer, src).wait_recv()

        def score_of(src, scores_ref):
            return score_steps(stack_heads(q_all[layer, src], head_dim, scale), lambda start: mem_k[layer, start:start + KEY_BLOCK, :], n_keys,
                               lambda start: mem_at + start < mem_len_ref[0], scores_ref)

        def put_stats(src, tops, dens):
            top, den = jnp.concatenate(tops, axis=0), jnp.concatenate(dens, axis=0)
            lane = lax.broadcasted_iota(jnp.int32, (rows, 128), 1)
            stats = jnp.zeros((rows, 128), F32)
            for h in range(hpg):
                stats = jnp.where(lane == h, top[h * rows:(h + 1) * rows], stats)
                stats = jnp.where(lane == hpg + h, den[h * rows:(h + 1) * rows], stats)
            stat_send[layer, src] = jnp.transpose(stats)[:2 * hpg]

        def values_of(weights_ref, parts):
            return value_steps(lambda start, stop: mem_vals[layer, start:stop, :], n_keys, weights_ref, parts)

        def put_part(src, parts):
            part_send[layer, src] = unstack_heads(parts[0], rows, head_dim).astype(BF16)

        def stages(after, s_after, now, s_now, w_now, before, w_before):
            tops, dens, parts = [], [], []
            interleave(score_of(after, s_after), exponent_steps(n_keys, s_now, w_now, tops, dens, LAG), values_of(w_before, parts))
            put_stats(now, tops, dens)
            put_part(before, parts)

        def send(src, copy):
            @pl.when(src != me)
            def _():
                copy(layer, src).start()

        phase(f'cross{layer}')

        def pair(turn):
            return turn + (chip // (mem_chips - 1)) * (turn // 2) * (1 - 2 * lax.rem(turn, 2))

        def turn_body(turn, carry):
            first = pair(turn) * CORES
            for i in range(group // 2):
                if later:
                    @pl.when(turn == i)
                    def _():
                        for other, name in later[i::group // 2]:
                            weight_copy(name, other).start()
            second = first + 1
            before = pair(lax.rem(turn + chips - 1, chips)) * CORES + 1
            after = pair(lax.rem(turn + 1, chips)) * CORES
            wait_queries(second)
            stages(second, scores_b, first, scores_a, weights_a, before, weights_b)
            send(first, stat_copy)

            @pl.when(turn > 0)
            def _():
                send(before, part_copy)

            @pl.when(turn < chips - 1)
            def _():
                wait_queries(after)
            stages(after, scores_a, second, scores_b, weights_b, first, weights_a)
            send(second, stat_copy)
            send(first, part_copy)
            return carry

        @pl.when(chip < mem_chips)
        def _():
            wait_queries(0)
            interleave(score_of(0, scores_a))
            lax.fori_loop(0, chips, turn_body, 0)
            parts = []
            interleave(values_of(weights_b, parts))
            last = pair(jnp.int32(chips - 1)) * CORES + 1
            put_part(last, parts)
            send(last, part_copy)
            part_recv[layer, me] = part_send[layer, me]
            stat_recv[layer, me] = stat_send[layer, me]

        @pl.when(chip >= mem_chips)
        def _():
            for other, name in later:
                weight_copy(name, other).start()
        phase(f'arrived{layer}')

        for src in range(mem_chips * CORES):
            @pl.when(src != me)
            def _():
                stat_arrival(layer, src).wait_recv()
                part_arrival(layer, src).wait_recv()

        phase(f'combine{layer}')
        factors = [None] * (mem_chips * CORES)
        for g in range(CORES):
            members = [c * CORES + g for c in range(mem_chips)]
            tops = [stat_recv[layer, i, 0:hpg] for i in members]
            dens = [stat_recv[layer, i, hpg:2 * hpg] for i in members]
            best = functools.reduce(jnp.maximum, tops)
            shares = [jnp.exp(t - best) for t in tops]
            total = functools.reduce(jnp.add, [s * d for s, d in zip(shares, dens)])
            for i, s in zip(members, shares):
                factors[i] = s / total
        packed = jnp.concatenate(factors + [jnp.zeros((128 - mem_chips * CORES * hpg, rows), F32)], axis=0)
        packed = jnp.transpose(packed)
        lane_group = lane_groups(rows, half, head_dim)
        attended = []
        for g in range(CORES):
            total = jnp.zeros((rows, half), F32)
            for c in range(mem_chips):
                i = c * CORES + g
                factor = jnp.zeros((rows, half), F32)
                for h in range(hpg):
                    factor = jnp.where(lane_group == h, packed[:, i * hpg + h:i * hpg + h + 1], factor)
                total = total + part_recv[layer, i].astype(F32) * factor
            attended.append(total.astype(BF16))
        attended = jnp.concatenate(attended, axis=-1)
        phase(f'co{layer}')
        weight_copy('cross_o', layer).wait()
        hidden = (hid[...].astype(F32) + mm(attended, w['cross_o'][layer])).astype(BF16)

        phase(f'mlp{layer}')
        normed = rms_norm(hidden, norm_mlp[layer:layer + 1, :])
        for name in ('mlp_gate', 'mlp_up', 'mlp_down'):
            weight_copy(name, layer).wait()
        update = None
        for start in range(0, w['mlp_gate'].shape[-1], FF_BLOCK):
            cols = slice(start, start + FF_BLOCK)
            gate = mm(normed, w['mlp_gate'][layer, :, cols])
            up = mm(normed, w['mlp_up'][layer, :, cols])
            act = (gate * jax.nn.sigmoid(gate) * up).astype(BF16)
            part = mm(act, w['mlp_down'][layer, cols, :])
            update = part if update is None else update + part
        hidden = (hidden.astype(F32) + update).astype(BF16)
        hid[...] = hidden

    phase('end')
    out_ref[...] = hid[...]

    @pl.when(chip < mem_chips)
    def _():
        mem_out.wait_send()
    for layer in range(n_layers):
        for condition, copy in x_sends(layer):
            pl.when(condition)(copy.wait_send)
        pl.when(chip == 0)(x_forward_first(layer).wait_send)
        for part in (0, 1):
            pl.when((chip == 1) if part else (chip > 0) & (chip < chips - 1))(x_forward(layer, part).wait_send)
        for turn in range(chips - 1):
            @pl.when(turn < chip)
            def _():
                for part in (0, 1):
                    x_relay_copy(layer, turn, part).wait_send()
        for d in range(1, chips):
            @pl.when(lax.rem(chip + d, chips) < mem_chips)
            def _():
                for k in range(CORES):
                    q_copy(layer, d, k).wait_send()

        @pl.when(chip < mem_chips)
        def _():
            q_to_partner(layer).wait_send()
            for step in range(1, group):
                part_copy(layer, lax.rem(me + step, group)).wait_send()
                stat_copy(layer, lax.rem(me + step, group)).wait_send()
    phase(None)


def solution(mesh):
    group = mesh.shape['sp']
    row_spec = P(('dp', 'sp'), None)

    def local_step(hidden, memory, mem_len, norm_self, norm_cross, norm_mlp, self_q, self_k, self_v, self_o, cross_q, cross_k, cross_v, cross_o, mlp_gate, mlp_up, mlp_down):
        rows, width = hidden.shape
        mem_rows = memory.shape[0]
        n_layers, n_heads, head_dim = self_o.shape[:3]
        inner = n_heads * head_dim
        half = inner // CORES
        hpg = half // head_dim
        all_keys = max(group * rows, CORES * mem_rows)
        weights = dict(
            self_q=self_q, self_k=self_k, self_v=self_v, self_o=self_o.reshape(n_layers, inner, width), cross_k=cross_k, cross_v=cross_v,
            cross_q=cross_q, cross_o=cross_o.reshape(n_layers, inner, width), mlp_gate=mlp_gate, mlp_up=mlp_up, mlp_down=mlp_down)
        w_scratch = [
            pltpu.VMEM((n_layers, width, half) if name in HALVED else weights[name].shape, BF16) for name in WEIGHTS]
        dma = pltpu.SemaphoreType.DMA
        vmem = pl.BlockSpec(memory_space=pltpu.VMEM)
        hbm = pl.BlockSpec(memory_space=pl.ANY)
        return pl.pallas_call(
            functools.partial(kernel, group, n_layers, head_dim),
            out_shape=jax.ShapeDtypeStruct((rows, width), BF16),
            in_specs=[vmem, hbm, pl.BlockSpec(memory_space=pltpu.SMEM), vmem, vmem, vmem] + [hbm] * len(WEIGHTS),
            out_specs=vmem,
            scratch_shapes=w_scratch + [
                pltpu.VMEM((CORES, mem_rows, width), BF16),
                pltpu.VMEM((n_layers, group, rows, width), BF16),
                pltpu.VMEM((group, rows, width), BF16),
                pltpu.VMEM((group, rows, width), BF16),
                pltpu.VMEM((n_layers, CORES * mem_rows, half), BF16),
                pltpu.VMEM((n_layers, CORES * mem_rows, half), BF16),
                pltpu.VMEM((n_layers, CORES, rows, half), BF16),
                pltpu.VMEM((n_layers, group, rows, half), BF16),
                pltpu.VMEM((n_layers, group, rows, half), BF16),
                pltpu.VMEM((n_layers, group, rows, half), BF16),
                pltpu.VMEM((n_layers, group, 2 * hpg, rows), F32),
                pltpu.VMEM((n_layers, group, 2 * hpg, rows), F32),
                pltpu.VMEM((rows, width), BF16),
                pltpu.VMEM((hpg * rows, all_keys), F32),
                pltpu.VMEM((hpg * rows, all_keys), F32),
                pltpu.VMEM((hpg * rows, all_keys), BF16),
                pltpu.VMEM((hpg * rows, all_keys), BF16),
                dma((len(WEIGHTS), n_layers)),
                dma((1,)), dma((1,)), dma((1,)),
                dma((n_layers, 8)), dma((n_layers, group // CORES - 1, 2)), dma((n_layers, group, 2)),
                dma((n_layers, group)), dma((n_layers, group)),
                dma((n_layers, group)), dma((n_layers, group)),
                dma((n_layers, group)), dma((n_layers, group)),
            ],
            compiler_params=pltpu.CompilerParams(collective_id=0, has_side_effects=True, vmem_limit_bytes=60 * 1024 * 1024),
        )(hidden, memory, mem_len, norm_self, norm_cross, norm_mlp, *[weights[name] for name in WEIGHTS])

    return jax.shard_map(local_step, mesh=mesh, in_specs=(row_spec, row_spec, P('dp')) + (P(),) * 14, out_specs=row_spec, check_vma=False)
```
